32 devices in a mesh: group: 2 (over core), gx: 4 (over y, x), gy: 4 (over z).
Axes of the slice: x: 2, y: 2, z: 4, core: 2. Of those that a mesh axis runs over, the one named last changes fastest.
Arguments:
- forcing: float32 [2, 80, 32, 1024], P('group', None, 'gx', 'gy'), may hold values from -24 to 24
- conduct: bfloat16 [2, 80, 32, 1024], P('group', None, 'gx', 'gy'), may hold values from 0.25 to 4
- diag_add: bfloat16 [2, 80, 32, 1024], P('group', None, 'gx', 'gy'), may hold values from 0.049804688 to 0.5
- ice_mask: int32 [32, 1024], P('gx', 'gy'), may hold values 0 or 1
- grounded: int32 [32, 1024], P('gx', 'gy'), may hold values 0 or 1
Outputs:
- solution: float32 [2, 80, 32, 1024], P('group', None, 'gx', 'gy')
- residual: float32 [2, 80, 32, 1024], P('group', None, 'gx', 'gy')
The draws below stay inside these ranges and needn't reach their ends.
All inputs are finite; a program needn't handle non-finite values. No bound on the sum of `ice_mask` or of `grounded` on one device may be relied on, other than what follows from the above.
Results may differ from the reference program's by a relative error of at most 0.0003.
Values sent between devices are 32-bit elements; how exact they have to be, the bound alone decides.
No kernel may reach another device: no remote copies, remote signals or barrier semaphores. Data moves between devices by JAX's collectives and lax.ppermute only.
A program may use at most 64 MiB of HBM per device.

```python
import math
import jax
import jax.numpy as jnp
from jax import lax

LAYERS = 80
ITERS = 6
NX = 32
NY = 1024


def place_ends(result, own_key, low, high):
    longest = result.shape.index(max(result.shape))
    spots = []
    for shift in (0, 1):
        where = [jax.random.randint(jax.random.fold_in(own_key, axis), (), 0, length) for axis, length in enumerate(result.shape)]
        where[longest] = (where[longest] + shift) % result.shape[longest]
        spots.append(tuple(where))
    return result.at[spots[0]].set(low).at[spots[1]].set(high)


def steps_of(key, dims, cuts, low, largest):
    def one(dim, parts):
        steps = jax.random.uniform(jax.random.fold_in(jax.random.fold_in(key, 6), dim), (parts,), jnp.float32, low / len(cuts), largest / len(cuts))
        return jnp.repeat(jnp.exp(steps), dims[dim] // parts).reshape((-1,) + (1,) * (len(dims) - dim - 1))

    loudness = one(*cuts[0])
    for cut in cuts[1:]:
        loudness = loudness * one(*cut)
    return loudness


def noise(stream_key, shape, scale, most, pieces=(), held_as=jnp.bfloat16):
    entries = jax.random.normal(stream_key, shape, jnp.float32) * scale
    if len(pieces) > 0:
        entries = steps_of(stream_key, shape, pieces, -0.22, 0.18) * entries
    return jnp.clip(entries, min=-most, max=most).astype(held_as)


def setup_inputs(seed: int = 0) -> dict:
    streams_of = jax.random.split(jax.random.key(seed), 6)
    forcing = noise(streams_of[0], (2, LAYERS, NX, NY), 4.0, 24.0, ((0, 2), (2, 4), (3, 4)), jnp.float32)
    conduct = jnp.clip(jnp.exp(math.log(4.0) - 2.7725887 * jax.random.uniform(streams_of[1], (2, LAYERS, NX, NY), jnp.float32) ** steps_of(streams_of[1], (2, LAYERS, NX, NY), ((0, 2), (2, 4), (3, 4)), -0.2, 0.2)), 0.25, 4.0).astype(jnp.bfloat16)
    diag_add = jnp.clip(jnp.exp(math.log(0.5) - 2.306499 * jax.random.uniform(streams_of[2], (2, LAYERS, NX, NY), jnp.float32) ** steps_of(streams_of[2], (2, LAYERS, NX, NY), ((0, 2), (2, 4), (3, 4)), -0.2, 0.2)), 0.049804688, 0.5).astype(jnp.bfloat16)
    ice_mask = place_ends((jax.random.randint(streams_of[3], (NX, NY), 0, 8) < 7).astype(jnp.int32), jax.random.fold_in(streams_of[3], 1), 0, 1)
    grounded = place_ends((jax.random.randint(streams_of[4], (NX, NY), 0, 8) < 3).astype(jnp.int32), jax.random.fold_in(streams_of[4], 1), 0, 1)
    return dict(forcing=forcing, conduct=conduct, diag_add=diag_add, ice_mask=ice_mask, grounded=grounded)


far_weight = 0.25
cross_weight = 0.5
vertical_weight = 4.0
friction_gain = 8.0
NEIGHBOURS = ((1, 0, 1.0), (-1, 0, 1.0), (0, 1, 1.0), (0, -1, 1.0), (2, 0, far_weight), (-2, 0, far_weight), (0, 2, far_weight), (0, -2, far_weight), (1, 1, cross_weight), (1, -1, cross_weight), (-1, 1, cross_weight), (-1, -1, cross_weight))

def beside_sum(padded, extent_x, extent_y):
    summed = jnp.zeros((padded.shape[0], extent_x, extent_y), jnp.float32)
    for shift_x, shift_y, weight in NEIGHBOURS:
        summed = summed + weight * padded[:, 2 + shift_x:2 + shift_x + extent_x, 2 + shift_y:2 + shift_y + extent_y]
    return summed

def vertical_sum(values):
    zeroes = jnp.zeros_like(values[:1])
    return jnp.concatenate([values[1:], zeroes], 0) + jnp.concatenate([zeroes, values[:-1]], 0)

def spread(values):
    padded = jnp.pad(values, ((0, 0), (2, 2), (2, 2)))
    return beside_sum(padded, values.shape[1], values.shape[2]) + vertical_weight * vertical_sum(values)

def group_setup(group_id, forcing, conduct, diag_add, ice_mask, grounded):
    ice_cells = ice_mask.astype(jnp.float32)
    ground_cells = grounded.astype(jnp.float32)
    if group_id == 0:
        active = ice_cells
    else:
        active = ice_cells * (1.0 - ground_cells)
    layers = forcing.shape[1]
    coupling = jnp.sqrt(conduct[group_id].astype(jnp.float32)) * active
    base_diag = diag_add[group_id].astype(jnp.float32)
    if group_id == 0:
        base_diag = base_diag.at[0].add(friction_gain * ground_cells * ice_cells)
    diagonal = base_diag + coupling * spread(coupling)
    edge_layer = 0 if group_id == 0 else layers - 1
    shared_value = active * lax.optimization_barrier(jnp.mean(forcing[group_id], axis=0))
    shared_weight = coupling[edge_layer]
    return (active, coupling, diagonal, edge_layer, shared_value, shared_weight)

def solve(source, coupling, diagonal):
    inverse = 1.0 / diagonal
    solution = jnp.zeros_like(source)
    residual = source
    precond = inverse * residual
    direction = precond
    norm_now = jnp.sum(residual * precond)
    for iteration in range(ITERS):
        applied = diagonal * direction - coupling * spread(coupling * direction)
        step_size = norm_now / jnp.sum(direction * applied)
        solution = solution + step_size * direction
        residual = residual - step_size * applied
        if iteration + 1 < ITERS:
            precond = inverse * residual
            norm_next = jnp.sum(residual * precond)
            direction = precond + norm_next / norm_now * direction
            norm_now = norm_next
    return (solution, residual)

def reference(forcing, conduct, diag_add, ice_mask, grounded):
    setups = [group_setup(group_id, forcing, conduct, diag_add, ice_mask, grounded) for group_id in (0, 1)]
    solutions = []
    residuals = []
    for group_id in (0, 1):
        active, coupling, diagonal, edge_layer, shared_value, shared_weight = setups[group_id]
        partner = setups[1 - group_id]
        source = active * forcing[group_id]
        source = source.at[edge_layer].add(active * partner[5] * partner[4])
        solution, residual = solve(source, coupling, diagonal)
        solutions.append(solution)
        residuals.append(residual)
    return (jnp.stack(solutions), jnp.stack(residuals))
```

```python
import math

import jax
import jax.numpy as jnp
from jax import lax
from jax.sharding import PartitionSpec as P

ITERS = 6


far_weight = 0.25
cross_weight = 0.5
vertical_weight = 4.0
friction_gain = 8.0
NEIGHBOURS = (
    (1, 0, 1.0),
    (-1, 0, 1.0),
    (0, 1, 1.0),
    (0, -1, 1.0),
    (2, 0, far_weight),
    (-2, 0, far_weight),
    (0, 2, far_weight),
    (0, -2, far_weight),
    (1, 1, cross_weight),
    (1, -1, cross_weight),
    (-1, 1, cross_weight),
    (-1, -1, cross_weight),
)


def with_halo(block, sides, width):
    for axis, dim in sides:
        count = lax.axis_size(axis)
        place = lax.axis_index(axis)
        ahead = [(i, (i + 1) % count) for i in range(count)]
        back = [(target, source) for source, target in ahead]
        low = lax.ppermute(
            lax.slice_in_dim(block, block.shape[dim] - width, None, axis=dim), axis, ahead
        )
        high = lax.ppermute(lax.slice_in_dim(block, 0, width, axis=dim), axis, back)
        low = jnp.where(place > 0, low, 0.0)
        high = jnp.where(place < count - 1, high, 0.0)
        block = jnp.concatenate([low, block, high], axis=dim)
    return block


def from_partner(shard, axis, distance):
    return lax.ppermute(shard, axis, [(i, i ^ 1 << distance) for i in range(lax.axis_size(axis))])


def beside_sum(padded, extent_x, extent_y):
    summed = jnp.zeros((padded.shape[0], extent_x, extent_y), jnp.float32)
    for shift_x, shift_y, weight in NEIGHBOURS:
        summed = (
            summed
            + weight
            * padded[:, 2 + shift_x : 2 + shift_x + extent_x, 2 + shift_y : 2 + shift_y + extent_y]
        )
    return summed


def vertical_sum(values):
    zeroes = jnp.zeros_like(values[:1])
    return jnp.concatenate([values[1:], zeroes], 0) + jnp.concatenate([zeroes, values[:-1]], 0)


def spread_padded(padded, values):
    return beside_sum(padded, values.shape[1], values.shape[2]) + vertical_weight * vertical_sum(
        values
    )


def operate(vector, coupling, diagonal):
    scaled = coupling * vector
    padded = with_halo(scaled, (("gx", 1), ("gy", 2)), 2)
    return diagonal * vector - coupling * spread_padded(padded, scaled)


def sum_over(partial, axes):
    count = math.prod(lax.axis_size(axis) for axis in axes)
    sent = jnp.broadcast_to(partial[None, None], (count, 1) + partial.shape)
    return jnp.sum(lax.all_to_all(sent, axes, 0, 0, tiled=True), axis=(0, 1))


def paired_sums(residual, precond, applied):
    partial = jnp.stack([jnp.sum(residual * precond), jnp.sum(applied * precond)])
    summed = sum_over(partial, ("gx", "gy"))
    return summed[0], summed[1]


def on_device(forcing, conduct, diag_add, ice_mask, grounded):
    own_force = forcing[0]
    layers = own_force.shape[0]
    group_id = lax.axis_index("group")
    is_ice = (group_id == 0).astype(jnp.float32)
    ice_cells = ice_mask.astype(jnp.float32)
    ground_cells = grounded.astype(jnp.float32)
    active = ice_cells * (1.0 - (1.0 - is_ice) * ground_cells)
    coupling = jnp.sqrt(conduct[0].astype(jnp.float32)) * active
    layer_index = lax.broadcasted_iota(jnp.int32, (layers, 1, 1), 0)
    edge_layer = jnp.where(group_id == 0, 0, layers - 1).astype(jnp.int32)
    edge_pick = (layer_index == edge_layer).astype(jnp.float32)
    bottom = (layer_index == 0).astype(jnp.float32)
    base_diag = diag_add[0].astype(jnp.float32) + bottom * (
        is_ice * friction_gain * ground_cells * ice_cells
    )
    padded_coupling = with_halo(coupling, (("gx", 1), ("gy", 2)), 2)
    diagonal = base_diag + coupling * spread_padded(padded_coupling, coupling)
    shared_value = active * jnp.mean(own_force, axis=0)
    shared_weight = lax.dynamic_index_in_dim(coupling, edge_layer, 0, keepdims=False)
    received = from_partner(jnp.stack([shared_value, shared_weight]), "group", 0)
    source = active * own_force + edge_pick * (active * received[1] * received[0])
    inverse = 1.0 / diagonal
    solution = jnp.zeros_like(source)
    residual = source
    precond = inverse * residual
    applied = operate(precond, coupling, diagonal)
    norm_now, curve = paired_sums(residual, precond, applied)
    step_size = norm_now / curve
    direction = precond
    along = applied
    for iteration in range(ITERS):
        solution = solution + step_size * direction
        residual = residual - step_size * along
        if iteration + 1 < ITERS:
            precond = inverse * residual
            applied = operate(precond, coupling, diagonal)
            norm_next, curve = paired_sums(residual, precond, applied)
            step_ratio = norm_next / norm_now
            step_size = norm_next / (curve - step_ratio * norm_next / step_size)
            direction = precond + step_ratio * direction
            along = applied + step_ratio * along
            norm_now = norm_next
    return (solution[None], residual[None])


def solution(mesh):
    in_specs = (
        P("group", None, "gx", "gy"),
        P("group", None, "gx", "gy"),
        P("group", None, "gx", "gy"),
        P("gx", "gy"),
        P("gx", "gy"),
    )
    out_specs = (P("group", None, "gx", "gy"), P("group", None, "gx", "gy"))
    return jax.shard_map(
        on_device, mesh=mesh, in_specs=in_specs, out_specs=out_specs, check_vma=False
    )
```

```python
import math

import jax
import jax.numpy as jnp
from jax import lax
from jax.experimental import pallas as pl
from jax.experimental.pallas import tpu as pltpu
from jax.sharding import PartitionSpec as P

ITERS = 6
LANES = 128
SUBLANES = 8
HALO = 16
SHIFTS = (0.0, 0.75, 1.5, 0.25, 1.75, 1.0)
PAIRS = tuple((i, j) for i in range(ITERS + 1) for j in range(i + 1) if j < ITERS)


far_weight = 0.25
cross_weight = 0.5
vertical_weight = 4.0
friction_gain = 8.0
NEIGHBOURS = (
    (1, 0, 1.0),
    (-1, 0, 1.0),
    (0, 1, 1.0),
    (0, -1, 1.0),
    (2, 0, far_weight),
    (-2, 0, far_weight),
    (0, 2, far_weight),
    (0, -2, far_weight),
    (1, 1, cross_weight),
    (1, -1, cross_weight),
    (-1, 1, cross_weight),
    (-1, -1, cross_weight),
)


def with_halo(block, sides, width):
    for axis, dim in sides:
        count = lax.axis_size(axis)
        place = lax.axis_index(axis)
        ahead = [(i, (i + 1) % count) for i in range(count)]
        back = [(target, source) for source, target in ahead]
        low = lax.ppermute(
            lax.slice_in_dim(block, block.shape[dim] - width, None, axis=dim), axis, ahead
        )
        high = lax.ppermute(lax.slice_in_dim(block, 0, width, axis=dim), axis, back)
        low = jnp.where(place > 0, low, 0.0)
        high = jnp.where(place < count - 1, high, 0.0)
        block = jnp.concatenate([low, block, high], axis=dim)
    return block


def from_partner(shard, axis, distance):
    return lax.ppermute(shard, axis, [(i, i ^ 1 << distance) for i in range(lax.axis_size(axis))])


def beside_sum(padded, extent_x, extent_y):
    summed = jnp.zeros((padded.shape[0], extent_x, extent_y), jnp.float32)
    for shift_x, shift_y, weight in NEIGHBOURS:
        summed = (
            summed
            + weight
            * padded[:, 2 + shift_x : 2 + shift_x + extent_x, 2 + shift_y : 2 + shift_y + extent_y]
        )
    return summed


def vertical_sum(values):
    zeroes = jnp.zeros_like(values[:1])
    return jnp.concatenate([values[1:], zeroes], 0) + jnp.concatenate([zeroes, values[:-1]], 0)


def spread_padded(padded, values):
    return beside_sum(padded, values.shape[1], values.shape[2]) + vertical_weight * vertical_sum(
        values
    )


def operate(vector, coupling, diagonal):
    scaled = coupling * vector
    padded = with_halo(scaled, (("gx", 1), ("gy", 2)), 2)
    return diagonal * vector - coupling * spread_padded(padded, scaled)


def sum_over(partial, axes):
    count = math.prod(lax.axis_size(axis) for axis in axes)
    sent = jnp.broadcast_to(partial[None, None], (count, 1) + partial.shape)
    return jnp.sum(lax.all_to_all(sent, axes, 0, 0, tiled=True), axis=(0, 1))


def paired_sums(residual, precond, applied):
    partial = jnp.stack([jnp.sum(residual * precond), jnp.sum(applied * precond)])
    summed = sum_over(partial, ("gx", "gy"))
    return summed[0], summed[1]


def on_device(forcing, conduct, diag_add, ice_mask, grounded):
    own_force = forcing[0]
    layers = own_force.shape[0]
    group_id = lax.axis_index("group")
    is_ice = (group_id == 0).astype(jnp.float32)
    ice_cells = ice_mask.astype(jnp.float32)
    ground_cells = grounded.astype(jnp.float32)
    active = ice_cells * (1.0 - (1.0 - is_ice) * ground_cells)
    coupling = jnp.sqrt(conduct[0].astype(jnp.float32)) * active
    layer_index = lax.broadcasted_iota(jnp.int32, (layers, 1, 1), 0)
    edge_layer = jnp.where(group_id == 0, 0, layers - 1).astype(jnp.int32)
    edge_pick = (layer_index == edge_layer).astype(jnp.float32)
    bottom = (layer_index == 0).astype(jnp.float32)
    base_diag = diag_add[0].astype(jnp.float32) + bottom * (
        is_ice * friction_gain * ground_cells * ice_cells
    )
    padded_coupling = with_halo(coupling, (("gx", 1), ("gy", 2)), 2)
    diagonal = base_diag + coupling * spread_padded(padded_coupling, coupling)
    shared_value = active * jnp.mean(own_force, axis=0)
    shared_weight = lax.dynamic_index_in_dim(coupling, edge_layer, 0, keepdims=False)
    received = from_partner(jnp.stack([shared_value, shared_weight]), "group", 0)
    source = active * own_force + edge_pick * (active * received[1] * received[0])
    inverse = 1.0 / diagonal
    solution = jnp.zeros_like(source)
    residual = source
    precond = inverse * residual
    applied = operate(precond, coupling, diagonal)
    norm_now, curve = paired_sums(residual, precond, applied)
    step_size = norm_now / curve
    direction = precond
    along = applied
    for iteration in range(ITERS):
        solution = solution + step_size * direction
        residual = residual - step_size * along
        if iteration + 1 < ITERS:
            precond = inverse * residual
            applied = operate(precond, coupling, diagonal)
            norm_next, curve = paired_sums(residual, precond, applied)
            step_ratio = norm_next / norm_now
            step_size = norm_next / (curve - step_ratio * norm_next / step_size)
            direction = precond + step_ratio * direction
            along = applied + step_ratio * along
            norm_now = norm_next
    return (solution[None], residual[None])


def ring(count, step):
    return [(i, (i + step) % count) for i in range(count)]


def lanes_of(rows):
    return lax.broadcasted_iota(jnp.int32, (rows, LANES), 1)


def prepare_kernel(group_ref, force_ref, conduct_ref, diag_ref, ice_ref, ground_ref, fields_ref, low_ref, high_ref):
    layers = force_ref.shape[1]
    per_group = LANES // HALO
    is_ice = jnp.where(group_ref[0] == 0, 1.0, 0.0)
    ice = ice_ref[...].astype(jnp.float32)
    ground = ground_ref[...].astype(jnp.float32)
    active = ice * (1.0 - (1.0 - is_ice) * ground)
    friction = is_ice * friction_gain * ground * ice
    lane = lanes_of(SUBLANES)

    def step(q, carry):
        low, high = [None] * 3, [None] * 3
        for j in range(per_group):
            layer = q * per_group + j
            coupling = jnp.sqrt(conduct_ref[0, layer].astype(jnp.float32)) * active
            base = diag_ref[0, layer].astype(jnp.float32)
            if j == 0:
                base = base + friction * jnp.where(q == 0, 1.0, 0.0)
            force = active * force_ref[0, layer]
            for k, value in enumerate((coupling, base, force)):
                fields_ref[k, layer] = value
                first = pltpu.roll(value[:, :LANES], HALO * j, 1) if j else value[:, :LANES]
                last = value[:, -LANES:]
                turn = (HALO * (j + 1)) % LANES
                last = pltpu.roll(last, turn, 1) if turn else last
                if j == 0:
                    low[k], high[k] = first, last
                else:
                    here = lane >= HALO * j
                    low[k] = jnp.where(here, first, low[k])
                    high[k] = jnp.where(here, last, high[k])
        for k in range(3):
            low_ref[k, q] = low[k]
            high_ref[k, q] = high[k]
        return carry

    lax.fori_loop(0, layers // per_group, step, 0)


def pack_kernel(edge_ref, fields_ref, low_ref, high_ref, out_ref):
    layers = fields_ref.shape[1]
    count = out_ref.shape[0]
    per_group = LANES // HALO
    spare = LANES - 3 * LANES // 4
    width = fields_ref.shape[3] // count
    lane = lanes_of(SUBLANES)

    def step(q, carry):
        for k in range(3):
            low, high = low_ref[k, q], high_ref[k, q]
            if k == 0:
                low, high = low * edge_ref[0], high * edge_ref[1]
            main = [[None] * 3 for _ in range(count)]
            for j in range(per_group):
                value = fields_ref[k, q * per_group + j]
                pieces = [
                    pltpu.roll(value[:, p * LANES : (p + 1) * LANES], HALO, 1)
                    for p in range(value.shape[1] // LANES)
                ]
                turn = (LANES - HALO * j) % LANES
                before = pltpu.roll(low, turn, 1) if turn else low
                turn = (LANES - HALO * j + HALO) % LANES
                after = pltpu.roll(high, turn, 1) if turn else high
                wide = [jnp.where(lane < HALO, before, pieces[0])]
                for p in range(1, len(pieces)):
                    wide.append(jnp.where(lane < HALO, pieces[p - 1], pieces[p]))
                wide.append(jnp.where(lane < HALO, pieces[-1], after))
                turned = [pltpu.roll(piece, width, 1) for piece in wide]
                for d in range(count):
                    p = d * width // LANES
                    if d * width % LANES == 0:
                        window = wide[p]
                    else:
                        window = jnp.where(lane < width, turned[p], turned[p + 1])
                    m = j % 4
                    if m < 3:
                        main[d][m] = window
                    else:
                        for n in range(3):
                            tail = pltpu.roll(window, LANES - spare * (n + 1), 1)
                            out_ref[d, k, q * (per_group // 4) + j // 4, n] = jnp.where(
                                lane < LANES - spare, main[d][n], tail
                            )
        return carry

    lax.fori_loop(0, layers // per_group, step, 0)


def unpack_kernel(edge_ref, got_ref, fields_ref, shared_ref):
    count, _, groups = got_ref.shape[:3]
    layers = 4 * groups
    spare = LANES // 4
    lane = lanes_of(SUBLANES)
    for d in range(count):
        rows = pl.ds(SUBLANES * d, SUBLANES)

        def step(g, total, d=d, rows=rows):
            for k in range(3):
                fill = 1.0 if k == 1 else 0.0
                held = [got_ref[d, k, g, n] for n in range(3)]
                last = jnp.where(
                    lane < spare,
                    pltpu.roll(held[0], spare, 1),
                    jnp.where(
                        lane < 2 * spare, pltpu.roll(held[1], 2 * spare, 1), pltpu.roll(held[2], 3 * spare, 1)
                    ),
                )
                for n, value in enumerate(held + [last]):
                    value = jnp.where(lane < LANES - spare, value, fill)
                    fields_ref[k, 4 * g + n, rows] = value
                    if k == 2:
                        total = total + value
            return total

        total = lax.fori_loop(0, groups, step, jnp.zeros((SUBLANES, LANES), jnp.float32), unroll=2)
        shared_ref[0, rows] = total / layers
        shared_ref[1, rows] = fields_ref[0, edge_ref[0], rows]


def two_sum(a, b):
    total = a + b
    part = total - a
    return total, (a - (total - part)) + (b - part)


def add_pairs(high, low, other_high, other_low):
    total, error = two_sum(high, other_high)
    return total, low + other_low + error


def stencil(held_ref, layer, rows):
    def at(shift):
        return held_ref[layer + 1, pl.ds(SUBLANES + shift, rows)]

    here = at(0)
    near = at(1) + at(-1)
    mixed = here + cross_weight * near
    far = at(2) + at(-2) + pltpu.roll(here, 2, 1) + pltpu.roll(here, LANES - 2, 1)
    beside = near + pltpu.roll(mixed, 1, 1) + pltpu.roll(mixed, LANES - 1, 1) + far_weight * far
    above = held_ref[layer + 2, pl.ds(SUBLANES, rows)] + held_ref[layer, pl.ds(SUBLANES, rows)]
    return beside + vertical_weight * above


def krylov_kernel(edge_ref, fields_ref, got_ref, basis_ref, scale_ref, sums_ref, held_ref, factor_ref, gram_ref):
    layers, rows = fields_ref.shape[1:3]
    inner = pl.ds(SUBLANES, rows)
    empty = jnp.zeros((layers + 2, SUBLANES, LANES), jnp.float32)
    for side in range(2):
        held_ref[side, :, :SUBLANES] = empty
        held_ref[side, :, SUBLANES + rows :] = empty
        held_ref[side, 0] = jnp.zeros((rows + 2 * SUBLANES, LANES), jnp.float32)
        held_ref[side, layers + 1] = jnp.zeros((rows + 2 * SUBLANES, LANES), jnp.float32)

    def fill(layer, carry):
        held_ref[0, layer + 1, inner] = fields_ref[0, layer]
        return carry

    lax.fori_loop(0, layers, fill, 0, unroll=4)
    active = jnp.where(fields_ref[0, 0] > 0.0, 1.0, 0.0)
    term = active * got_ref[1] * got_ref[0]

    def begin(layer, carry):
        coupling = fields_ref[0, layer]
        diagonal = fields_ref[1, layer] + coupling * stencil(held_ref.at[0], layer, rows)
        root = jnp.sqrt(diagonal)
        inverse = 1.0 / root
        factor = coupling * inverse
        source = fields_ref[2, layer] + term * jnp.where(layer == edge_ref[0], 1.0, 0.0)
        vector = source * inverse
        scale_ref[0, layer] = inverse
        scale_ref[1, layer] = root
        factor_ref[layer] = factor
        basis_ref[0, layer] = vector
        held_ref[1, layer + 1, inner] = factor * vector
        return carry

    lax.fori_loop(0, layers, begin, 0, unroll=2)
    for k in range(ITERS):
        source_side = (k + 1) % 2

        def apply(layer, carry, k=k, source_side=source_side):
            factor = factor_ref[layer]
            spread = stencil(held_ref.at[source_side], layer, rows)
            vector = (1.0 - SHIFTS[k]) * basis_ref[k, layer] - factor * spread
            basis_ref[k + 1, layer] = vector
            if k + 1 < ITERS:
                held_ref[1 - source_side, layer + 1, inner] = factor * vector
            return carry

        lax.fori_loop(0, layers, apply, 0, unroll=2)

    lane = lanes_of(SUBLANES)
    width = LANES - LANES // 4 - 2 * HALO
    own = (lane >= HALO) & (lane < HALO + width)
    gram_ref[...] = jnp.zeros(gram_ref.shape, jnp.float32)

    def products(g, carry):
        sums = [None] * len(PAIRS)
        for n in range(2):
            for d in range(rows // SUBLANES):
                vectors = [basis_ref[k, 2 * g + n, pl.ds(SUBLANES * d, SUBLANES)] for k in range(ITERS + 1)]
                masked = [jnp.where(own, vector, 0.0) for vector in vectors]
                for p, (i, j) in enumerate(PAIRS):
                    product = masked[j] * vectors[i]
                    sums[p] = product if sums[p] is None else sums[p] + product
        for p in range(len(PAIRS)):
            high, low = add_pairs(gram_ref[0, p], gram_ref[1, p], sums[p], 0.0)
            gram_ref[0, p] = high
            gram_ref[1, p] = low
        return carry

    lax.fori_loop(0, layers // 2, products, 0)
    high, low = gram_ref[0, :, 0], gram_ref[1, :, 0]
    for row in range(1, SUBLANES):
        high, low = add_pairs(high, low, gram_ref[0, :, row], gram_ref[1, :, row])
    turn = LANES // 2
    while turn:
        high, low = add_pairs(high, low, pltpu.roll(high, turn, 1), pltpu.roll(low, turn, 1))
        turn //= 2
    packed = high[:SUBLANES]
    share = LANES // 4
    for g in range(4):
        part = slice(SUBLANES * g, SUBLANES * (g + 1))
        if g:
            packed = jnp.where(lane >= share * g, high[part], packed)
        packed = jnp.where((lane >= share * g + share // 2) & (lane < share * (g + 1)), low[part], packed)
    for d in range(sums_ref.shape[0]):
        sums_ref[d] = packed


def tree_sum(terms):
    while len(terms) > 1:
        terms = [sum(terms[i : i + 2]) for i in range(0, len(terms), 2)]
    return terms[0]


def quadratic(gram, left, right):
    products = []
    for i, a in enumerate(left):
        inside = [gram[max(i, j), min(i, j)] * b for j, b in enumerate(right)]
        products.append(a * tree_sum(inside))
    return tree_sum(products)


def iterate(gram):
    one = jnp.ones_like(gram[0, 0])
    zero = jnp.zeros_like(one)
    residual, direction, answer = [one], [one], []
    norm = gram[0, 0]
    for iteration in range(ITERS):
        applied = [SHIFTS[k] * c if SHIFTS[k] else zero for k, c in enumerate(direction)] + [zero]
        for k, c in enumerate(direction):
            applied[k + 1] = applied[k + 1] + c
        curve = quadratic(gram, direction, applied)
        step = norm / curve
        answer = [a + step * c for a, c in zip(answer + [zero], direction)]
        residual = [r - step * c for r, c in zip(residual + [zero], applied)]
        if iteration + 1 < ITERS:
            following = quadratic(gram, residual, residual)
            ratio = following / norm
            direction = [r + ratio * c for r, c in zip(residual, direction + [zero])]
            norm = following
    return answer, residual


def combine_kernel(sums_ref, basis_ref, scale_ref, out_ref, gram_ref):
    layers, rows = basis_ref.shape[1:3]
    share = LANES // 4
    parts = [(sums_ref[d], pltpu.roll(sums_ref[d], LANES - share // 2, 1)) for d in range(sums_ref.shape[0])]
    while len(parts) > 1:
        parts = [add_pairs(*parts[i], *parts[i + 1]) if i + 1 < len(parts) else parts[i] for i in range(0, len(parts), 2)]
    gram_ref[...] = parts[0][0] + parts[0][1]
    gram = {
        pair: gram_ref[pl.ds(p % SUBLANES, 1), pl.ds(share * (p // SUBLANES), 1)] for p, pair in enumerate(PAIRS)
    }
    answer, residual = iterate(gram)
    answer = [jnp.broadcast_to(c, (SUBLANES, LANES)) for c in answer]
    residual = [jnp.broadcast_to(c, (SUBLANES, LANES)) for c in residual]
    half = LANES // 2
    lane = lanes_of(SUBLANES)

    def step(layer, carry):
        for d in range(rows // SUBLANES):
            part = pl.ds(SUBLANES * d, SUBLANES)
            vectors = [basis_ref[k, layer, part] for k in range(ITERS + 1)]
            first = tree_sum([c * v for c, v in zip(answer, vectors)]) * scale_ref[0, layer, part]
            second = tree_sum([c * v for c, v in zip(residual, vectors)]) * scale_ref[1, layer, part]
            out_ref[d, layer] = jnp.where(
                lane < half, pltpu.roll(first, LANES - HALO, 1), pltpu.roll(second, half - HALO, 1)
            )
        return carry

    lax.fori_loop(0, layers, step, 0, unroll=2)


def finish_kernel(got_ref, solution_ref, residual_ref):
    count, layers = got_ref.shape[:2]
    half = LANES // 2
    lane = lanes_of(SUBLANES)

    def step(layer, carry):
        for p in range(count // 2):
            left, right = got_ref[2 * p, layer], got_ref[2 * p + 1, layer]
            place = pl.ds(LANES * p, LANES)
            solution_ref[0, layer, :, place] = jnp.where(lane < half, left, pltpu.roll(right, half, 1))
            residual_ref[0, layer, :, place] = jnp.where(lane < half, pltpu.roll(left, half, 1), right)
        return carry

    lax.fori_loop(0, layers, step, 0, unroll=4)


def call(kernel, outs, specs, *args, scratch=(), limit=24):
    return pl.pallas_call(
        kernel,
        name=kernel.__name__,
        out_shape=[jax.ShapeDtypeStruct(shape, jnp.float32) for shape in outs],
        in_specs=[pl.BlockSpec(memory_space=pltpu.SMEM)] * specs
        + [pl.BlockSpec(memory_space=pltpu.VMEM)] * (len(args) - specs),
        out_specs=[pl.BlockSpec(memory_space=pltpu.VMEM)] * len(outs),
        scratch_shapes=[pltpu.VMEM(shape, jnp.float32) for shape in scratch],
        compiler_params=pltpu.CompilerParams(vmem_limit_bytes=limit * 2**20),
    )(*args)


def in_windows(forcing, conduct, diag_add, ice_mask, grounded):
    _, layers, block_x, block_y = forcing.shape
    count_x, count_y = lax.axis_size("gx"), lax.axis_size("gy")
    rows = count_x * block_x
    group = lax.axis_index("group").astype(jnp.int32)
    place = lax.axis_index("gy")
    edge = jnp.where(group == 0, 0, layers - 1).astype(jnp.int32)[None]
    inside = jnp.stack([place > 0, place < count_y - 1]).astype(jnp.float32)
    rim = (3, layers * HALO // LANES, block_x, LANES)
    fields, low, high = call(
        prepare_kernel, [(3, layers, block_x, block_y), rim, rim], 1,
        group[None], forcing, conduct, diag_add, ice_mask, grounded,
    )
    before = lax.ppermute(high, "gy", ring(count_y, 1))
    after = lax.ppermute(low, "gy", ring(count_y, -1))
    (packed,) = call(
        pack_kernel, [(count_x, 3, layers // 4, 3, block_x, LANES)], 1, inside, fields, before, after
    )
    got = lax.all_to_all(packed, "gx", 0, 0, tiled=True)
    windows, shared = call(
        unpack_kernel, [(3, layers, rows, LANES), (2, rows, LANES)], 1, edge, got
    )
    received = from_partner(shared, "group", 0)
    padded = rows + 2 * SUBLANES
    basis, scale, sums = call(
        krylov_kernel,
        [(ITERS + 1, layers, rows, LANES), (2, layers, rows, LANES), (count_x * count_y, SUBLANES, LANES)],
        1, edge, windows, received,
        scratch=[(2, layers + 2, padded, LANES), (layers, rows, LANES), (2, 32, SUBLANES, LANES)],
        limit=32,
    )
    sums = lax.all_to_all(sums, ("gx", "gy"), 0, 0, tiled=True)
    (mixed,) = call(
        combine_kernel, [(count_x, layers, block_x, LANES)], 0, sums, basis, scale,
        scratch=[(SUBLANES, LANES)],
    )
    mixed = lax.all_to_all(mixed, "gx", 0, 0, tiled=True)
    return tuple(call(finish_kernel, [forcing.shape, forcing.shape], 0, mixed))


def fits_windows(layers, block_x, block_y, count_x):
    width = block_y // count_x
    return (
        layers % (LANES // HALO) == 0
        and block_x == SUBLANES
        and block_y % LANES == 0
        and 2 * width == LANES
        and HALO >= 2 * (ITERS + 1)
    )


def per_device(forcing, conduct, diag_add, ice_mask, grounded):
    _, layers, block_x, block_y = forcing.shape
    way = in_windows if fits_windows(layers, block_x, block_y, lax.axis_size("gx")) else on_device
    return way(forcing, conduct, diag_add, ice_mask, grounded)


def solution(mesh):
    in_specs = (
        P("group", None, "gx", "gy"),
        P("group", None, "gx", "gy"),
        P("group", None, "gx", "gy"),
        P("gx", "gy"),
        P("gx", "gy"),
    )
    out_specs = (P("group", None, "gx", "gy"), P("group", None, "gx", "gy"))
    return jax.shard_map(
        per_device, mesh=mesh, in_specs=in_specs, out_specs=out_specs, check_vma=False
    )
```

```python
import math

import jax
import jax.numpy as jnp
from jax import lax
from jax.experimental import pallas as pl
from jax.experimental.pallas import tpu as pltpu
from jax.sharding import PartitionSpec as P

ITERS = 6
LANES = 128
SUBLANES = 8
HALO = 16
SHIFTS = (0.0, 0.75, 1.5, 0.25, 1.75, 1.0)
UNROLL = 8
PAIRS = tuple((i, j) for i in range(ITERS + 1) for j in range(i + 1) if j < ITERS)


far_weight = 0.25
cross_weight = 0.5
vertical_weight = 4.0
friction_gain = 8.0
NEIGHBOURS = (
    (1, 0, 1.0),
    (-1, 0, 1.0),
    (0, 1, 1.0),
    (0, -1, 1.0),
    (2, 0, far_weight),
    (-2, 0, far_weight),
    (0, 2, far_weight),
    (0, -2, far_weight),
    (1, 1, cross_weight),
    (1, -1, cross_weight),
    (-1, 1, cross_weight),
    (-1, -1, cross_weight),
)


def with_halo(block, sides, width):
    for axis, dim in sides:
        count = lax.axis_size(axis)
        place = lax.axis_index(axis)
        ahead = [(i, (i + 1) % count) for i in range(count)]
        back = [(target, source) for source, target in ahead]
        low = lax.ppermute(
            lax.slice_in_dim(block, block.shape[dim] - width, None, axis=dim), axis, ahead
        )
        high = lax.ppermute(lax.slice_in_dim(block, 0, width, axis=dim), axis, back)
        low = jnp.where(place > 0, low, 0.0)
        high = jnp.where(place < count - 1, high, 0.0)
        block = jnp.concatenate([low, block, high], axis=dim)
    return block


def from_partner(shard, axis, distance):
    return lax.ppermute(shard, axis, [(i, i ^ 1 << distance) for i in range(lax.axis_size(axis))])


def beside_sum(padded, extent_x, extent_y):
    summed = jnp.zeros((padded.shape[0], extent_x, extent_y), jnp.float32)
    for shift_x, shift_y, weight in NEIGHBOURS:
        summed = (
            summed
            + weight
            * padded[:, 2 + shift_x : 2 + shift_x + extent_x, 2 + shift_y : 2 + shift_y + extent_y]
        )
    return summed


def vertical_sum(values):
    zeroes = jnp.zeros_like(values[:1])
    return jnp.concatenate([values[1:], zeroes], 0) + jnp.concatenate([zeroes, values[:-1]], 0)


def spread_padded(padded, values):
    return beside_sum(padded, values.shape[1], values.shape[2]) + vertical_weight * vertical_sum(
        values
    )


def operate(vector, coupling, diagonal):
    scaled = coupling * vector
    padded = with_halo(scaled, (("gx", 1), ("gy", 2)), 2)
    return diagonal * vector - coupling * spread_padded(padded, scaled)


def sum_over(partial, axes):
    count = math.prod(lax.axis_size(axis) for axis in axes)
    sent = jnp.broadcast_to(partial[None, None], (count, 1) + partial.shape)
    return jnp.sum(lax.all_to_all(sent, axes, 0, 0, tiled=True), axis=(0, 1))


def paired_sums(residual, precond, applied):
    partial = jnp.stack([jnp.sum(residual * precond), jnp.sum(applied * precond)])
    summed = sum_over(partial, ("gx", "gy"))
    return summed[0], summed[1]


def on_device(forcing, conduct, diag_add, ice_mask, grounded):
    own_force = forcing[0]
    layers = own_force.shape[0]
    group_id = lax.axis_index("group")
    is_ice = (group_id == 0).astype(jnp.float32)
    ice_cells = ice_mask.astype(jnp.float32)
    ground_cells = grounded.astype(jnp.float32)
    active = ice_cells * (1.0 - (1.0 - is_ice) * ground_cells)
    coupling = jnp.sqrt(conduct[0].astype(jnp.float32)) * active
    layer_index = lax.broadcasted_iota(jnp.int32, (layers, 1, 1), 0)
    edge_layer = jnp.where(group_id == 0, 0, layers - 1).astype(jnp.int32)
    edge_pick = (layer_index == edge_layer).astype(jnp.float32)
    bottom = (layer_index == 0).astype(jnp.float32)
    base_diag = diag_add[0].astype(jnp.float32) + bottom * (
        is_ice * friction_gain * ground_cells * ice_cells
    )
    padded_coupling = with_halo(coupling, (("gx", 1), ("gy", 2)), 2)
    diagonal = base_diag + coupling * spread_padded(padded_coupling, coupling)
    shared_value = active * jnp.mean(own_force, axis=0)
    shared_weight = lax.dynamic_index_in_dim(coupling, edge_layer, 0, keepdims=False)
    received = from_partner(jnp.stack([shared_value, shared_weight]), "group", 0)
    source = active * own_force + edge_pick * (active * received[1] * received[0])
    inverse = 1.0 / diagonal
    solution = jnp.zeros_like(source)
    residual = source
    precond = inverse * residual
    applied = operate(precond, coupling, diagonal)
    norm_now, curve = paired_sums(residual, precond, applied)
    step_size = norm_now / curve
    direction = precond
    along = applied
    for iteration in range(ITERS):
        solution = solution + step_size * direction
        residual = residual - step_size * along
        if iteration + 1 < ITERS:
            precond = inverse * residual
            applied = operate(precond, coupling, diagonal)
            norm_next, curve = paired_sums(residual, precond, applied)
            step_ratio = norm_next / norm_now
            step_size = norm_next / (curve - step_ratio * norm_next / step_size)
            direction = precond + step_ratio * direction
            along = applied + step_ratio * along
            norm_now = norm_next
    return (solution[None], residual[None])


def ring(count, step):
    return [(i, (i + step) % count) for i in range(count)]


def lanes_of(rows):
    return lax.broadcasted_iota(jnp.int32, (rows, LANES), 1)


def prepare_kernel(group_ref, force_ref, conduct_ref, diag_ref, ice_ref, ground_ref, fields_ref, low_ref, high_ref):
    layers = force_ref.shape[1]
    per_group = LANES // HALO
    is_ice = jnp.where(group_ref[0] == 0, 1.0, 0.0)
    ice = ice_ref[...].astype(jnp.float32)
    ground = ground_ref[...].astype(jnp.float32)
    active = ice * (1.0 - (1.0 - is_ice) * ground)
    friction = is_ice * friction_gain * ground * ice
    lane = lanes_of(SUBLANES)

    def step(q, carry):
        low, high = [None] * 3, [None] * 3
        for j in range(per_group):
            layer = q * per_group + j
            coupling = jnp.sqrt(conduct_ref[0, layer].astype(jnp.float32)) * active
            base = diag_ref[0, layer].astype(jnp.float32)
            if j == 0:
                base = base + friction * jnp.where(q == 0, 1.0, 0.0)
            force = active * force_ref[0, layer]
            for k, value in enumerate((coupling, base, force)):
                fields_ref[k, layer] = value
                first = pltpu.roll(value[:, :LANES], HALO * j, 1) if j else value[:, :LANES]
                last = value[:, -LANES:]
                turn = (HALO * (j + 1)) % LANES
                last = pltpu.roll(last, turn, 1) if turn else last
                if j == 0:
                    low[k], high[k] = first, last
                else:
                    here = lane >= HALO * j
                    low[k] = jnp.where(here, first, low[k])
                    high[k] = jnp.where(here, last, high[k])
        for k in range(3):
            low_ref[k, q] = low[k]
            high_ref[k, q] = high[k]
        return carry

    lax.fori_loop(0, layers // per_group, step, 0)


def pack_kernel(edge_ref, fields_ref, low_ref, high_ref, out_ref):
    layers = fields_ref.shape[1]
    count = out_ref.shape[0]
    per_group = LANES // HALO
    spare = LANES - 3 * LANES // 4
    width = fields_ref.shape[3] // count
    lane = lanes_of(SUBLANES)

    def step(q, carry):
        for k in range(3):
            low, high = low_ref[k, q], high_ref[k, q]
            if k == 0:
                low, high = low * edge_ref[0], high * edge_ref[1]
            main = [[None] * 3 for _ in range(count)]
            for j in range(per_group):
                value = fields_ref[k, q * per_group + j]
                pieces = [
                    pltpu.roll(value[:, p * LANES : (p + 1) * LANES], HALO, 1)
                    for p in range(value.shape[1] // LANES)
                ]
                turn = (LANES - HALO * j) % LANES
                before = pltpu.roll(low, turn, 1) if turn else low
                turn = (LANES - HALO * j + HALO) % LANES
                after = pltpu.roll(high, turn, 1) if turn else high
                wide = [jnp.where(lane < HALO, before, pieces[0])]
                for p in range(1, len(pieces)):
                    wide.append(jnp.where(lane < HALO, pieces[p - 1], pieces[p]))
                wide.append(jnp.where(lane < HALO, pieces[-1], after))
                turned = [pltpu.roll(piece, width, 1) for piece in wide]
                for d in range(count):
                    p = d * width // LANES
                    if d * width % LANES == 0:
                        window = wide[p]
                    else:
                        window = jnp.where(lane < width, turned[p], turned[p + 1])
                    m = j % 4
                    if m < 3:
                        main[d][m] = window
                    else:
                        for n in range(3):
                            tail = pltpu.roll(window, LANES - spare * (n + 1), 1)
                            out_ref[d, k, q * (per_group // 4) + j // 4, n] = jnp.where(
                                lane < LANES - spare, main[d][n], tail
                            )
        return carry

    lax.fori_loop(0, layers // per_group, step, 0)


def unpack_kernel(edge_ref, got_ref, fields_ref, shared_ref):
    count, _, groups = got_ref.shape[:3]
    layers = 4 * groups
    spare = LANES // 4
    lane = lanes_of(SUBLANES)
    for d in range(count):
        rows = pl.ds(SUBLANES * d, SUBLANES)

        def step(g, total, d=d, rows=rows):
            for k in range(3):
                fill = 1.0 if k == 1 else 0.0
                held = [got_ref[d, k, g, n] for n in range(3)]
                last = jnp.where(
                    lane < spare,
                    pltpu.roll(held[0], spare, 1),
                    jnp.where(
                        lane < 2 * spare, pltpu.roll(held[1], 2 * spare, 1), pltpu.roll(held[2], 3 * spare, 1)
                    ),
                )
                for n, value in enumerate(held + [last]):
                    value = jnp.where(lane < LANES - spare, value, fill)
                    fields_ref[k, 4 * g + n, rows] = value
                    if k == 2:
                        total = total + value
            return total

        total = lax.fori_loop(0, groups, step, jnp.zeros((SUBLANES, LANES), jnp.float32), unroll=2)
        shared_ref[0, rows] = total / layers
        shared_ref[1, rows] = fields_ref[0, edge_ref[0], rows]


def two_sum(a, b):
    total = a + b
    part = total - a
    return total, (a - (total - part)) + (b - part)


def add_pairs(high, low, other_high, other_low):
    total, error = two_sum(high, other_high)
    return total, low + other_low + error


def stencil(held_ref, layer, rows):
    def at(shift):
        return held_ref[layer + 1, pl.ds(SUBLANES + shift, rows)]

    here = at(0)
    near = at(1) + at(-1)
    mixed = here + cross_weight * near
    far = at(2) + at(-2) + pltpu.roll(here, 2, 1) + pltpu.roll(here, LANES - 2, 1)
    beside = near + pltpu.roll(mixed, 1, 1) + pltpu.roll(mixed, LANES - 1, 1) + far_weight * far
    above = held_ref[layer + 2, pl.ds(SUBLANES, rows)] + held_ref[layer, pl.ds(SUBLANES, rows)]
    return beside + vertical_weight * above


def blocks(total, size, body):
    def step(g, carry):
        body(g * size)
        return carry

    lax.fori_loop(0, total // size, step, 0)


def krylov_kernel(edge_ref, fields_ref, got_ref, *refs):
    basis = refs[: ITERS + 1]
    scale_ref, sums_ref, even_ref, odd_ref, factor_ref, gram_ref = refs[ITERS + 1 :]
    held = (even_ref, odd_ref)
    layers, rows = fields_ref.shape[1:3]
    inner = pl.ds(SUBLANES, rows)
    empty = jnp.zeros((layers + 2, SUBLANES, LANES), jnp.float32)
    for ref in held:
        ref[:, :SUBLANES] = empty
        ref[:, SUBLANES + rows :] = empty
        ref[0] = jnp.zeros((rows + 2 * SUBLANES, LANES), jnp.float32)
        ref[layers + 1] = jnp.zeros((rows + 2 * SUBLANES, LANES), jnp.float32)

    def fill(first):
        for layer in range(8):
            even_ref[first + layer + 1, inner] = fields_ref[0, first + layer]

    blocks(layers, 8, fill)
    active = jnp.where(fields_ref[0, 0] > 0.0, 1.0, 0.0)
    term = active * got_ref[1] * got_ref[0]

    def begin(first):
        for layer in range(UNROLL):
            layer = first + layer
            coupling = fields_ref[0, layer]
            diagonal = fields_ref[1, layer] + coupling * stencil(even_ref, layer, rows)
            root = jnp.sqrt(diagonal)
            inverse = 1.0 / root
            factor = coupling * inverse
            source = fields_ref[2, layer] + term * jnp.where(layer == edge_ref[0], 1.0, 0.0)
            vector = source * inverse
            scale_ref[0, layer] = inverse
            scale_ref[1, layer] = root
            factor_ref[layer] = factor
            basis[0][layer] = vector
            odd_ref[layer + 1, inner] = factor * vector

    blocks(layers, UNROLL, begin)
    for k in range(ITERS):
        source_ref, target_ref = held[(k + 1) % 2], held[k % 2]

        def apply(first):
            for layer in range(UNROLL):
                layer = first + layer
                factor = factor_ref[layer]
                spread = stencil(source_ref, layer, rows)
                before = basis[k][layer]
                before = (1.0 - SHIFTS[k]) * before if SHIFTS[k] else before
                vector = before - factor * spread
                basis[k + 1][layer] = vector
                if k + 1 < ITERS:
                    target_ref[layer + 1, inner] = factor * vector

        blocks(layers, UNROLL, apply)

    lane = lanes_of(SUBLANES)
    half = LANES // 2
    gram_ref[...] = jnp.zeros(gram_ref.shape, jnp.float32)

    def products(first):
        sums = [None] * len(PAIRS)
        for n in range(0, 4, 2):
            for d in range(rows // SUBLANES):
                part = pl.ds(SUBLANES * d, SUBLANES)
                vectors = [
                    jnp.where(
                        lane < half,
                        pltpu.roll(ref[first + n, part], LANES - HALO, 1),
                        pltpu.roll(ref[first + n + 1, part], half - HALO, 1),
                    )
                    for ref in basis
                ]
                for p, (i, j) in enumerate(PAIRS):
                    product = vectors[j] * vectors[i]
                    sums[p] = product if sums[p] is None else sums[p] + product
        for p in range(len(PAIRS)):
            high, low = add_pairs(gram_ref[0, p], gram_ref[1, p], sums[p], 0.0)
            gram_ref[0, p] = high
            gram_ref[1, p] = low

    blocks(layers, 4, products)
    high, low = gram_ref[0, :, 0], gram_ref[1, :, 0]
    for row in range(1, SUBLANES):
        high, low = add_pairs(high, low, gram_ref[0, :, row], gram_ref[1, :, row])
    turn = LANES // 2
    while turn:
        high, low = add_pairs(high, low, pltpu.roll(high, turn, 1), pltpu.roll(low, turn, 1))
        turn //= 2
    packed = high[:SUBLANES]
    share = LANES // 4
    for g in range(4):
        part = slice(SUBLANES * g, SUBLANES * (g + 1))
        if g:
            packed = jnp.where(lane >= share * g, high[part], packed)
        packed = jnp.where((lane >= share * g + share // 2) & (lane < share * (g + 1)), low[part], packed)
    for d in range(sums_ref.shape[0]):
        sums_ref[d] = packed


def tree_sum(terms):
    while len(terms) > 1:
        terms = [sum(terms[i : i + 2]) for i in range(0, len(terms), 2)]
    return terms[0]


def quadratic(gram, left, right):
    products = []
    for i, a in enumerate(left):
        inside = [gram[max(i, j), min(i, j)] * b for j, b in enumerate(right)]
        products.append(a * tree_sum(inside))
    return tree_sum(products)


def iterate(gram):
    one = jnp.ones_like(gram[0, 0])
    zero = jnp.zeros_like(one)
    residual, direction, answer = [one], [one], []
    norm = gram[0, 0]
    for iteration in range(ITERS):
        applied = [SHIFTS[k] * c if SHIFTS[k] else zero for k, c in enumerate(direction)] + [zero]
        for k, c in enumerate(direction):
            applied[k + 1] = applied[k + 1] + c
        curve = quadratic(gram, direction, applied)
        step = norm / curve
        answer = [a + step * c for a, c in zip(answer + [zero], direction)]
        residual = [r - step * c for r, c in zip(residual + [zero], applied)]
        if iteration + 1 < ITERS:
            following = quadratic(gram, residual, residual)
            ratio = following / norm
            direction = [r + ratio * c for r, c in zip(residual, direction + [zero])]
            norm = following
    return answer, residual


def combine_kernel(sums_ref, *refs):
    basis = refs[: ITERS + 1]
    scale_ref, out_ref, gram_ref = refs[ITERS + 1 :]
    layers, rows = scale_ref.shape[1:3]
    share = LANES // 4
    parts = [(sums_ref[d], pltpu.roll(sums_ref[d], LANES - share // 2, 1)) for d in range(sums_ref.shape[0])]
    while len(parts) > 1:
        parts = [add_pairs(*parts[i], *parts[i + 1]) if i + 1 < len(parts) else parts[i] for i in range(0, len(parts), 2)]
    gram_ref[...] = parts[0][0] + parts[0][1]
    gram = {
        pair: gram_ref[pl.ds(p % SUBLANES, 1), pl.ds(share * (p // SUBLANES), 1)] for p, pair in enumerate(PAIRS)
    }
    answer, residual = iterate(gram)
    answer = [jnp.broadcast_to(c, (SUBLANES, LANES)) for c in answer]
    residual = [jnp.broadcast_to(c, (SUBLANES, LANES)) for c in residual]
    half = LANES // 2
    lane = lanes_of(SUBLANES)

    def mix(first):
        for layer in range(UNROLL):
            layer = first + layer
            for d in range(rows // SUBLANES):
                part = pl.ds(SUBLANES * d, SUBLANES)
                vectors = [ref[layer, part] for ref in basis]
                answered = tree_sum([c * v for c, v in zip(answer, vectors)]) * scale_ref[0, layer, part]
                left = tree_sum([c * v for c, v in zip(residual, vectors)]) * scale_ref[1, layer, part]
                out_ref[d, layer] = jnp.where(
                    lane < half, pltpu.roll(answered, LANES - HALO, 1), pltpu.roll(left, half - HALO, 1)
                )

    blocks(layers, UNROLL, mix)


def finish_kernel(got_ref, solution_ref, residual_ref):
    count, layers = got_ref.shape[:2]
    half = LANES // 2
    lane = lanes_of(SUBLANES)
    for layer in range(layers):
        for p in range(count // 2):
            left, right = got_ref[2 * p, layer], got_ref[2 * p + 1, layer]
            place = pl.ds(LANES * p, LANES)
            solution_ref[0, layer, :, place] = jnp.where(lane < half, left, pltpu.roll(right, half, 1))
            residual_ref[0, layer, :, place] = jnp.where(lane < half, pltpu.roll(left, half, 1), right)


def call(kernel, outs, specs, *args, scratch=(), limit=24):
    return pl.pallas_call(
        kernel,
        name=kernel.__name__,
        out_shape=[jax.ShapeDtypeStruct(shape, jnp.float32) for shape in outs],
        in_specs=[pl.BlockSpec(memory_space=pltpu.SMEM)] * specs
        + [pl.BlockSpec(memory_space=pltpu.VMEM)] * (len(args) - specs),
        out_specs=[pl.BlockSpec(memory_space=pltpu.VMEM)] * len(outs),
        scratch_shapes=[pltpu.VMEM(shape, jnp.float32) for shape in scratch],
        compiler_params=pltpu.CompilerParams(vmem_limit_bytes=limit * 2**20),
    )(*args)


def in_windows(forcing, conduct, diag_add, ice_mask, grounded):
    _, layers, block_x, block_y = forcing.shape
    count_x, count_y = lax.axis_size("gx"), lax.axis_size("gy")
    rows = count_x * block_x
    group = lax.axis_index("group").astype(jnp.int32)
    place = lax.axis_index("gy")
    edge = jnp.where(group == 0, 0, layers - 1).astype(jnp.int32)[None]
    inside = jnp.stack([place > 0, place < count_y - 1]).astype(jnp.float32)
    rim = (3, layers * HALO // LANES, block_x, LANES)
    fields, low, high = call(
        prepare_kernel, [(3, layers, block_x, block_y), rim, rim], 1,
        group[None], forcing, conduct, diag_add, ice_mask, grounded,
    )
    before = lax.ppermute(high, "gy", ring(count_y, 1))
    after = lax.ppermute(low, "gy", ring(count_y, -1))
    (packed,) = call(
        pack_kernel, [(count_x, 3, layers // 4, 3, block_x, LANES)], 1, inside, fields, before, after
    )
    got = lax.all_to_all(packed, "gx", 0, 0, tiled=True)
    windows, shared = call(
        unpack_kernel, [(3, layers, rows, LANES), (2, rows, LANES)], 1, edge, got
    )
    received = from_partner(shared, "group", 0)
    padded = rows + 2 * SUBLANES
    window = (layers, rows, LANES)
    *basis, scale, sums = call(
        krylov_kernel,
        [window] * (ITERS + 1) + [(2,) + window, (count_x * count_y, SUBLANES, LANES)],
        1, edge, windows, received,
        scratch=[(layers + 2, padded, LANES)] * 2 + [window, (2, 32, SUBLANES, LANES)],
        limit=32,
    )
    sums = lax.all_to_all(sums, ("gx", "gy"), 0, 0, tiled=True)
    (mixed,) = call(
        combine_kernel, [(count_x, layers, block_x, LANES)], 0, sums, *basis, scale,
        scratch=[(SUBLANES, LANES)],
    )
    mixed = lax.all_to_all(mixed, "gx", 0, 0, tiled=True)
    steps = 4
    part = pl.BlockSpec((1, layers // steps, block_x, block_y), lambda i: (0, i, 0, 0))
    return tuple(
        pl.pallas_call(
            finish_kernel,
            name="finish_kernel",
            grid=(steps,),
            out_shape=[jax.ShapeDtypeStruct(forcing.shape, jnp.float32)] * 2,
            in_specs=[pl.BlockSpec((count_x, layers // steps, block_x, LANES), lambda i: (0, i, 0, 0))],
            out_specs=[part, part],
            compiler_params=pltpu.CompilerParams(vmem_limit_bytes=24 * 2**20),
        )(mixed)
    )


def fits_windows(layers, block_x, block_y, count_x):
    width = block_y // count_x
    return (
        layers % (LANES // HALO) == 0
        and block_x == SUBLANES
        and block_y % LANES == 0
        and 2 * width == LANES
        and HALO >= 2 * (ITERS + 1)
    )


def per_device(forcing, conduct, diag_add, ice_mask, grounded):
    _, layers, block_x, block_y = forcing.shape
    way = in_windows if fits_windows(layers, block_x, block_y, lax.axis_size("gx")) else on_device
    return way(forcing, conduct, diag_add, ice_mask, grounded)


def solution(mesh):
    in_specs = (
        P("group", None, "gx", "gy"),
        P("group", None, "gx", "gy"),
        P("group", None, "gx", "gy"),
        P("gx", "gy"),
        P("gx", "gy"),
    )
    out_specs = (P("group", None, "gx", "gy"), P("group", None, "gx", "gy"))
    return jax.shard_map(
        per_device, mesh=mesh, in_specs=in_specs, out_specs=out_specs, check_vma=False
    )
```

```python
import math

import jax
import jax.numpy as jnp
from jax import lax
from jax.experimental import pallas as pl
from jax.experimental.pallas import tpu as pltpu
from jax.sharding import PartitionSpec as P

ITERS = 6
LANES = 128
SUBLANES = 8
HALO = 16
SHIFTS = (0.0, 0.75, 1.5, 0.25, 1.75, 1.0)
UNROLL = 16
PAIRS = tuple((i, j) for i in range(ITERS + 1) for j in range(i + 1) if j < ITERS)


far_weight = 0.25
cross_weight = 0.5
vertical_weight = 4.0
friction_gain = 8.0
NEIGHBOURS = (
    (1, 0, 1.0),
    (-1, 0, 1.0),
    (0, 1, 1.0),
    (0, -1, 1.0),
    (2, 0, far_weight),
    (-2, 0, far_weight),
    (0, 2, far_weight),
    (0, -2, far_weight),
    (1, 1, cross_weight),
    (1, -1, cross_weight),
    (-1, 1, cross_weight),
    (-1, -1, cross_weight),
)


def with_halo(block, sides, width):
    for axis, dim in sides:
        count = lax.axis_size(axis)
        place = lax.axis_index(axis)
        ahead = [(i, (i + 1) % count) for i in range(count)]
        back = [(target, source) for source, target in ahead]
        low = lax.ppermute(
            lax.slice_in_dim(block, block.shape[dim] - width, None, axis=dim), axis, ahead
        )
        high = lax.ppermute(lax.slice_in_dim(block, 0, width, axis=dim), axis, back)
        low = jnp.where(place > 0, low, 0.0)
        high = jnp.where(place < count - 1, high, 0.0)
        block = jnp.concatenate([low, block, high], axis=dim)
    return block


def from_partner(shard, axis, distance):
    return lax.ppermute(shard, axis, [(i, i ^ 1 << distance) for i in range(lax.axis_size(axis))])


def beside_sum(padded, extent_x, extent_y):
    summed = jnp.zeros((padded.shape[0], extent_x, extent_y), jnp.float32)
    for shift_x, shift_y, weight in NEIGHBOURS:
        summed = (
            summed
            + weight
            * padded[:, 2 + shift_x : 2 + shift_x + extent_x, 2 + shift_y : 2 + shift_y + extent_y]
        )
    return summed


def vertical_sum(values):
    zeroes = jnp.zeros_like(values[:1])
    return jnp.concatenate([values[1:], zeroes], 0) + jnp.concatenate([zeroes, values[:-1]], 0)


def spread_padded(padded, values):
    return beside_sum(padded, values.shape[1], values.shape[2]) + vertical_weight * vertical_sum(
        values
    )


def operate(vector, coupling, diagonal):
    scaled = coupling * vector
    padded = with_halo(scaled, (("gx", 1), ("gy", 2)), 2)
    return diagonal * vector - coupling * spread_padded(padded, scaled)


def sum_over(partial, axes):
    count = math.prod(lax.axis_size(axis) for axis in axes)
    sent = jnp.broadcast_to(partial[None, None], (count, 1) + partial.shape)
    return jnp.sum(lax.all_to_all(sent, axes, 0, 0, tiled=True), axis=(0, 1))


def paired_sums(residual, precond, applied):
    partial = jnp.stack([jnp.sum(residual * precond), jnp.sum(applied * precond)])
    summed = sum_over(partial, ("gx", "gy"))
    return summed[0], summed[1]


def on_device(forcing, conduct, diag_add, ice_mask, grounded):
    own_force = forcing[0]
    layers = own_force.shape[0]
    group_id = lax.axis_index("group")
    is_ice = (group_id == 0).astype(jnp.float32)
    ice_cells = ice_mask.astype(jnp.float32)
    ground_cells = grounded.astype(jnp.float32)
    active = ice_cells * (1.0 - (1.0 - is_ice) * ground_cells)
    coupling = jnp.sqrt(conduct[0].astype(jnp.float32)) * active
    layer_index = lax.broadcasted_iota(jnp.int32, (layers, 1, 1), 0)
    edge_layer = jnp.where(group_id == 0, 0, layers - 1).astype(jnp.int32)
    edge_pick = (layer_index == edge_layer).astype(jnp.float32)
    bottom = (layer_index == 0).astype(jnp.float32)
    base_diag = diag_add[0].astype(jnp.float32) + bottom * (
        is_ice * friction_gain * ground_cells * ice_cells
    )
    padded_coupling = with_halo(coupling, (("gx", 1), ("gy", 2)), 2)
    diagonal = base_diag + coupling * spread_padded(padded_coupling, coupling)
    shared_value = active * jnp.mean(own_force, axis=0)
    shared_weight = lax.dynamic_index_in_dim(coupling, edge_layer, 0, keepdims=False)
    received = from_partner(jnp.stack([shared_value, shared_weight]), "group", 0)
    source = active * own_force + edge_pick * (active * received[1] * received[0])
    inverse = 1.0 / diagonal
    solution = jnp.zeros_like(source)
    residual = source
    precond = inverse * residual
    applied = operate(precond, coupling, diagonal)
    norm_now, curve = paired_sums(residual, precond, applied)
    step_size = norm_now / curve
    direction = precond
    along = applied
    for iteration in range(ITERS):
        solution = solution + step_size * direction
        residual = residual - step_size * along
        if iteration + 1 < ITERS:
            precond = inverse * residual
            applied = operate(precond, coupling, diagonal)
            norm_next, curve = paired_sums(residual, precond, applied)
            step_ratio = norm_next / norm_now
            step_size = norm_next / (curve - step_ratio * norm_next / step_size)
            direction = precond + step_ratio * direction
            along = applied + step_ratio * along
            norm_now = norm_next
    return (solution[None], residual[None])


def ring(count, step):
    return [(i, (i + step) % count) for i in range(count)]


def lanes_of(rows):
    return lax.broadcasted_iota(jnp.int32, (rows, LANES), 1)


def blocks(total, size, body):
    def step(g, carry):
        body(g * size)
        return carry

    lax.fori_loop(0, total // size, step, 0)


def slots_of(rows):
    return lanes_of(rows) // HALO


RIGHT = tuple((4 + 2 * j) % 8 for j in range(4))
LEFT = tuple((7 + 2 * j) % 8 for j in range(4))


def turned(value, amount):
    return pltpu.roll(value, amount % LANES, 1) if amount % LANES else value


def by_partner(place, values):
    bit = 1
    while bit < len(values):
        swap = (place & bit) != 0
        values = [jnp.where(swap, values[d ^ bit], values[d]) for d in range(len(values))]
        bit *= 2
    return values


def prepare_kernel(where_ref, force_ref, conduct_ref, diag_ref, ice_ref, ground_ref, *refs):
    count = (len(refs) - 10) // 2
    own_refs, rim_refs = refs[:count], refs[count : 2 * count]
    low_ref, high_ref, force, conduct, diag, ice, ground, sems, small_sems, _ = refs[2 * count :]
    layers = force.shape[0]
    chunks = sems.shape[0]
    depth = layers // chunks
    small = [
        pltpu.make_async_copy(ice_ref, ice, small_sems.at[0]),
        pltpu.make_async_copy(ground_ref, ground, small_sems.at[1]),
    ]
    copies = []
    for copy in small:
        copy.start()
    for c in range(chunks):
        part = pl.ds(c * depth, depth)
        row = []
        for n, (source, target) in enumerate(((force_ref, force), (conduct_ref, conduct), (diag_ref, diag))):
            copy = pltpu.make_async_copy(source.at[0, part], target.at[part], sems.at[c, n])
            copy.start()
            row.append(copy)
        copies.append(row)
    place = where_ref[1]
    is_ice = jnp.where(where_ref[0] == 0, 1.0, 0.0)
    for copy in small:
        copy.wait()
    ice_cells = ice[...].astype(jnp.float32)
    ground_cells = ground[...].astype(jnp.float32)
    active = ice_cells * (1.0 - (1.0 - is_ice) * ground_cells)
    friction = is_ice * friction_gain * ground_cells * ice_cells
    lane = lanes_of(SUBLANES)
    slot = slots_of(SUBLANES)
    half = LANES // 2

    def step(q, carry):
        for k in range(3):
            low = high = None
            for group in range(2):
                rims = [None] * count
                pair = []
                for j in range(4):
                    layer = q * 8 + group * 4 + j
                    if k == 0:
                        value = jnp.sqrt(conduct[layer].astype(jnp.float32)) * active
                    elif k == 1:
                        value = diag[layer].astype(jnp.float32)
                        if group == 0 and j == 0:
                            value = value + friction * jnp.where(q == 0, 1.0, 0.0)
                    else:
                        value = active * force[layer]
                    pieces = [value[:, LANES * p : LANES * (p + 1)] for p in range(count // 2)]
                    halves = [turned(piece, half) for piece in pieces]
                    pair.append((pieces, halves))
                    even = halves if j == 2 else [turned(piece, 32 * j) for piece in pieces]
                    odd = halves if j == 0 else pieces if j == 2 else [turned(piece, half + 32 * j) for piece in pieces]
                    for d in range(count):
                        p = d // 2
                        sources = []
                        if d % 2 == 0:
                            sources.append((RIGHT[j], even[p]))
                            if d:
                                sources.append((LEFT[j], even[p - 1]))
                        else:
                            sources.append((LEFT[j], odd[p]))
                            if d + 1 < count:
                                sources.append((RIGHT[j], odd[p + 1]))
                        for target, source in sources:
                            rims[d] = source if rims[d] is None else jnp.where(slot == target, source, rims[d])
                    if group == 0:
                        first, last, first_slot, last_slot = odd[0], even[-1], RIGHT[j], LEFT[j]
                    else:
                        first, last = turned(pieces[0], 112 + 32 * j), turned(pieces[-1], 80 + 32 * j)
                        first_slot, last_slot = LEFT[j], RIGHT[j]
                    low = first if low is None else jnp.where(slot == first_slot, first, low)
                    high = last if high is None else jnp.where(slot == last_slot, last, high)
                    if j % 2:
                        (even_pieces, even_halves), (odd_pieces, odd_halves) = pair[-2:]
                        packed = []
                        for d in range(count):
                            p = d // 2
                            if d % 2 == 0:
                                packed.append(jnp.where(lane < half, even_pieces[p], odd_halves[p]))
                            else:
                                packed.append(jnp.where(lane < half, even_halves[p], odd_pieces[p]))
                        for ref, packed_value in zip(own_refs, by_partner(place, packed)):
                            ref[k, q * 4 + group * 2 + j // 2] = packed_value
                for ref, rim in zip(rim_refs, by_partner(place, rims)):
                    ref[k, q * 2 + group] = rim
            low_ref[k, q] = low
            high_ref[k, q] = high
        return carry

    for c in range(chunks):
        for copy in copies[c]:
            copy.wait()
        lax.fori_loop(c * depth // 8, (c + 1) * depth // 8, step, 0)


def rims_kernel(place_ref, edge_ref, low_ref, high_ref, *refs):
    count = len(refs) // 2
    groups = low_ref.shape[1]
    odd = slots_of(SUBLANES) % 2 == 1
    first = [jnp.where(odd, place_ref[0], -1) == k for k in range(count)]
    last = [jnp.where(odd, -1, place_ref[0] ^ (count - 1)) == k for k in range(count)]

    def step(q):
        for k in range(3):
            before, after = low_ref[k, q], high_ref[k, q]
            if k == 0:
                before, after = before * edge_ref[0], after * edge_ref[1]
            befores, afters = (before, turned(before, 48)), (after, turned(after, 80))
            for n in range(count):
                for group in range(2):
                    rim = refs[n][k, 2 * q + group]
                    rim = jnp.where(first[n], befores[group], rim)
                    refs[count + n][k, 2 * q + group] = jnp.where(last[n], afters[group], rim)

    def pair(start):
        step(start)
        step(start + 1)

    blocks(groups, 2, pair)


def assemble_kernel(where_ref, *refs):
    count = (len(refs) - 2) // 2
    own_refs, rim_refs = refs[:count], refs[count : 2 * count]
    fields_ref, shared_ref = refs[2 * count :]
    groups = rim_refs[0].shape[1]
    lane = lanes_of(SUBLANES)
    half = LANES // 2
    inside = (lane < half + HALO) | (lane >= LANES - HALO)
    rows = [pl.ds(pl.multiple_of(SUBLANES * (where_ref[1] ^ n), SUBLANES), SUBLANES) for n in range(count)]

    def step(i, totals):
        totals = list(totals)
        for u in range(2):
            g = 2 * i + u
            for k in range(3):
                fill = 1.0 if k == 1 else 0.0
                for n in range(count):
                    rim = rim_refs[n][k, g]
                    for pair in range(2):
                        packed = own_refs[n][k, 2 * g + pair]
                        for own, j in ((packed, 2 * pair), (turned(packed, half), 2 * pair + 1)):
                            value = jnp.where(lane < half, own, jnp.where(inside, turned(rim, -32 * j), fill))
                            fields_ref[k, 4 * g + j, rows[n]] = value
                            if k == 2:
                                totals[n] = totals[n] + value
        return tuple(totals)

    zero = jnp.zeros((SUBLANES, LANES), jnp.float32)
    totals = lax.fori_loop(0, groups // 2, step, (zero,) * count)
    for n in range(count):
        shared_ref[0, rows[n]] = totals[n] / (4 * groups)
        shared_ref[1, rows[n]] = fields_ref[0, where_ref[0], rows[n]]


def two_sum(a, b):
    total = a + b
    part = total - a
    return total, (a - (total - part)) + (b - part)


def add_pairs(high, low, other_high, other_low):
    total, error = two_sum(high, other_high)
    return total, low + other_low + error


def stencil(held_ref, layer, rows):
    def at(shift):
        return held_ref[layer + 1, pl.ds(SUBLANES + shift, rows)]

    here = at(0)
    near = at(1) + at(-1)
    mixed = here + cross_weight * near
    far = at(2) + at(-2) + pltpu.roll(here, 2, 1) + pltpu.roll(here, LANES - 2, 1)
    beside = near + pltpu.roll(mixed, 1, 1) + pltpu.roll(mixed, LANES - 1, 1) + far_weight * far
    above = held_ref[layer + 2, pl.ds(SUBLANES, rows)] + held_ref[layer, pl.ds(SUBLANES, rows)]
    return beside + vertical_weight * above


def scale_kernel(fields_ref, scale_ref, factor_ref, held_ref):
    layers, rows = fields_ref.shape[1:3]
    inner = pl.ds(SUBLANES, rows)
    clear_edges(held_ref, rows)

    def fill(first):
        for layer in range(UNROLL):
            held_ref[first + layer + 1, inner] = fields_ref[0, first + layer]

    blocks(layers, UNROLL, fill)

    def begin(first):
        for layer in range(UNROLL):
            layer = first + layer
            coupling = fields_ref[0, layer]
            diagonal = fields_ref[1, layer] + coupling * stencil(held_ref, layer, rows)
            root = jnp.sqrt(diagonal)
            inverse = 1.0 / root
            scale_ref[0, layer] = inverse
            scale_ref[1, layer] = root
            factor_ref[layer] = coupling * inverse

    blocks(layers, UNROLL, begin)


def clear_edges(ref, rows):
    layers = ref.shape[0]
    empty = jnp.zeros((layers, SUBLANES, LANES), jnp.float32)
    ref[:, :SUBLANES] = empty
    ref[:, SUBLANES + rows :] = empty
    ref[0] = jnp.zeros((rows + 2 * SUBLANES, LANES), jnp.float32)
    ref[layers - 1] = jnp.zeros((rows + 2 * SUBLANES, LANES), jnp.float32)


def krylov_kernel(edge_ref, fields_ref, got_ref, scale_ref, factor_ref, *refs):
    basis = refs[: ITERS + 1]
    sums_ref, even_ref, odd_ref, gram_ref = refs[ITERS + 1 :]
    held = (even_ref, odd_ref)
    layers, rows = fields_ref.shape[1:3]
    inner = pl.ds(SUBLANES, rows)
    for ref in held:
        clear_edges(ref, rows)
    active = jnp.where(fields_ref[0, 0] > 0.0, 1.0, 0.0)
    term = active * got_ref[1] * got_ref[0]

    def begin(first):
        for layer in range(UNROLL):
            layer = first + layer
            source = fields_ref[2, layer] + term * jnp.where(layer == edge_ref[0], 1.0, 0.0)
            vector = source * scale_ref[0, layer]
            basis[0][layer] = vector
            odd_ref[layer + 1, inner] = factor_ref[layer] * vector

    blocks(layers, UNROLL, begin)
    for k in range(ITERS):
        source_ref, target_ref = held[(k + 1) % 2], held[k % 2]

        def apply(first):
            for layer in range(UNROLL):
                layer = first + layer
                factor = factor_ref[layer]
                spread = stencil(source_ref, layer, rows)
                before = basis[k][layer]
                before = (1.0 - SHIFTS[k]) * before if SHIFTS[k] else before
                vector = before - factor * spread
                basis[k + 1][layer] = vector
                if k + 1 < ITERS:
                    target_ref[layer + 1, inner] = factor * vector

        blocks(layers, UNROLL, apply)

    lane = lanes_of(SUBLANES)
    half = LANES // 2
    gram_ref[...] = jnp.zeros(gram_ref.shape, jnp.float32)

    def products(first):
        sums = [None] * len(PAIRS)
        for n in range(0, 8, 2):
            for d in range(rows // SUBLANES):
                part = pl.ds(SUBLANES * d, SUBLANES)
                vectors = [
                    jnp.where(lane < half, ref[first + n, part], turned(ref[first + n + 1, part], half))
                    for ref in basis
                ]
                for p, (i, j) in enumerate(PAIRS):
                    product = vectors[j] * vectors[i]
                    sums[p] = product if sums[p] is None else sums[p] + product
        for p in range(len(PAIRS)):
            high, low = add_pairs(gram_ref[0, p], gram_ref[1, p], sums[p], 0.0)
            gram_ref[0, p] = high
            gram_ref[1, p] = low

    blocks(layers, 8, products)
    high, low = gram_ref[0, :, 0], gram_ref[1, :, 0]
    for row in range(1, SUBLANES):
        high, low = add_pairs(high, low, gram_ref[0, :, row], gram_ref[1, :, row])
    turn = LANES // 2
    while turn:
        high, low = add_pairs(high, low, pltpu.roll(high, turn, 1), pltpu.roll(low, turn, 1))
        turn //= 2
    packed = high[:SUBLANES]
    share = LANES // 4
    for g in range(4):
        part = slice(SUBLANES * g, SUBLANES * (g + 1))
        if g:
            packed = jnp.where(lane >= share * g, high[part], packed)
        packed = jnp.where((lane >= share * g + share // 2) & (lane < share * (g + 1)), low[part], packed)
    for d in range(sums_ref.shape[0]):
        sums_ref[d] = packed


def tree_sum(terms):
    while len(terms) > 1:
        terms = [sum(terms[i : i + 2]) for i in range(0, len(terms), 2)]
    return terms[0]


def quadratic(gram, left, right):
    products = []
    for i, a in enumerate(left):
        inside = [gram[max(i, j), min(i, j)] * b for j, b in enumerate(right)]
        products.append(a * tree_sum(inside))
    return tree_sum(products)


def iterate(gram):
    one = jnp.ones_like(gram[0, 0])
    zero = jnp.zeros_like(one)
    residual, direction, answer = [one], [one], []
    norm = gram[0, 0]
    for iteration in range(ITERS):
        applied = [SHIFTS[k] * c if SHIFTS[k] else zero for k, c in enumerate(direction)] + [zero]
        for k, c in enumerate(direction):
            applied[k + 1] = applied[k + 1] + c
        curve = quadratic(gram, direction, applied)
        step = norm / curve
        answer = [a + step * c for a, c in zip(answer + [zero], direction)]
        residual = [r - step * c for r, c in zip(residual + [zero], applied)]
        if iteration + 1 < ITERS:
            following = quadratic(gram, residual, residual)
            ratio = following / norm
            direction = [r + ratio * c for r, c in zip(residual, direction + [zero])]
            norm = following
    return answer, residual


def combine_kernel(sums_ref, *refs):
    basis = refs[: ITERS + 1]
    scale_ref, out_ref, gram_ref = refs[ITERS + 1 :]
    layers, rows = scale_ref.shape[1:3]
    share = LANES // 4
    parts = [(sums_ref[d], pltpu.roll(sums_ref[d], LANES - share // 2, 1)) for d in range(sums_ref.shape[0])]
    while len(parts) > 1:
        parts = [add_pairs(*parts[i], *parts[i + 1]) if i + 1 < len(parts) else parts[i] for i in range(0, len(parts), 2)]
    gram_ref[...] = parts[0][0] + parts[0][1]
    gram = {
        pair: gram_ref[pl.ds(p % SUBLANES, 1), pl.ds(share * (p // SUBLANES), 1)] for p, pair in enumerate(PAIRS)
    }
    answer, residual = iterate(gram)
    answer = [jnp.broadcast_to(c, (SUBLANES, LANES)) for c in answer]
    residual = [jnp.broadcast_to(c, (SUBLANES, LANES)) for c in residual]
    half = LANES // 2
    lane = lanes_of(SUBLANES)

    def mix(first):
        for layer in range(UNROLL):
            layer = first + layer
            for d in range(rows // SUBLANES):
                part = pl.ds(SUBLANES * d, SUBLANES)
                vectors = [ref[layer, part] for ref in basis]
                answered = tree_sum([c * v for c, v in zip(answer, vectors)]) * scale_ref[0, layer, part]
                left = tree_sum([c * v for c, v in zip(residual, vectors)]) * scale_ref[1, layer, part]
                out_ref[d, layer] = jnp.where(lane < half, answered, turned(left, half))

    blocks(layers, UNROLL, mix)


def finish_kernel(got_ref, solution_ref, residual_ref):
    count, layers = got_ref.shape[:2]
    half = LANES // 2
    lane = lanes_of(SUBLANES)
    for layer in range(layers):
        for p in range(count // 2):
            left, right = got_ref[2 * p, layer], got_ref[2 * p + 1, layer]
            place = pl.ds(LANES * p, LANES)
            solution_ref[0, layer, :, place] = jnp.where(lane < half, left, pltpu.roll(right, half, 1))
            residual_ref[0, layer, :, place] = jnp.where(lane < half, pltpu.roll(left, half, 1), right)


def call(kernel, outs, specs, *args, scratch=(), limit=24, flops=10**6, apart=0):
    return pl.pallas_call(
        kernel,
        name=kernel.__name__,
        out_shape=[jax.ShapeDtypeStruct(shape, jnp.float32) for shape in outs],
        in_specs=[pl.BlockSpec(memory_space=pltpu.SMEM)] * specs
        + [pl.BlockSpec(memory_space=pl.ANY)] * apart
        + [pl.BlockSpec(memory_space=pltpu.VMEM)] * (len(args) - specs - apart),
        out_specs=[pl.BlockSpec(memory_space=pltpu.VMEM)] * len(outs),
        scratch_shapes=[pltpu.VMEM(shape, jnp.float32) if isinstance(shape, tuple) else shape for shape in scratch],
        compiler_params=pltpu.CompilerParams(vmem_limit_bytes=limit * 2**20),
        cost_estimate=pl.CostEstimate(flops=flops, bytes_accessed=0, transcendentals=0),
    )(*args)


def exchanged(parts):
    count = len(parts)
    return [parts[0]] + [
        lax.ppermute(parts[k], "gx", [(i, i ^ k) for i in range(count)]) for k in range(1, count)
    ]


def in_windows(forcing, conduct, diag_add, ice_mask, grounded):
    _, layers, block_x, block_y = forcing.shape
    count_x, count_y = lax.axis_size("gx"), lax.axis_size("gy")
    rows = count_x * block_x
    group = lax.axis_index("group").astype(jnp.int32)
    place_x = lax.axis_index("gx").astype(jnp.int32)
    place_y = lax.axis_index("gy")
    edge = jnp.where(group == 0, 0, layers - 1).astype(jnp.int32)
    inside = jnp.stack([place_y > 0, place_y < count_y - 1]).astype(jnp.float32)
    own = (3, layers // 2, block_x, LANES)
    rim = (3, layers // 4, block_x, LANES)
    side = (3, layers // 8, block_x, LANES)
    block = (layers, block_x, block_y)
    chunks = 5 if layers % 40 == 0 else 1
    *made, low, high = call(
        prepare_kernel, [own] * count_x + [rim] * count_x + [side] * 2, 1,
        jnp.stack([group, place_x]), forcing, conduct, diag_add, ice_mask, grounded,
        scratch=[
            block,
            pltpu.VMEM(block, conduct.dtype),
            pltpu.VMEM(block, diag_add.dtype),
            pltpu.VMEM(ice_mask.shape, ice_mask.dtype),
            pltpu.VMEM(grounded.shape, grounded.dtype),
            pltpu.SemaphoreType.DMA((chunks, 3)),
            pltpu.SemaphoreType.DMA((2,)),
            (SUBLANES, LANES),
        ],
        apart=5,
    )
    before = lax.ppermute(high, "gy", ring(count_y, 1))
    after = lax.ppermute(low, "gy", ring(count_y, -1))
    owns = exchanged(made[:count_x])
    rims = call(
        rims_kernel, [rim] * count_x, 2, place_x[None], inside, before, after, *made[count_x:]
    )
    rims = exchanged(rims)
    windows, shared = call(
        assemble_kernel, [(3, layers, rows, LANES), (2, rows, LANES)], 1,
        jnp.stack([edge, place_x]), *owns, *rims,
    )
    received = from_partner(shared, "group", 0)
    padded = (layers + 2, rows + 2 * SUBLANES, LANES)
    window = (layers, rows, LANES)
    scale, factor = call(scale_kernel, [(2,) + window, window], 0, windows, scratch=[padded], flops=4 * 10**7)
    *basis, sums = call(
        krylov_kernel,
        [window] * (ITERS + 1) + [(count_x * count_y, SUBLANES, LANES)],
        1, edge[None], windows, received, scale, factor,
        scratch=[padded] * 2 + [(2, 32, SUBLANES, LANES)],
        limit=32,
    )
    sums = lax.all_to_all(sums, ("gx", "gy"), 0, 0, tiled=True)
    (mixed,) = call(
        combine_kernel, [(count_x, layers, block_x, LANES)], 0, sums, *basis, scale,
        scratch=[(SUBLANES, LANES)],
    )
    mixed = lax.all_to_all(mixed, "gx", 0, 0, tiled=True)
    steps = 4
    part = pl.BlockSpec((1, layers // steps, block_x, block_y), lambda i: (0, i, 0, 0))
    return tuple(
        pl.pallas_call(
            finish_kernel,
            name="finish_kernel",
            grid=(steps,),
            out_shape=[jax.ShapeDtypeStruct(forcing.shape, jnp.float32)] * 2,
            in_specs=[pl.BlockSpec((count_x, layers // steps, block_x, LANES), lambda i: (0, i, 0, 0))],
            out_specs=[part, part],
            compiler_params=pltpu.CompilerParams(vmem_limit_bytes=24 * 2**20),
        )(mixed)
    )


def fits_windows(layers, block_x, block_y, count_x):
    width = block_y // count_x
    return (
        layers % (LANES // HALO) == 0
        and block_x == SUBLANES
        and block_y % LANES == 0
        and 2 * width == LANES
        and HALO >= 2 * (ITERS + 1)
    )


def per_device(forcing, conduct, diag_add, ice_mask, grounded):
    _, layers, block_x, block_y = forcing.shape
    way = in_windows if fits_windows(layers, block_x, block_y, lax.axis_size("gx")) else on_device
    return way(forcing, conduct, diag_add, ice_mask, grounded)


def solution(mesh):
    in_specs = (
        P("group", None, "gx", "gy"),
        P("group", None, "gx", "gy"),
        P("group", None, "gx", "gy"),
        P("gx", "gy"),
        P("gx", "gy"),
    )
    out_specs = (P("group", None, "gx", "gy"), P("group", None, "gx", "gy"))
    return jax.shard_map(
        per_device, mesh=mesh, in_specs=in_specs, out_specs=out_specs, check_vma=False
    )
```

```python
import functools
import math

import jax
import jax.numpy as jnp
from jax import lax
from jax.experimental import pallas as pl
from jax.experimental.pallas import tpu as pltpu
from jax.sharding import PartitionSpec as P


ITERS = 6
LANES = 128
SUBLANES = 8
HALO = 16
SHIFTS = (0.0, 0.75, 1.5, 0.25, 1.75, 1.0)
UNROLL = 16
PARTS = 2
PAIRS = tuple((i, j) for i in range(ITERS + 1) for j in range(i + 1) if j < ITERS)


far_weight = 0.25
cross_weight = 0.5
vertical_weight = 4.0
friction_gain = 8.0
NEIGHBOURS = (
    (1, 0, 1.0),
    (-1, 0, 1.0),
    (0, 1, 1.0),
    (0, -1, 1.0),
    (2, 0, far_weight),
    (-2, 0, far_weight),
    (0, 2, far_weight),
    (0, -2, far_weight),
    (1, 1, cross_weight),
    (1, -1, cross_weight),
    (-1, 1, cross_weight),
    (-1, -1, cross_weight),
)


def with_halo(block, sides, width):
    for axis, dim in sides:
        count = lax.axis_size(axis)
        place = lax.axis_index(axis)
        ahead = [(i, (i + 1) % count) for i in range(count)]
        back = [(target, source) for source, target in ahead]
        low = lax.ppermute(
            lax.slice_in_dim(block, block.shape[dim] - width, None, axis=dim), axis, ahead
        )
        high = lax.ppermute(lax.slice_in_dim(block, 0, width, axis=dim), axis, back)
        low = jnp.where(place > 0, low, 0.0)
        high = jnp.where(place < count - 1, high, 0.0)
        block = jnp.concatenate([low, block, high], axis=dim)
    return block


def from_partner(shard, axis, distance):
    return lax.ppermute(shard, axis, [(i, i ^ 1 << distance) for i in range(lax.axis_size(axis))])


def beside_sum(padded, extent_x, extent_y):
    summed = jnp.zeros((padded.shape[0], extent_x, extent_y), jnp.float32)
    for shift_x, shift_y, weight in NEIGHBOURS:
        summed = (
            summed
            + weight
            * padded[:, 2 + shift_x : 2 + shift_x + extent_x, 2 + shift_y : 2 + shift_y + extent_y]
        )
    return summed


def vertical_sum(values):
    zeroes = jnp.zeros_like(values[:1])
    return jnp.concatenate([values[1:], zeroes], 0) + jnp.concatenate([zeroes, values[:-1]], 0)


def spread_padded(padded, values):
    return beside_sum(padded, values.shape[1], values.shape[2]) + vertical_weight * vertical_sum(
        values
    )


def operate(vector, coupling, diagonal):
    scaled = coupling * vector
    padded = with_halo(scaled, (("gx", 1), ("gy", 2)), 2)
    return diagonal * vector - coupling * spread_padded(padded, scaled)


def sum_over(partial, axes):
    count = math.prod(lax.axis_size(axis) for axis in axes)
    sent = jnp.broadcast_to(partial[None, None], (count, 1) + partial.shape)
    return jnp.sum(lax.all_to_all(sent, axes, 0, 0, tiled=True), axis=(0, 1))


def paired_sums(residual, precond, applied):
    partial = jnp.stack([jnp.sum(residual * precond), jnp.sum(applied * precond)])
    summed = sum_over(partial, ("gx", "gy"))
    return summed[0], summed[1]


def on_device(forcing, conduct, diag_add, ice_mask, grounded):
    own_force = forcing[0]
    layers = own_force.shape[0]
    group_id = lax.axis_index("group")
    is_ice = (group_id == 0).astype(jnp.float32)
    ice_cells = ice_mask.astype(jnp.float32)
    ground_cells = grounded.astype(jnp.float32)
    active = ice_cells * (1.0 - (1.0 - is_ice) * ground_cells)
    coupling = jnp.sqrt(conduct[0].astype(jnp.float32)) * active
    layer_index = lax.broadcasted_iota(jnp.int32, (layers, 1, 1), 0)
    edge_layer = jnp.where(group_id == 0, 0, layers - 1).astype(jnp.int32)
    edge_pick = (layer_index == edge_layer).astype(jnp.float32)
    bottom = (layer_index == 0).astype(jnp.float32)
    base_diag = diag_add[0].astype(jnp.float32) + bottom * (
        is_ice * friction_gain * ground_cells * ice_cells
    )
    padded_coupling = with_halo(coupling, (("gx", 1), ("gy", 2)), 2)
    diagonal = base_diag + coupling * spread_padded(padded_coupling, coupling)
    shared_value = active * jnp.mean(own_force, axis=0)
    shared_weight = lax.dynamic_index_in_dim(coupling, edge_layer, 0, keepdims=False)
    received = from_partner(jnp.stack([shared_value, shared_weight]), "group", 0)
    source = active * own_force + edge_pick * (active * received[1] * received[0])
    inverse = 1.0 / diagonal
    solution = jnp.zeros_like(source)
    residual = source
    precond = inverse * residual
    applied = operate(precond, coupling, diagonal)
    norm_now, curve = paired_sums(residual, precond, applied)
    step_size = norm_now / curve
    direction = precond
    along = applied
    for iteration in range(ITERS):
        solution = solution + step_size * direction
        residual = residual - step_size * along
        if iteration + 1 < ITERS:
            precond = inverse * residual
            applied = operate(precond, coupling, diagonal)
            norm_next, curve = paired_sums(residual, precond, applied)
            step_ratio = norm_next / norm_now
            step_size = norm_next / (curve - step_ratio * norm_next / step_size)
            direction = precond + step_ratio * direction
            along = applied + step_ratio * along
            norm_now = norm_next
    return (solution[None], residual[None])


def ring(count, step):
    return [(i, (i + step) % count) for i in range(count)]


def lanes_of(rows):
    return lax.broadcasted_iota(jnp.int32, (rows, LANES), 1)


def blocks(total, size, body):
    def step(g, carry):
        body(g * size)
        return carry

    lax.fori_loop(0, total // size, step, 0)


def slots_of(rows):
    return lanes_of(rows) // HALO


RIGHT = tuple((4 + 2 * j) % 8 for j in range(4))
LEFT = tuple((7 + 2 * j) % 8 for j in range(4))


def turned(value, amount):
    return pltpu.roll(value, amount % LANES, 1) if amount % LANES else value


def by_partner(place, values):
    bit = 1
    while bit < len(values):
        swap = (place & bit) != 0
        values = [jnp.where(swap, values[d ^ bit], values[d]) for d in range(len(values))]
        bit *= 2
    return values


def partner_rows(place, count):
    return [pl.ds(pl.multiple_of(SUBLANES * (place ^ n), SUBLANES), SUBLANES) for n in range(count)]


def prepare_kernel(where_ref, force_ref, conduct_ref, diag_ref, ice_ref, ground_ref, *refs):
    count = (len(refs) - 10) // 2
    own_refs, rim_refs = refs[:count], refs[count : 2 * count]
    low_ref, high_ref, force, conduct, diag, ice, ground, sems, small_sems, _ = refs[2 * count :]
    layers = force.shape[0]
    chunks = sems.shape[0]
    depth = layers // chunks
    small = [
        pltpu.make_async_copy(ice_ref, ice, small_sems.at[0]),
        pltpu.make_async_copy(ground_ref, ground, small_sems.at[1]),
    ]
    copies = []
    for copy in small:
        copy.start()
    for c in range(chunks):
        part = pl.ds(c * depth, depth)
        row = []
        for n, (source, target) in enumerate(((force_ref, force), (conduct_ref, conduct), (diag_ref, diag))):
            copy = pltpu.make_async_copy(source.at[0, part], target.at[part], sems.at[c, n])
            copy.start()
            row.append(copy)
        copies.append(row)
    place = where_ref[1]
    is_ice = jnp.where(where_ref[0] == 0, 1.0, 0.0)
    for copy in small:
        copy.wait()
    ice_cells = ice[...].astype(jnp.float32)
    ground_cells = ground[...].astype(jnp.float32)
    active = ice_cells * (1.0 - (1.0 - is_ice) * ground_cells)
    friction = is_ice * friction_gain * ground_cells * ice_cells
    lane = lanes_of(SUBLANES)
    slot = slots_of(SUBLANES)
    half = LANES // 2

    def step(q, carry):
        for k in range(3):
            low = high = None
            for group in range(2):
                rims = [None] * count
                pair = []
                for j in range(4):
                    layer = q * 8 + group * 4 + j
                    if k == 0:
                        value = jnp.sqrt(conduct[layer].astype(jnp.float32)) * active
                    elif k == 1:
                        value = diag[layer].astype(jnp.float32)
                        if group == 0 and j == 0:
                            value = value + friction * jnp.where(q == 0, 1.0, 0.0)
                    else:
                        value = active * force[layer]
                    pieces = [value[:, LANES * p : LANES * (p + 1)] for p in range(count // 2)]
                    halves = [turned(piece, half) for piece in pieces]
                    pair.append((pieces, halves))
                    even = halves if j == 2 else [turned(piece, 32 * j) for piece in pieces]
                    odd = halves if j == 0 else pieces if j == 2 else [turned(piece, half + 32 * j) for piece in pieces]
                    for d in range(count):
                        p = d // 2
                        sources = []
                        if d % 2 == 0:
                            sources.append((RIGHT[j], even[p]))
                            if d:
                                sources.append((LEFT[j], even[p - 1]))
                        else:
                            sources.append((LEFT[j], odd[p]))
                            if d + 1 < count:
                                sources.append((RIGHT[j], odd[p + 1]))
                        for target, source in sources:
                            rims[d] = source if rims[d] is None else jnp.where(slot == target, source, rims[d])
                    if group == 0:
                        first, last, first_slot, last_slot = odd[0], even[-1], RIGHT[j], LEFT[j]
                    else:
                        first, last = turned(pieces[0], 112 + 32 * j), turned(pieces[-1], 80 + 32 * j)
                        first_slot, last_slot = LEFT[j], RIGHT[j]
                    low = first if low is None else jnp.where(slot == first_slot, first, low)
                    high = last if high is None else jnp.where(slot == last_slot, last, high)
                    if j % 2:
                        (even_pieces, even_halves), (odd_pieces, odd_halves) = pair[-2:]
                        packed = []
                        for d in range(count):
                            p = d // 2
                            if d % 2 == 0:
                                packed.append(jnp.where(lane < half, even_pieces[p], odd_halves[p]))
                            else:
                                packed.append(jnp.where(lane < half, even_halves[p], odd_pieces[p]))
                        for ref, packed_value in zip(own_refs, by_partner(place, packed)):
                            ref[k, q * 4 + group * 2 + j // 2] = packed_value
                for ref, rim in zip(rim_refs, by_partner(place, rims)):
                    ref[k, q * 2 + group] = rim
            low_ref[k, q] = low
            high_ref[k, q] = high
        return carry

    for c in range(chunks):
        for copy in copies[c]:
            copy.wait()
        lax.fori_loop(c * depth // 8, (c + 1) * depth // 8, step, 0)


def rims_kernel(place_ref, edge_ref, low_ref, high_ref, *refs):
    count = len(refs) // 2
    groups = low_ref.shape[1]
    odd = slots_of(SUBLANES) % 2 == 1
    first = [jnp.where(odd, place_ref[0], -1) == k for k in range(count)]
    last = [jnp.where(odd, -1, place_ref[0] ^ (count - 1)) == k for k in range(count)]

    def step(q):
        for k in range(3):
            before, after = low_ref[k, q], high_ref[k, q]
            if k == 0:
                before, after = before * edge_ref[0], after * edge_ref[1]
            befores, afters = (before, turned(before, 48)), (after, turned(after, 80))
            for n in range(count):
                for group in range(2):
                    rim = refs[n][k, 2 * q + group]
                    rim = jnp.where(first[n], befores[group], rim)
                    refs[count + n][k, 2 * q + group] = jnp.where(last[n], afters[group], rim)

    def pair(start):
        step(start)
        step(start + 1)

    blocks(groups, 2, pair)


def assemble_kernel(where_ref, *refs):
    count = (len(refs) - 2) // 2
    own_refs, rim_refs = refs[:count], refs[count : 2 * count]
    fields_ref, shared_ref = refs[2 * count :]
    groups = rim_refs[0].shape[1]
    lane = lanes_of(SUBLANES)
    half = LANES // 2
    inside = (lane < half + HALO) | (lane >= LANES - HALO)
    rows = partner_rows(where_ref[1], count)

    def step(i, totals):
        totals = list(totals)
        for u in range(2):
            g = 2 * i + u
            for k in range(3):
                fill = 1.0 if k == 1 else 0.0
                for n in range(count):
                    rim = rim_refs[n][k, g]
                    for pair in range(2):
                        packed = own_refs[n][k, 2 * g + pair]
                        for own, j in ((packed, 2 * pair), (turned(packed, half), 2 * pair + 1)):
                            value = jnp.where(lane < half, own, jnp.where(inside, turned(rim, -32 * j), fill))
                            fields_ref[k, 4 * g + j, rows[n]] = value
                            if k == 2:
                                totals[n] = totals[n] + value
        return tuple(totals)

    zero = jnp.zeros((SUBLANES, LANES), jnp.float32)
    totals = lax.fori_loop(0, groups // 2, step, (zero,) * count)
    for n in range(count):
        shared_ref[0, rows[n]] = totals[n] / (4 * groups)
        shared_ref[1, rows[n]] = fields_ref[0, where_ref[0], rows[n]]


def two_sum(a, b):
    total = a + b
    part = total - a
    return total, (a - (total - part)) + (b - part)


def add_pairs(high, low, other_high, other_low):
    total, error = two_sum(high, other_high)
    return total, low + other_low + error


def stencil(held_ref, layer, rows):
    def at(shift):
        return held_ref[layer + 1, pl.ds(SUBLANES + shift, rows)]

    here = at(0)
    near = at(1) + at(-1)
    mixed = here + cross_weight * near
    wide = turned(mixed, 1) + far_weight * (here + turned(here, 2))
    far = at(2) + at(-2) - 2.0 * here
    above = held_ref[layer + 2, pl.ds(SUBLANES, rows)] + held_ref[layer, pl.ds(SUBLANES, rows)]
    flat = near + far_weight * far + vertical_weight * above
    return (flat + wide) + turned(wide, -2)


def scale_kernel(fields_ref, scale_ref, factor_ref, held_ref):
    layers, rows = fields_ref.shape[1:3]
    inner = pl.ds(SUBLANES, rows)
    clear_edges(held_ref, rows)

    def fill(first):
        for layer in range(UNROLL):
            held_ref[first + layer + 1, inner] = fields_ref[0, first + layer]

    blocks(layers, UNROLL, fill)

    def begin(first):
        for layer in range(UNROLL):
            layer = first + layer
            coupling = fields_ref[0, layer]
            diagonal = fields_ref[1, layer] + coupling * stencil(held_ref, layer, rows)
            root = jnp.sqrt(diagonal)
            inverse = 1.0 / root
            scale_ref[0, layer] = inverse
            scale_ref[1, layer] = root
            factor_ref[layer] = coupling * inverse

    blocks(layers, UNROLL, begin)


def clear_edges(ref, rows):
    layers = ref.shape[0]
    empty = jnp.zeros((layers, SUBLANES, LANES), jnp.float32)
    ref[:, :SUBLANES] = empty
    ref[:, SUBLANES + rows :] = empty
    ref[0] = jnp.zeros((rows + 2 * SUBLANES, LANES), jnp.float32)
    ref[layers - 1] = jnp.zeros((rows + 2 * SUBLANES, LANES), jnp.float32)


def krylov_kernel(edge_ref, fields_ref, got_ref, scale_ref, factor_ref, *refs):
    basis = refs[: ITERS + 1]
    sums_ref, even_ref, odd_ref, gram_ref = refs[ITERS + 1 :]
    held = (even_ref, odd_ref)
    layers, rows = fields_ref.shape[1:3]
    inner = pl.ds(SUBLANES, rows)
    for ref in held:
        clear_edges(ref, rows)
    active = jnp.where(fields_ref[0, 0] > 0.0, 1.0, 0.0)
    term = active * got_ref[1] * got_ref[0]

    def begin(first):
        for layer in range(UNROLL):
            layer = first + layer
            source = fields_ref[2, layer] + term * jnp.where(layer == edge_ref[0], 1.0, 0.0)
            vector = source * scale_ref[0, layer]
            basis[0][layer] = vector
            odd_ref[layer + 1, inner] = factor_ref[layer] * vector

    blocks(layers, UNROLL, begin)
    for k in range(ITERS):
        source_ref, target_ref = held[(k + 1) % 2], held[k % 2]

        def apply(first):
            for layer in range(UNROLL):
                layer = first + layer
                factor = factor_ref[layer]
                spread = stencil(source_ref, layer, rows)
                before = basis[k][layer]
                before = (1.0 - SHIFTS[k]) * before if SHIFTS[k] else before
                vector = before - factor * spread
                basis[k + 1][layer] = vector
                if k + 1 < ITERS:
                    target_ref[layer + 1, inner] = factor * vector

        blocks(layers, UNROLL, apply)

    lane = lanes_of(SUBLANES)
    half = LANES // 2
    gram_ref[...] = jnp.zeros(gram_ref.shape, jnp.float32)

    def products(first):
        sums = [None] * len(PAIRS)
        for n in range(0, 8, 2):
            for d in range(rows // SUBLANES):
                part = pl.ds(SUBLANES * d, SUBLANES)
                vectors = [
                    jnp.where(lane < half, ref[first + n, part], turned(ref[first + n + 1, part], half))
                    for ref in basis
                ]
                for p, (i, j) in enumerate(PAIRS):
                    product = vectors[j] * vectors[i]
                    sums[p] = product if sums[p] is None else sums[p] + product
        for p in range(len(PAIRS)):
            high, low = add_pairs(gram_ref[0, p], gram_ref[1, p], sums[p], 0.0)
            gram_ref[0, p] = high
            gram_ref[1, p] = low

    blocks(layers, 8, products)
    high, low = gram_ref[0, :, 0], gram_ref[1, :, 0]
    for row in range(1, SUBLANES):
        high, low = add_pairs(high, low, gram_ref[0, :, row], gram_ref[1, :, row])
    turn = LANES // 2
    while turn:
        high, low = add_pairs(high, low, pltpu.roll(high, turn, 1), pltpu.roll(low, turn, 1))
        turn //= 2
    packed = high[:SUBLANES]
    share = LANES // 4
    for g in range(4):
        part = slice(SUBLANES * g, SUBLANES * (g + 1))
        if g:
            packed = jnp.where(lane >= share * g, high[part], packed)
        packed = jnp.where((lane >= share * g + share // 2) & (lane < share * (g + 1)), low[part], packed)
    for d in range(sums_ref.shape[0]):
        sums_ref[d] = packed


def tree_sum(terms):
    while len(terms) > 1:
        terms = [sum(terms[i : i + 2]) for i in range(0, len(terms), 2)]
    return terms[0]


def quadratic(gram, left, right):
    products = []
    for i, a in enumerate(left):
        inside = [gram[max(i, j), min(i, j)] * b for j, b in enumerate(right)]
        products.append(a * tree_sum(inside))
    return tree_sum(products)


def iterate(gram):
    one = jnp.ones_like(gram[0, 0])
    zero = jnp.zeros_like(one)
    residual, direction, answer = [one], [one], []
    norm = gram[0, 0]
    for iteration in range(ITERS):
        applied = [SHIFTS[k] * c if SHIFTS[k] else zero for k, c in enumerate(direction)] + [zero]
        for k, c in enumerate(direction):
            applied[k + 1] = applied[k + 1] + c
        curve = quadratic(gram, direction, applied)
        step = norm / curve
        answer = [a + step * c for a, c in zip(answer + [zero], direction)]
        residual = [r - step * c for r, c in zip(residual + [zero], applied)]
        if iteration + 1 < ITERS:
            following = quadratic(gram, residual, residual)
            ratio = following / norm
            direction = [r + ratio * c for r, c in zip(residual, direction + [zero])]
            norm = following
    return answer, residual


def solve_kernel(sums_ref, coefs_ref, gram_ref):
    share = LANES // 4
    parts = [(sums_ref[d], turned(sums_ref[d], -share // 2)) for d in range(sums_ref.shape[0])]
    while len(parts) > 1:
        parts = [add_pairs(*parts[i], *parts[i + 1]) if i + 1 < len(parts) else parts[i] for i in range(0, len(parts), 2)]
    gram_ref[...] = parts[0][0] + parts[0][1]
    gram = {
        pair: gram_ref[pl.ds(p % SUBLANES, 1), pl.ds(share * (p // SUBLANES), 1)] for p, pair in enumerate(PAIRS)
    }
    answer, residual = iterate(gram)
    for n, coef in enumerate(answer + residual):
        coefs_ref[n] = jnp.broadcast_to(coef, (SUBLANES, LANES))


def combine_kernel(start, depth, where_ref, coefs_ref, *refs):
    basis = refs[: ITERS + 1]
    scale_ref, *out_refs = refs[ITERS + 1 :]
    half = LANES // 2
    lane = lanes_of(SUBLANES)
    rows = partner_rows(where_ref[1], len(out_refs))

    def mix(first):
        answer = [coefs_ref[n] for n in range(ITERS)]
        residual = [coefs_ref[ITERS + n] for n in range(ITERS + 1)]
        for layer in range(8):
            layer = first + layer
            for ref, part in zip(out_refs, rows):
                vectors = [basis_ref[start + layer, part] for basis_ref in basis]
                answered = tree_sum([c * v for c, v in zip(answer, vectors)]) * scale_ref[0, start + layer, part]
                left = tree_sum([c * v for c, v in zip(residual, vectors)]) * scale_ref[1, start + layer, part]
                ref[layer] = jnp.where(lane < half, answered, turned(left, half))

    blocks(depth, 8, mix)


def finish_kernel(start, depth, count, where_ref, *refs):
    parts = refs[:count]
    solution_ref, residual_ref, solved, left, sems = refs[-5:]
    half = LANES // 2
    lane = lanes_of(SUBLANES)
    copies = []
    for first in range(0, depth, 8):
        for layer in range(first, first + 8):
            got = by_partner(where_ref[1], [ref[layer] for ref in parts])
            for p in range(count // 2):
                place = pl.ds(LANES * p, LANES)
                low, high = got[2 * p : 2 * p + 2]
                solved[layer, :, place] = jnp.where(lane < half, low, turned(high, half))
                left[layer, :, place] = jnp.where(lane < half, turned(low, half), high)
    for n, (held, target) in enumerate(((solved, solution_ref), (left, residual_ref))):
        copy = pltpu.make_async_copy(held, target.at[0, pl.ds(start, depth)], sems.at[n])
        copy.start()
        copies.append(copy)
    for copy in copies:
        copy.wait()


def call(kernel, outs, args, smem=0, hbm=0, tail=0, scratch=(), limit=24, flops=10**6, aliases=None, hbm_outs=False):
    out_space = pltpu.HBM if hbm_outs else pltpu.VMEM
    return pl.pallas_call(
        kernel,
        out_shape=[jax.ShapeDtypeStruct(shape, jnp.float32) for shape in outs],
        in_specs=[pl.BlockSpec(memory_space=pltpu.SMEM)] * smem
        + [pl.BlockSpec(memory_space=pltpu.HBM)] * hbm
        + [pl.BlockSpec(memory_space=pltpu.VMEM)] * (len(args) - smem - hbm - tail)
        + [pl.BlockSpec(memory_space=pltpu.HBM)] * tail,
        out_specs=[pl.BlockSpec(memory_space=out_space)] * len(outs),
        scratch_shapes=[pltpu.VMEM(shape, jnp.float32) if isinstance(shape, tuple) else shape for shape in scratch],
        compiler_params=pltpu.CompilerParams(vmem_limit_bytes=limit * 2**20),
        cost_estimate=pl.CostEstimate(flops=flops, bytes_accessed=0, transcendentals=0),
        input_output_aliases=aliases or {},
    )(*args)


def exchanged(parts):
    count = len(parts)
    return [parts[0]] + [
        lax.ppermute(parts[k], "gx", [(i, i ^ k) for i in range(count)]) for k in range(1, count)
    ]


def in_windows(forcing, conduct, diag_add, ice_mask, grounded):
    _, layers, block_x, block_y = forcing.shape
    count_x, count_y = lax.axis_size("gx"), lax.axis_size("gy")
    rows = count_x * block_x
    group = lax.axis_index("group").astype(jnp.int32)
    place_x = lax.axis_index("gx").astype(jnp.int32)
    place_y = lax.axis_index("gy")
    edge = jnp.where(group == 0, 0, layers - 1).astype(jnp.int32)
    inside = jnp.stack([place_y > 0, place_y < count_y - 1]).astype(jnp.float32)
    own = (3, layers // 2, block_x, LANES)
    rim = (3, layers // 4, block_x, LANES)
    side = (3, layers // 8, block_x, LANES)
    block = (layers, block_x, block_y)
    chunks = 5 if layers % 40 == 0 else 1
    where = jnp.stack([edge, place_x])
    *made, low, high = call(
        prepare_kernel, [own] * count_x + [rim] * count_x + [side] * 2,
        (jnp.stack([group, place_x]), forcing, conduct, diag_add, ice_mask, grounded),
        smem=1, hbm=5,
        scratch=[
            block,
            pltpu.VMEM(block, conduct.dtype),
            pltpu.VMEM(block, diag_add.dtype),
            pltpu.VMEM(ice_mask.shape, ice_mask.dtype),
            pltpu.VMEM(grounded.shape, grounded.dtype),
            pltpu.SemaphoreType.DMA((chunks, 3)),
            pltpu.SemaphoreType.DMA((2,)),
            (SUBLANES, LANES),
        ],
    )
    owns = exchanged(made[:count_x])
    before = lax.ppermute(high, "gy", ring(count_y, 1))
    after = lax.ppermute(low, "gy", ring(count_y, -1))
    rims = call(rims_kernel, [rim] * count_x, (place_x[None], inside, before, after, *made[count_x:]), smem=2)
    rims = exchanged(rims)
    windows, shared = call(assemble_kernel, [(3, layers, rows, LANES), (2, rows, LANES)], (where, *owns, *rims), smem=1)
    received = from_partner(shared, "group", 0)
    padded = (layers + 2, rows + 2 * SUBLANES, LANES)
    window = (layers, rows, LANES)
    scale, factor = call(scale_kernel, [(2,) + window, window], (windows,), scratch=[padded], flops=4 * 10**7)
    *basis, sums = call(
        krylov_kernel, [window] * (ITERS + 1) + [(count_x * count_y, SUBLANES, LANES)],
        (edge[None], windows, received, scale, factor), smem=1,
        scratch=[padded] * 2 + [(2, 32, SUBLANES, LANES)], limit=32,
    )
    sums = lax.all_to_all(sums, ("gx", "gy"), 0, 0, tiled=True)
    (coefs,) = call(solve_kernel, [(2 * ITERS + 1, SUBLANES, LANES)], (sums,), scratch=[(SUBLANES, LANES)])
    depth = layers // PARTS
    arrived = []
    for n in range(PARTS):
        mixed = call(
            functools.partial(combine_kernel, n * depth, depth),
            [(depth, block_x, LANES)] * count_x, (where, coefs, *basis, scale), smem=1,
        )
        arrived.append(exchanged(mixed))
    outs = ()
    for n in range(PARTS):
        outs = tuple(
            call(
                functools.partial(finish_kernel, n * depth, depth, count_x),
                [forcing.shape] * 2, (where, *arrived[n], *outs), smem=1, tail=len(outs), hbm_outs=True,
                scratch=[(depth, block_x, block_y)] * 2 + [pltpu.SemaphoreType.DMA((2,))],
                aliases={1 + count_x + i: i for i in range(len(outs))},
            )
        )
    return outs


def fits_windows(layers, block_x, block_y, count_x):
    width = block_y // count_x
    return (
        layers % (LANES // HALO) == 0
        and block_x == SUBLANES
        and block_y % LANES == 0
        and 2 * width == LANES
        and HALO >= 2 * (ITERS + 1)
    )


def per_device(forcing, conduct, diag_add, ice_mask, grounded):
    _, layers, block_x, block_y = forcing.shape
    if not fits_windows(layers, block_x, block_y, lax.axis_size("gx")):
        return on_device(forcing, conduct, diag_add, ice_mask, grounded)
    return in_windows(forcing, conduct, diag_add, ice_mask, grounded)


def solution(mesh):
    in_specs = (
        P("group", None, "gx", "gy"),
        P("group", None, "gx", "gy"),
        P("group", None, "gx", "gy"),
        P("gx", "gy"),
        P("gx", "gy"),
    )
    out_specs = (P("group", None, "gx", "gy"), P("group", None, "gx", "gy"))
    return jax.shard_map(
        per_device, mesh=mesh, in_specs=in_specs, out_specs=out_specs, check_vma=False
    )
```

```python
import functools
import math

import jax
import jax.numpy as jnp
from jax import lax
from jax.experimental import pallas as pl
from jax.experimental.pallas import tpu as pltpu
from jax.sharding import PartitionSpec as P


ITERS = 6
LANES = 128
SUBLANES = 8
HALO = 16
SHIFTS = (0.0, 0.75, 1.5, 0.25, 1.75, 1.0)
UNROLL = 16
PARTS = 2
PAIRS = tuple((i, j) for i in range(ITERS + 1) for j in range(i + 1) if j < ITERS)


far_weight = 0.25
cross_weight = 0.5
vertical_weight = 4.0
friction_gain = 8.0
NEIGHBOURS = (
    (1, 0, 1.0),
    (-1, 0, 1.0),
    (0, 1, 1.0),
    (0, -1, 1.0),
    (2, 0, far_weight),
    (-2, 0, far_weight),
    (0, 2, far_weight),
    (0, -2, far_weight),
    (1, 1, cross_weight),
    (1, -1, cross_weight),
    (-1, 1, cross_weight),
    (-1, -1, cross_weight),
)


def with_halo(block, sides, width):
    for axis, dim in sides:
        count = lax.axis_size(axis)
        place = lax.axis_index(axis)
        ahead = [(i, (i + 1) % count) for i in range(count)]
        back = [(target, source) for source, target in ahead]
        low = lax.ppermute(
            lax.slice_in_dim(block, block.shape[dim] - width, None, axis=dim), axis, ahead
        )
        high = lax.ppermute(lax.slice_in_dim(block, 0, width, axis=dim), axis, back)
        low = jnp.where(place > 0, low, 0.0)
        high = jnp.where(place < count - 1, high, 0.0)
        block = jnp.concatenate([low, block, high], axis=dim)
    return block


def from_partner(shard, axis, distance):
    return lax.ppermute(shard, axis, [(i, i ^ 1 << distance) for i in range(lax.axis_size(axis))])


def beside_sum(padded, extent_x, extent_y):
    summed = jnp.zeros((padded.shape[0], extent_x, extent_y), jnp.float32)
    for shift_x, shift_y, weight in NEIGHBOURS:
        summed = (
            summed
            + weight
            * padded[:, 2 + shift_x : 2 + shift_x + extent_x, 2 + shift_y : 2 + shift_y + extent_y]
        )
    return summed


def vertical_sum(values):
    zeroes = jnp.zeros_like(values[:1])
    return jnp.concatenate([values[1:], zeroes], 0) + jnp.concatenate([zeroes, values[:-1]], 0)


def spread_padded(padded, values):
    return beside_sum(padded, values.shape[1], values.shape[2]) + vertical_weight * vertical_sum(
        values
    )


def operate(vector, coupling, diagonal):
    scaled = coupling * vector
    padded = with_halo(scaled, (("gx", 1), ("gy", 2)), 2)
    return diagonal * vector - coupling * spread_padded(padded, scaled)


def sum_over(partial, axes):
    count = math.prod(lax.axis_size(axis) for axis in axes)
    sent = jnp.broadcast_to(partial[None, None], (count, 1) + partial.shape)
    return jnp.sum(lax.all_to_all(sent, axes, 0, 0, tiled=True), axis=(0, 1))


def paired_sums(residual, precond, applied):
    partial = jnp.stack([jnp.sum(residual * precond), jnp.sum(applied * precond)])
    summed = sum_over(partial, ("gx", "gy"))
    return summed[0], summed[1]


def on_device(forcing, conduct, diag_add, ice_mask, grounded):
    own_force = forcing[0]
    layers = own_force.shape[0]
    group_id = lax.axis_index("group")
    is_ice = (group_id == 0).astype(jnp.float32)
    ice_cells = ice_mask.astype(jnp.float32)
    ground_cells = grounded.astype(jnp.float32)
    active = ice_cells * (1.0 - (1.0 - is_ice) * ground_cells)
    coupling = jnp.sqrt(conduct[0].astype(jnp.float32)) * active
    layer_index = lax.broadcasted_iota(jnp.int32, (layers, 1, 1), 0)
    edge_layer = jnp.where(group_id == 0, 0, layers - 1).astype(jnp.int32)
    edge_pick = (layer_index == edge_layer).astype(jnp.float32)
    bottom = (layer_index == 0).astype(jnp.float32)
    base_diag = diag_add[0].astype(jnp.float32) + bottom * (
        is_ice * friction_gain * ground_cells * ice_cells
    )
    padded_coupling = with_halo(coupling, (("gx", 1), ("gy", 2)), 2)
    diagonal = base_diag + coupling * spread_padded(padded_coupling, coupling)
    shared_value = active * jnp.mean(own_force, axis=0)
    shared_weight = lax.dynamic_index_in_dim(coupling, edge_layer, 0, keepdims=False)
    received = from_partner(jnp.stack([shared_value, shared_weight]), "group", 0)
    source = active * own_force + edge_pick * (active * received[1] * received[0])
    inverse = 1.0 / diagonal
    solution = jnp.zeros_like(source)
    residual = source
    precond = inverse * residual
    applied = operate(precond, coupling, diagonal)
    norm_now, curve = paired_sums(residual, precond, applied)
    step_size = norm_now / curve
    direction = precond
    along = applied
    for iteration in range(ITERS):
        solution = solution + step_size * direction
        residual = residual - step_size * along
        if iteration + 1 < ITERS:
            precond = inverse * residual
            applied = operate(precond, coupling, diagonal)
            norm_next, curve = paired_sums(residual, precond, applied)
            step_ratio = norm_next / norm_now
            step_size = norm_next / (curve - step_ratio * norm_next / step_size)
            direction = precond + step_ratio * direction
            along = applied + step_ratio * along
            norm_now = norm_next
    return (solution[None], residual[None])


def ring(count, step):
    return [(i, (i + step) % count) for i in range(count)]


def lanes_of(rows):
    return lax.broadcasted_iota(jnp.int32, (rows, LANES), 1)


def blocks(total, size, body):
    def step(g, carry):
        body(g * size)
        return carry

    lax.fori_loop(0, total // size, step, 0)


def slots_of(rows):
    return lanes_of(rows) // HALO


RIGHT = tuple((4 + 2 * j) % 8 for j in range(4))
LEFT = tuple((7 + 2 * j) % 8 for j in range(4))


def turned(value, amount):
    return pltpu.roll(value, amount % LANES, 1) if amount % LANES else value


def by_partner(place, values):
    bit = 1
    while bit < len(values):
        swap = (place & bit) != 0
        values = [jnp.where(swap, values[d ^ bit], values[d]) for d in range(len(values))]
        bit *= 2
    return values


def partner_rows(place, count):
    return [pl.ds(pl.multiple_of(SUBLANES * (place ^ n), SUBLANES), SUBLANES) for n in range(count)]


def prepare_kernel(where_ref, force_ref, conduct_ref, diag_ref, ice_ref, ground_ref, *refs):
    count = (len(refs) - 10) // 2
    own_refs, rim_refs = refs[:count], refs[count : 2 * count]
    low_ref, high_ref, force, conduct, diag, ice, ground, sems, small_sems, _ = refs[2 * count :]
    layers = force.shape[0]
    chunks = sems.shape[0]
    depth = layers // chunks
    small = [
        pltpu.make_async_copy(ice_ref, ice, small_sems.at[0]),
        pltpu.make_async_copy(ground_ref, ground, small_sems.at[1]),
    ]
    copies = []
    for copy in small:
        copy.start()
    for c in range(chunks):
        part = pl.ds(c * depth, depth)
        row = []
        for n, (source, target) in enumerate(((force_ref, force), (conduct_ref, conduct), (diag_ref, diag))):
            copy = pltpu.make_async_copy(source.at[0, part], target.at[part], sems.at[c, n])
            copy.start()
            row.append(copy)
        copies.append(row)
    place = where_ref[1]
    is_ice = jnp.where(where_ref[0] == 0, 1.0, 0.0)
    for copy in small:
        copy.wait()
    ice_cells = ice[...].astype(jnp.float32)
    ground_cells = ground[...].astype(jnp.float32)
    active = ice_cells * (1.0 - (1.0 - is_ice) * ground_cells)
    friction = is_ice * friction_gain * ground_cells * ice_cells
    lane = lanes_of(SUBLANES)
    slot = slots_of(SUBLANES)
    half = LANES // 2

    def step(q, carry):
        for k in range(3):
            low = high = None
            for group in range(2):
                rims = [None] * count
                pair = []
                for j in range(4):
                    layer = q * 8 + group * 4 + j
                    if k == 0:
                        value = jnp.sqrt(conduct[layer].astype(jnp.float32)) * active
                    elif k == 1:
                        value = diag[layer].astype(jnp.float32)
                        if group == 0 and j == 0:
                            value = value + friction * jnp.where(q == 0, 1.0, 0.0)
                    else:
                        value = active * force[layer]
                    pieces = [value[:, LANES * p : LANES * (p + 1)] for p in range(count // 2)]
                    halves = [turned(piece, half) for piece in pieces]
                    pair.append((pieces, halves))
                    even = halves if j == 2 else [turned(piece, 32 * j) for piece in pieces]
                    odd = halves if j == 0 else pieces if j == 2 else [turned(piece, half + 32 * j) for piece in pieces]
                    for d in range(count):
                        p = d // 2
                        sources = []
                        if d % 2 == 0:
                            sources.append((RIGHT[j], even[p]))
                            if d:
                                sources.append((LEFT[j], even[p - 1]))
                        else:
                            sources.append((LEFT[j], odd[p]))
                            if d + 1 < count:
                                sources.append((RIGHT[j], odd[p + 1]))
                        for target, source in sources:
                            rims[d] = source if rims[d] is None else jnp.where(slot == target, source, rims[d])
                    if group == 0:
                        first, last, first_slot, last_slot = odd[0], even[-1], RIGHT[j], LEFT[j]
                    else:
                        first, last = turned(pieces[0], 112 + 32 * j), turned(pieces[-1], 80 + 32 * j)
                        first_slot, last_slot = LEFT[j], RIGHT[j]
                    low = first if low is None else jnp.where(slot == first_slot, first, low)
                    high = last if high is None else jnp.where(slot == last_slot, last, high)
                    if j % 2:
                        (even_pieces, even_halves), (odd_pieces, odd_halves) = pair[-2:]
                        packed = []
                        for d in range(count):
                            p = d // 2
                            if d % 2 == 0:
                                packed.append(jnp.where(lane < half, even_pieces[p], odd_halves[p]))
                            else:
                                packed.append(jnp.where(lane < half, even_halves[p], odd_pieces[p]))
                        for ref, packed_value in zip(own_refs, by_partner(place, packed)):
                            ref[k, q * 4 + group * 2 + j // 2] = packed_value
                for ref, rim in zip(rim_refs, by_partner(place, rims)):
                    ref[k, q * 2 + group] = rim
            low_ref[k, q] = low
            high_ref[k, q] = high
        return carry

    for c in range(chunks):
        for copy in copies[c]:
            copy.wait()
        lax.fori_loop(c * depth // 8, (c + 1) * depth // 8, step, 0)


def rims_kernel(place_ref, edge_ref, low_ref, high_ref, *refs):
    count = len(refs) // 2
    groups = low_ref.shape[1]
    odd = slots_of(SUBLANES) % 2 == 1
    first = [jnp.where(odd, place_ref[0], -1) == k for k in range(count)]
    last = [jnp.where(odd, -1, place_ref[0] ^ (count - 1)) == k for k in range(count)]

    def step(q):
        for k in range(3):
            before, after = low_ref[k, q], high_ref[k, q]
            if k == 0:
                before, after = before * edge_ref[0], after * edge_ref[1]
            befores, afters = (before, turned(before, 48)), (after, turned(after, 80))
            for n in range(count):
                for group in range(2):
                    rim = refs[n][k, 2 * q + group]
                    rim = jnp.where(first[n], befores[group], rim)
                    refs[count + n][k, 2 * q + group] = jnp.where(last[n], afters[group], rim)

    def pair(start):
        step(start)
        step(start + 1)

    blocks(groups, 2, pair)


def assemble_kernel(where_ref, *refs):
    count = (len(refs) - 2) // 2
    own_refs, rim_refs = refs[:count], refs[count : 2 * count]
    fields_ref, shared_ref = refs[2 * count :]
    groups = rim_refs[0].shape[1]
    lane = lanes_of(SUBLANES)
    half = LANES // 2
    inside = (lane < half + HALO) | (lane >= LANES - HALO)
    rows = partner_rows(where_ref[1], count)

    def step(i, totals):
        totals = list(totals)
        for u in range(2):
            g = 2 * i + u
            for k in range(3):
                fill = 1.0 if k == 1 else 0.0
                for n in range(count):
                    rim = rim_refs[n][k, g]
                    for pair in range(2):
                        packed = own_refs[n][k, 2 * g + pair]
                        for own, j in ((packed, 2 * pair), (turned(packed, half), 2 * pair + 1)):
                            value = jnp.where(lane < half, own, jnp.where(inside, turned(rim, -32 * j), fill))
                            fields_ref[k, 4 * g + j, rows[n]] = value
                            if k == 2:
                                totals[n] = totals[n] + value
        return tuple(totals)

    zero = jnp.zeros((SUBLANES, LANES), jnp.float32)
    totals = lax.fori_loop(0, groups // 2, step, (zero,) * count)
    for n in range(count):
        shared_ref[0, rows[n]] = totals[n] / (4 * groups)
        shared_ref[1, rows[n]] = fields_ref[0, where_ref[0], rows[n]]


def two_sum(a, b):
    total = a + b
    part = total - a
    return total, (a - (total - part)) + (b - part)


def add_pairs(high, low, other_high, other_low):
    total, error = two_sum(high, other_high)
    return total, low + other_low + error


def stencil(held_ref, layer, rows):
    def at(shift):
        return held_ref[layer + 1, pl.ds(SUBLANES + shift, rows)]

    here = at(0)
    near = at(1) + at(-1)
    mixed = here + cross_weight * near
    far = at(2) + at(-2) + turned(here, 2) + turned(here, -2)
    beside = near + turned(mixed, 1) + turned(mixed, -1) + far_weight * far
    above = held_ref[layer + 2, pl.ds(SUBLANES, rows)] + held_ref[layer, pl.ds(SUBLANES, rows)]
    return beside + vertical_weight * above


def scale_kernel(fields_ref, scale_ref, factor_ref, held_ref):
    layers, rows = fields_ref.shape[1:3]
    inner = pl.ds(SUBLANES, rows)
    clear_edges(held_ref, rows)

    def fill(first):
        for layer in range(UNROLL):
            held_ref[first + layer + 1, inner] = fields_ref[0, first + layer]

    blocks(layers, UNROLL, fill)

    def begin(first):
        for layer in range(UNROLL):
            layer = first + layer
            coupling = fields_ref[0, layer]
            diagonal = fields_ref[1, layer] + coupling * stencil(held_ref, layer, rows)
            root = jnp.sqrt(diagonal)
            inverse = 1.0 / root
            scale_ref[0, layer] = inverse
            scale_ref[1, layer] = root
            factor_ref[layer] = coupling * inverse

    blocks(layers, UNROLL, begin)


def clear_edges(ref, rows):
    layers = ref.shape[0]
    empty = jnp.zeros((layers, SUBLANES, LANES), jnp.float32)
    ref[:, :SUBLANES] = empty
    ref[:, SUBLANES + rows :] = empty
    ref[0] = jnp.zeros((rows + 2 * SUBLANES, LANES), jnp.float32)
    ref[layers - 1] = jnp.zeros((rows + 2 * SUBLANES, LANES), jnp.float32)


def krylov_kernel(edge_ref, fields_ref, got_ref, scale_ref, factor_ref, *refs):
    basis = refs[: ITERS + 1]
    sums_ref, even_ref, odd_ref, gram_ref = refs[ITERS + 1 :]
    held = (even_ref, odd_ref)
    layers, rows = fields_ref.shape[1:3]
    inner = pl.ds(SUBLANES, rows)
    for ref in held:
        clear_edges(ref, rows)
    active = jnp.where(fields_ref[0, 0] > 0.0, 1.0, 0.0)
    term = active * got_ref[1] * got_ref[0]

    def begin(first):
        for layer in range(UNROLL):
            layer = first + layer
            source = fields_ref[2, layer] + term * jnp.where(layer == edge_ref[0], 1.0, 0.0)
            vector = source * scale_ref[0, layer]
            basis[0][layer] = vector
            odd_ref[layer + 1, inner] = factor_ref[layer] * vector

    blocks(layers, UNROLL, begin)
    for k in range(ITERS):
        source_ref, target_ref = held[(k + 1) % 2], held[k % 2]

        def apply(first):
            for layer in range(UNROLL):
                layer = first + layer
                factor = factor_ref[layer]
                spread = stencil(source_ref, layer, rows)
                before = basis[k][layer]
                before = (1.0 - SHIFTS[k]) * before if SHIFTS[k] else before
                vector = before - factor * spread
                basis[k + 1][layer] = vector
                if k + 1 < ITERS:
                    target_ref[layer + 1, inner] = factor * vector

        blocks(layers, UNROLL, apply)

    lane = lanes_of(SUBLANES)
    half = LANES // 2
    gram_ref[...] = jnp.zeros(gram_ref.shape, jnp.float32)

    def products(first):
        sums = [None] * len(PAIRS)
        for n in range(0, 8, 2):
            for d in range(rows // SUBLANES):
                part = pl.ds(SUBLANES * d, SUBLANES)
                vectors = [
                    jnp.where(lane < half, ref[first + n, part], turned(ref[first + n + 1, part], half))
                    for ref in basis
                ]
                for p, (i, j) in enumerate(PAIRS):
                    product = vectors[j] * vectors[i]
                    sums[p] = product if sums[p] is None else sums[p] + product
        for p in range(len(PAIRS)):
            high, low = add_pairs(gram_ref[0, p], gram_ref[1, p], sums[p], 0.0)
            gram_ref[0, p] = high
            gram_ref[1, p] = low

    blocks(layers, 8, products)
    high, low = gram_ref[0, :, 0], gram_ref[1, :, 0]
    for row in range(1, SUBLANES):
        high, low = add_pairs(high, low, gram_ref[0, :, row], gram_ref[1, :, row])
    turn = LANES // 2
    while turn:
        high, low = add_pairs(high, low, pltpu.roll(high, turn, 1), pltpu.roll(low, turn, 1))
        turn //= 2
    packed = high[:SUBLANES]
    share = LANES // 4
    for g in range(4):
        part = slice(SUBLANES * g, SUBLANES * (g + 1))
        if g:
            packed = jnp.where(lane >= share * g, high[part], packed)
        packed = jnp.where((lane >= share * g + share // 2) & (lane < share * (g + 1)), low[part], packed)
    for d in range(sums_ref.shape[0]):
        sums_ref[d] = packed


def tree_sum(terms):
    while len(terms) > 1:
        terms = [sum(terms[i : i + 2]) for i in range(0, len(terms), 2)]
    return terms[0]


def quadratic(gram, left, right):
    products = []
    for i, a in enumerate(left):
        inside = [gram[max(i, j), min(i, j)] * b for j, b in enumerate(right)]
        products.append(a * tree_sum(inside))
    return tree_sum(products)


def iterate(gram):
    one = jnp.ones_like(gram[0, 0])
    zero = jnp.zeros_like(one)
    residual, direction, answer = [one], [one], []
    norm = gram[0, 0]
    for iteration in range(ITERS):
        applied = [SHIFTS[k] * c if SHIFTS[k] else zero for k, c in enumerate(direction)] + [zero]
        for k, c in enumerate(direction):
            applied[k + 1] = applied[k + 1] + c
        curve = quadratic(gram, direction, applied)
        step = norm / curve
        answer = [a + step * c for a, c in zip(answer + [zero], direction)]
        residual = [r - step * c for r, c in zip(residual + [zero], applied)]
        if iteration + 1 < ITERS:
            following = quadratic(gram, residual, residual)
            ratio = following / norm
            direction = [r + ratio * c for r, c in zip(residual, direction + [zero])]
            norm = following
    return answer, residual


def solve_kernel(sums_ref, coefs_ref, gram_ref):
    share = LANES // 4
    parts = [(sums_ref[d], turned(sums_ref[d], -share // 2)) for d in range(sums_ref.shape[0])]
    while len(parts) > 1:
        parts = [add_pairs(*parts[i], *parts[i + 1]) if i + 1 < len(parts) else parts[i] for i in range(0, len(parts), 2)]
    gram_ref[...] = parts[0][0] + parts[0][1]
    gram = {
        pair: gram_ref[pl.ds(p % SUBLANES, 1), pl.ds(share * (p // SUBLANES), 1)] for p, pair in enumerate(PAIRS)
    }
    answer, residual = iterate(gram)
    for n, coef in enumerate(answer + residual):
        coefs_ref[n] = jnp.broadcast_to(coef, (SUBLANES, LANES))


def combine_kernel(start, depth, where_ref, coefs_ref, *refs):
    basis = refs[: ITERS + 1]
    scale_ref, *out_refs = refs[ITERS + 1 :]
    half = LANES // 2
    lane = lanes_of(SUBLANES)
    rows = partner_rows(where_ref[1], len(out_refs))

    def mix(first):
        answer = [coefs_ref[n] for n in range(ITERS)]
        residual = [coefs_ref[ITERS + n] for n in range(ITERS + 1)]
        for layer in range(8):
            layer = first + layer
            for ref, part in zip(out_refs, rows):
                vectors = [basis_ref[start + layer, part] for basis_ref in basis]
                answered = tree_sum([c * v for c, v in zip(answer, vectors)]) * scale_ref[0, start + layer, part]
                left = tree_sum([c * v for c, v in zip(residual, vectors)]) * scale_ref[1, start + layer, part]
                ref[layer] = jnp.where(lane < half, answered, turned(left, half))

    blocks(depth, 8, mix)


def finish_kernel(start, depth, count, where_ref, *refs):
    parts = refs[:count]
    solution_ref, residual_ref, solved, left, sems = refs[-5:]
    half = LANES // 2
    lane = lanes_of(SUBLANES)
    copies = []
    for first in range(0, depth, 8):
        for layer in range(first, first + 8):
            got = by_partner(where_ref[1], [ref[layer] for ref in parts])
            for p in range(count // 2):
                place = pl.ds(LANES * p, LANES)
                low, high = got[2 * p : 2 * p + 2]
                solved[layer, :, place] = jnp.where(lane < half, low, turned(high, half))
                left[layer, :, place] = jnp.where(lane < half, turned(low, half), high)
    for n, (held, target) in enumerate(((solved, solution_ref), (left, residual_ref))):
        copy = pltpu.make_async_copy(held, target.at[0, pl.ds(start, depth)], sems.at[n])
        copy.start()
        copies.append(copy)
    for copy in copies:
        copy.wait()


def call(kernel, outs, args, smem=0, hbm=0, tail=0, scratch=(), limit=24, flops=10**6, aliases=None, hbm_outs=False):
    out_space = pltpu.HBM if hbm_outs else pltpu.VMEM
    return pl.pallas_call(
        kernel,
        out_shape=[jax.ShapeDtypeStruct(shape, jnp.float32) for shape in outs],
        in_specs=[pl.BlockSpec(memory_space=pltpu.SMEM)] * smem
        + [pl.BlockSpec(memory_space=pltpu.HBM)] * hbm
        + [pl.BlockSpec(memory_space=pltpu.VMEM)] * (len(args) - smem - hbm - tail)
        + [pl.BlockSpec(memory_space=pltpu.HBM)] * tail,
        out_specs=[pl.BlockSpec(memory_space=out_space)] * len(outs),
        scratch_shapes=[pltpu.VMEM(shape, jnp.float32) if isinstance(shape, tuple) else shape for shape in scratch],
        compiler_params=pltpu.CompilerParams(vmem_limit_bytes=limit * 2**20),
        cost_estimate=pl.CostEstimate(flops=flops, bytes_accessed=0, transcendentals=0),
        input_output_aliases=aliases or {},
    )(*args)


def exchanged(parts):
    count = len(parts)
    return [parts[0]] + [
        lax.ppermute(parts[k], "gx", [(i, i ^ k) for i in range(count)]) for k in range(1, count)
    ]


def in_windows(forcing, conduct, diag_add, ice_mask, grounded):
    _, layers, block_x, block_y = forcing.shape
    count_x, count_y = lax.axis_size("gx"), lax.axis_size("gy")
    rows = count_x * block_x
    group = lax.axis_index("group").astype(jnp.int32)
    place_x = lax.axis_index("gx").astype(jnp.int32)
    place_y = lax.axis_index("gy")
    edge = jnp.where(group == 0, 0, layers - 1).astype(jnp.int32)
    inside = jnp.stack([place_y > 0, place_y < count_y - 1]).astype(jnp.float32)
    own = (3, layers // 2, block_x, LANES)
    rim = (3, layers // 4, block_x, LANES)
    side = (3, layers // 8, block_x, LANES)
    block = (layers, block_x, block_y)
    chunks = 5 if layers % 40 == 0 else 1
    where = jnp.stack([edge, place_x])
    forcing, conduct, diag_add, ice_mask, grounded = [
        pltpu.with_memory_space_constraint(x, pltpu.HBM)
        for x in (forcing, conduct, diag_add, ice_mask, grounded)
    ]
    *made, low, high = call(
        prepare_kernel, [own] * count_x + [rim] * count_x + [side] * 2,
        (jnp.stack([group, place_x]), forcing, conduct, diag_add, ice_mask, grounded),
        smem=1, hbm=5,
        scratch=[
            block,
            pltpu.VMEM(block, conduct.dtype),
            pltpu.VMEM(block, diag_add.dtype),
            pltpu.VMEM(ice_mask.shape, ice_mask.dtype),
            pltpu.VMEM(grounded.shape, grounded.dtype),
            pltpu.SemaphoreType.DMA((chunks, 3)),
            pltpu.SemaphoreType.DMA((2,)),
            (SUBLANES, LANES),
        ],
    )
    owns = exchanged(made[:count_x])
    before = lax.ppermute(high, "gy", ring(count_y, 1))
    after = lax.ppermute(low, "gy", ring(count_y, -1))
    rims = call(rims_kernel, [rim] * count_x, (place_x[None], inside, before, after, *made[count_x:]), smem=2)
    rims = exchanged(rims)
    windows, shared = call(assemble_kernel, [(3, layers, rows, LANES), (2, rows, LANES)], (where, *owns, *rims), smem=1)
    received = from_partner(shared, "group", 0)
    padded = (layers + 2, rows + 2 * SUBLANES, LANES)
    window = (layers, rows, LANES)
    scale, factor = call(scale_kernel, [(2,) + window, window], (windows,), scratch=[padded], flops=4 * 10**7)
    *basis, sums = call(
        krylov_kernel, [window] * (ITERS + 1) + [(count_x * count_y, SUBLANES, LANES)],
        (edge[None], windows, received, scale, factor), smem=1,
        scratch=[padded] * 2 + [(2, 32, SUBLANES, LANES)], limit=32,
    )
    sums = lax.all_to_all(sums, ("gx", "gy"), 0, 0, tiled=True)
    (coefs,) = call(solve_kernel, [(2 * ITERS + 1, SUBLANES, LANES)], (sums,), scratch=[(SUBLANES, LANES)])
    depth = layers // PARTS
    arrived = []
    for n in range(PARTS):
        mixed = call(
            functools.partial(combine_kernel, n * depth, depth),
            [(depth, block_x, LANES)] * count_x, (where, coefs, *basis, scale), smem=1,
        )
        arrived.append(exchanged(mixed))
    outs = ()
    for n in range(PARTS):
        outs = tuple(
            call(
                functools.partial(finish_kernel, n * depth, depth, count_x),
                [forcing.shape] * 2, (where, *arrived[n], *outs), smem=1, tail=len(outs), hbm_outs=True,
                scratch=[(depth, block_x, block_y)] * 2 + [pltpu.SemaphoreType.DMA((2,))],
                aliases={1 + count_x + i: i for i in range(len(outs))},
            )
        )
    return outs


def fits_windows(layers, block_x, block_y, count_x):
    width = block_y // count_x
    return (
        layers % (LANES // HALO) == 0
        and block_x == SUBLANES
        and block_y % LANES == 0
        and 2 * width == LANES
        and HALO >= 2 * (ITERS + 1)
    )


def per_device(forcing, conduct, diag_add, ice_mask, grounded):
    _, layers, block_x, block_y = forcing.shape
    if not fits_windows(layers, block_x, block_y, lax.axis_size("gx")):
        return on_device(forcing, conduct, diag_add, ice_mask, grounded)
    return in_windows(forcing, conduct, diag_add, ice_mask, grounded)


def solution(mesh):
    in_specs = (
        P("group", None, "gx", "gy"),
        P("group", None, "gx", "gy"),
        P("group", None, "gx", "gy"),
        P("gx", "gy"),
        P("gx", "gy"),
    )
    out_specs = (P("group", None, "gx", "gy"), P("group", None, "gx", "gy"))
    return jax.shard_map(
        per_device, mesh=mesh, in_specs=in_specs, out_specs=out_specs, check_vma=False
    )
```

```python
import functools
import math

import jax
import jax.numpy as jnp
from jax import lax
from jax.experimental import pallas as pl
from jax.experimental.pallas import tpu as pltpu
from jax.sharding import PartitionSpec as P


ITERS = 6
LANES = 128
SUBLANES = 8
HALO = 16
SHIFTS = (0.0, 0.75, 1.5, 0.25, 1.75, 1.0)
UNROLL = 16
PARTS = 2
PAIRS = tuple((i, j) for i in range(ITERS + 1) for j in range(i + 1) if j < ITERS)


far_weight = 0.25
cross_weight = 0.5
vertical_weight = 4.0
friction_gain = 8.0
NEIGHBOURS = (
    (1, 0, 1.0),
    (-1, 0, 1.0),
    (0, 1, 1.0),
    (0, -1, 1.0),
    (2, 0, far_weight),
    (-2, 0, far_weight),
    (0, 2, far_weight),
    (0, -2, far_weight),
    (1, 1, cross_weight),
    (1, -1, cross_weight),
    (-1, 1, cross_weight),
    (-1, -1, cross_weight),
)


def with_halo(block, sides, width):
    for axis, dim in sides:
        count = lax.axis_size(axis)
        place = lax.axis_index(axis)
        ahead = [(i, (i + 1) % count) for i in range(count)]
        back = [(target, source) for source, target in ahead]
        low = lax.ppermute(
            lax.slice_in_dim(block, block.shape[dim] - width, None, axis=dim), axis, ahead
        )
        high = lax.ppermute(lax.slice_in_dim(block, 0, width, axis=dim), axis, back)
        low = jnp.where(place > 0, low, 0.0)
        high = jnp.where(place < count - 1, high, 0.0)
        block = jnp.concatenate([low, block, high], axis=dim)
    return block


def from_partner(shard, axis, distance):
    return lax.ppermute(shard, axis, [(i, i ^ 1 << distance) for i in range(lax.axis_size(axis))])


def beside_sum(padded, extent_x, extent_y):
    summed = jnp.zeros((padded.shape[0], extent_x, extent_y), jnp.float32)
    for shift_x, shift_y, weight in NEIGHBOURS:
        summed = (
            summed
            + weight
            * padded[:, 2 + shift_x : 2 + shift_x + extent_x, 2 + shift_y : 2 + shift_y + extent_y]
        )
    return summed


def vertical_sum(values):
    zeroes = jnp.zeros_like(values[:1])
    return jnp.concatenate([values[1:], zeroes], 0) + jnp.concatenate([zeroes, values[:-1]], 0)


def spread_padded(padded, values):
    return beside_sum(padded, values.shape[1], values.shape[2]) + vertical_weight * vertical_sum(
        values
    )


def operate(vector, coupling, diagonal):
    scaled = coupling * vector
    padded = with_halo(scaled, (("gx", 1), ("gy", 2)), 2)
    return diagonal * vector - coupling * spread_padded(padded, scaled)


def sum_over(partial, axes):
    count = math.prod(lax.axis_size(axis) for axis in axes)
    sent = jnp.broadcast_to(partial[None, None], (count, 1) + partial.shape)
    return jnp.sum(lax.all_to_all(sent, axes, 0, 0, tiled=True), axis=(0, 1))


def paired_sums(residual, precond, applied):
    partial = jnp.stack([jnp.sum(residual * precond), jnp.sum(applied * precond)])
    summed = sum_over(partial, ("gx", "gy"))
    return summed[0], summed[1]


def on_device(forcing, conduct, diag_add, ice_mask, grounded):
    own_force = forcing[0]
    layers = own_force.shape[0]
    group_id = lax.axis_index("group")
    is_ice = (group_id == 0).astype(jnp.float32)
    ice_cells = ice_mask.astype(jnp.float32)
    ground_cells = grounded.astype(jnp.float32)
    active = ice_cells * (1.0 - (1.0 - is_ice) * ground_cells)
    coupling = jnp.sqrt(conduct[0].astype(jnp.float32)) * active
    layer_index = lax.broadcasted_iota(jnp.int32, (layers, 1, 1), 0)
    edge_layer = jnp.where(group_id == 0, 0, layers - 1).astype(jnp.int32)
    edge_pick = (layer_index == edge_layer).astype(jnp.float32)
    bottom = (layer_index == 0).astype(jnp.float32)
    base_diag = diag_add[0].astype(jnp.float32) + bottom * (
        is_ice * friction_gain * ground_cells * ice_cells
    )
    padded_coupling = with_halo(coupling, (("gx", 1), ("gy", 2)), 2)
    diagonal = base_diag + coupling * spread_padded(padded_coupling, coupling)
    shared_value = active * jnp.mean(own_force, axis=0)
    shared_weight = lax.dynamic_index_in_dim(coupling, edge_layer, 0, keepdims=False)
    received = from_partner(jnp.stack([shared_value, shared_weight]), "group", 0)
    source = active * own_force + edge_pick * (active * received[1] * received[0])
    inverse = 1.0 / diagonal
    solution = jnp.zeros_like(source)
    residual = source
    precond = inverse * residual
    applied = operate(precond, coupling, diagonal)
    norm_now, curve = paired_sums(residual, precond, applied)
    step_size = norm_now / curve
    direction = precond
    along = applied
    for iteration in range(ITERS):
        solution = solution + step_size * direction
        residual = residual - step_size * along
        if iteration + 1 < ITERS:
            precond = inverse * residual
            applied = operate(precond, coupling, diagonal)
            norm_next, curve = paired_sums(residual, precond, applied)
            step_ratio = norm_next / norm_now
            step_size = norm_next / (curve - step_ratio * norm_next / step_size)
            direction = precond + step_ratio * direction
            along = applied + step_ratio * along
            norm_now = norm_next
    return (solution[None], residual[None])


def ring(count, step):
    return [(i, (i + step) % count) for i in range(count)]


def lanes_of(rows):
    return lax.broadcasted_iota(jnp.int32, (rows, LANES), 1)


def blocks(total, size, body):
    def step(g, carry):
        body(g * size)
        return carry

    lax.fori_loop(0, total // size, step, 0)


def slots_of(rows):
    return lanes_of(rows) // HALO


RIGHT = tuple((4 + 2 * j) % 8 for j in range(4))
LEFT = tuple((7 + 2 * j) % 8 for j in range(4))


def turned(value, amount):
    return pltpu.roll(value, amount % LANES, 1) if amount % LANES else value


def by_partner(place, values):
    bit = 1
    while bit < len(values):
        swap = (place & bit) != 0
        values = [jnp.where(swap, values[d ^ bit], values[d]) for d in range(len(values))]
        bit *= 2
    return values


def partner_rows(place, count, skip=0):
    return [pl.ds(pl.multiple_of(SUBLANES * (place ^ n) + skip, SUBLANES), SUBLANES) for n in range(count)]


def prepare_kernel(where_ref, force_ref, conduct_ref, diag_ref, ice_ref, ground_ref, *refs):
    count = (len(refs) - 11) // 4
    own_refs, rim_refs, force_own_refs, force_rim_refs = [refs[count * n : count * (n + 1)] for n in range(4)]
    low_ref, high_ref, active_ref, shared_ref, force, conduct, diag, ice, ground, sems, small_sems = refs[4 * count :]
    layers = force.shape[0]
    chunks = sems.shape[0]
    depth = layers // chunks
    small = [
        pltpu.make_async_copy(ice_ref, ice, small_sems.at[0]),
        pltpu.make_async_copy(ground_ref, ground, small_sems.at[1]),
    ]
    copies = []
    for copy in small:
        copy.start()
    for c in range(chunks):
        part = pl.ds(c * depth, depth)
        row = []
        for n, (source, target) in enumerate(((force_ref, force), (conduct_ref, conduct), (diag_ref, diag))):
            copy = pltpu.make_async_copy(source.at[0, part], target.at[part], sems.at[c, n])
            copy.start()
            row.append(copy)
        copies.append(row)
    place = where_ref[1]
    is_ice = jnp.where(where_ref[0] == 0, 1.0, 0.0)
    for copy in small:
        copy.wait()
    ice_cells = ice[...].astype(jnp.float32)
    ground_cells = ground[...].astype(jnp.float32)
    active = ice_cells * (1.0 - (1.0 - is_ice) * ground_cells)
    friction = is_ice * friction_gain * ground_cells * ice_cells
    active_ref[...] = active
    lane = lanes_of(SUBLANES)
    slot = slots_of(SUBLANES)
    half = LANES // 2

    def step(q, total):
        for k in range(3):
            owns, rims_out = (force_own_refs, force_rim_refs) if k == 2 else (own_refs, rim_refs)
            lead = () if k == 2 else (k,)
            low = high = None
            for group in range(2):
                rims = [None] * count
                pair = []
                for j in range(4):
                    layer = q * 8 + group * 4 + j
                    if k == 0:
                        value = jnp.sqrt(conduct[layer].astype(jnp.float32)) * active
                    elif k == 1:
                        value = diag[layer].astype(jnp.float32)
                        if group == 0 and j == 0:
                            value = value + friction * jnp.where(q == 0, 1.0, 0.0)
                    else:
                        value = active * force[layer]
                        total = total + value
                    pieces = [value[:, LANES * p : LANES * (p + 1)] for p in range(count // 2)]
                    halves = [turned(piece, half) for piece in pieces]
                    pair.append((pieces, halves))
                    even = halves if j == 2 else [turned(piece, 32 * j) for piece in pieces]
                    odd = halves if j == 0 else pieces if j == 2 else [turned(piece, half + 32 * j) for piece in pieces]
                    for d in range(count):
                        p = d // 2
                        sources = []
                        if d % 2 == 0:
                            sources.append((RIGHT[j], even[p]))
                            if d:
                                sources.append((LEFT[j], even[p - 1]))
                        else:
                            sources.append((LEFT[j], odd[p]))
                            if d + 1 < count:
                                sources.append((RIGHT[j], odd[p + 1]))
                        for target, source in sources:
                            rims[d] = source if rims[d] is None else jnp.where(slot == target, source, rims[d])
                    if group == 0:
                        first, last, first_slot, last_slot = odd[0], even[-1], RIGHT[j], LEFT[j]
                    else:
                        first, last = turned(pieces[0], 112 + 32 * j), turned(pieces[-1], 80 + 32 * j)
                        first_slot, last_slot = LEFT[j], RIGHT[j]
                    low = first if low is None else jnp.where(slot == first_slot, first, low)
                    high = last if high is None else jnp.where(slot == last_slot, last, high)
                    if j % 2:
                        (even_pieces, even_halves), (odd_pieces, odd_halves) = pair[-2:]
                        packed = []
                        for d in range(count):
                            p = d // 2
                            if d % 2 == 0:
                                packed.append(jnp.where(lane < half, even_pieces[p], odd_halves[p]))
                            else:
                                packed.append(jnp.where(lane < half, even_halves[p], odd_pieces[p]))
                        for ref, packed_value in zip(owns, by_partner(place, packed)):
                            ref[(*lead, q * 4 + group * 2 + j // 2)] = packed_value
                for ref, rim in zip(rims_out, by_partner(place, rims)):
                    ref[(*lead, q * 2 + group)] = rim
            low_ref[k, q] = low
            high_ref[k, q] = high
        return total

    total = jnp.zeros_like(active)
    for c in range(chunks):
        for copy in copies[c]:
            copy.wait()
        total = lax.fori_loop(c * depth // 8, (c + 1) * depth // 8, step, total)
    weight = jnp.sqrt(conduct[where_ref[2]].astype(jnp.float32)) * active
    shared_ref[...] = weight * (total / layers)


def merge_kernel(place_ref, edge_ref, low_ref, high_ref, term_ref, before_ref, after_ref, *refs):
    count = len(refs) // 5
    rims, owns, force_rims, rims_out, force_out = [refs[count * n : count * (n + 1)] for n in range(5)]
    groups = low_ref.shape[1]
    odd = slots_of(SUBLANES) % 2 == 1
    first = [jnp.where(odd, place_ref[0], -1) == k for k in range(count)]
    last = [jnp.where(odd, -1, place_ref[0] ^ (count - 1)) == k for k in range(count)]

    def step(q):
        for k in range(3):
            before, after = low_ref[k, q], high_ref[k, q]
            if k == 0:
                before, after = before * edge_ref[0], after * edge_ref[1]
            befores, afters = (before, turned(before, 48)), (after, turned(after, 80))
            for n in range(count):
                for group in range(2):
                    g = 2 * q + group
                    rim = force_rims[n][g] if k == 2 else rims[n][k, g]
                    rim = jnp.where(last[n], afters[group], jnp.where(first[n], befores[group], rim))
                    if k == 2:
                        force_out[n][4 * groups + g] = rim
                    else:
                        rims_out[n][k, g] = rim
        for n in range(count):
            for m in range(4):
                force_out[n][4 * q + m] = owns[n][4 * q + m]

    def pair(start):
        step(start)
        step(start + 1)

    blocks(groups, 2, pair)
    lane = lanes_of(SUBLANES)
    half = LANES // 2
    pieces = [term_ref[:, LANES * p : LANES * (p + 1)] for p in range(count // 2)]
    halves = [turned(piece, half) for piece in pieces] + [turned(after_ref[...], half)]
    windows = []
    for d in range(count):
        p = d // 2
        if d % 2 == 0:
            own, right, left = pieces[p], pieces[p], pieces[p - 1] if p else before_ref[...]
        else:
            own, right, left = halves[p], halves[p + 1], halves[p]
        outer = jnp.where(lane >= LANES - HALO, left, 0.0)
        windows.append(jnp.where(lane < half, own, jnp.where(lane < half + HALO, right, outer)))
    for ref, value in zip(force_out, by_partner(place_ref[0], windows)):
        ref[6 * groups] = value


def window_of(own, rim, j, fill):
    lane = lanes_of(SUBLANES)
    half = LANES // 2
    inside = (lane < half + HALO) | (lane >= LANES - HALO)
    return jnp.where(lane < half, turned(own, half * (j % 2)), jnp.where(inside, turned(rim, -32 * j), fill))


def two_sum(a, b):
    total = a + b
    part = total - a
    return total, (a - (total - part)) + (b - part)


def add_pairs(high, low, other_high, other_low):
    total, error = two_sum(high, other_high)
    return total, low + other_low + error


def stencil(held_ref, layer, rows):
    def at(shift):
        return held_ref[layer + 1, pl.ds(SUBLANES + shift, rows)]

    here = at(0)
    near = at(1) + at(-1)
    mixed = here + cross_weight * near
    far = at(2) + at(-2) + turned(here, 2) + turned(here, -2)
    beside = near + turned(mixed, 1) + turned(mixed, -1) + far_weight * far
    above = held_ref[layer + 2, pl.ds(SUBLANES, rows)] + held_ref[layer, pl.ds(SUBLANES, rows)]
    return beside + vertical_weight * above


def scale_kernel(place_ref, *refs):
    count = (len(refs) - 4) // 2
    own_refs, rim_refs = refs[:count], refs[count : 2 * count]
    scale_ref, factor_ref, held_ref, base_ref = refs[2 * count :]
    layers, rows = base_ref.shape[:2]
    clear_edges(held_ref, rows)
    places = partner_rows(place_ref[0], count)
    padded = partner_rows(place_ref[0], count, SUBLANES)

    def gather(first):
        for u in range(2):
            g = first + u
            for n in range(count):
                for j in range(4):
                    layer = 4 * g + j
                    coupling, base = [
                        window_of(own_refs[n][k, 2 * g + j // 2], rim_refs[n][k, g], j, 1.0 if k else 0.0)
                        for k in range(2)
                    ]
                    held_ref[layer + 1, padded[n]] = coupling
                    base_ref[layer, places[n]] = base

    blocks(layers // 4, 2, gather)

    def begin(first):
        for layer in range(UNROLL):
            layer = first + layer
            coupling = held_ref[layer + 1, pl.ds(SUBLANES, rows)]
            diagonal = base_ref[layer] + coupling * stencil(held_ref, layer, rows)
            root = jnp.sqrt(diagonal)
            inverse = 1.0 / root
            scale_ref[0, layer] = inverse
            scale_ref[1, layer] = root
            factor_ref[layer] = coupling * inverse

    blocks(layers, UNROLL, begin)


def clear_edges(ref, rows):
    layers = ref.shape[0]
    empty = jnp.zeros((layers, SUBLANES, LANES), jnp.float32)
    ref[:, :SUBLANES] = empty
    ref[:, SUBLANES + rows :] = empty
    ref[0] = jnp.zeros((rows + 2 * SUBLANES, LANES), jnp.float32)
    ref[layers - 1] = jnp.zeros((rows + 2 * SUBLANES, LANES), jnp.float32)


def krylov_kernel(where_ref, scale_ref, factor_ref, *refs):
    count = len(refs) - ITERS - 1 - 4
    force_refs = refs[:count]
    basis = refs[count : count + ITERS + 1]
    sums_ref, even_ref, odd_ref, gram_ref = refs[count + ITERS + 1 :]
    held = (even_ref, odd_ref)
    layers, rows = factor_ref.shape[:2]
    inner = pl.ds(SUBLANES, rows)
    for ref in held:
        clear_edges(ref, rows)
    places = partner_rows(where_ref[1], count)
    padded = partner_rows(where_ref[1], count, SUBLANES)

    def begin(first):
        for u in range(4):
            g = first + u
            for n in range(count):
                term = force_refs[n][3 * layers // 4]
                for j in range(4):
                    layer = 4 * g + j
                    source = window_of(force_refs[n][2 * g + j // 2], force_refs[n][layers // 2 + g], j, 0.0)
                    source = source + term * jnp.where(layer == where_ref[0], 1.0, 0.0)
                    vector = source * scale_ref[0, layer, places[n]]
                    basis[0][layer, places[n]] = vector
                    odd_ref[layer + 1, padded[n]] = factor_ref[layer, places[n]] * vector

    blocks(layers // 4, 4, begin)
    for k in range(ITERS):
        source_ref, target_ref = held[(k + 1) % 2], held[k % 2]

        def apply(first):
            for layer in range(UNROLL):
                layer = first + layer
                factor = factor_ref[layer]
                spread = stencil(source_ref, layer, rows)
                before = basis[k][layer]
                before = (1.0 - SHIFTS[k]) * before if SHIFTS[k] else before
                vector = before - factor * spread
                basis[k + 1][layer] = vector
                if k + 1 < ITERS:
                    target_ref[layer + 1, inner] = factor * vector

        blocks(layers, UNROLL, apply)

    lane = lanes_of(SUBLANES)
    half = LANES // 2
    gram_ref[...] = jnp.zeros(gram_ref.shape, jnp.float32)

    def products(first):
        sums = [None] * len(PAIRS)
        for n in range(0, 8, 2):
            for d in range(rows // SUBLANES):
                part = pl.ds(SUBLANES * d, SUBLANES)
                vectors = [
                    jnp.where(lane < half, ref[first + n, part], turned(ref[first + n + 1, part], half))
                    for ref in basis
                ]
                for p, (i, j) in enumerate(PAIRS):
                    product = vectors[j] * vectors[i]
                    sums[p] = product if sums[p] is None else sums[p] + product
        for p in range(len(PAIRS)):
            high, low = add_pairs(gram_ref[0, p], gram_ref[1, p], sums[p], 0.0)
            gram_ref[0, p] = high
            gram_ref[1, p] = low

    blocks(layers, 8, products)
    high, low = gram_ref[0, :, 0], gram_ref[1, :, 0]
    for row in range(1, SUBLANES):
        high, low = add_pairs(high, low, gram_ref[0, :, row], gram_ref[1, :, row])
    turn = LANES // 2
    while turn:
        high, low = add_pairs(high, low, pltpu.roll(high, turn, 1), pltpu.roll(low, turn, 1))
        turn //= 2
    packed = high[:SUBLANES]
    share = LANES // 4
    for g in range(4):
        part = slice(SUBLANES * g, SUBLANES * (g + 1))
        if g:
            packed = jnp.where(lane >= share * g, high[part], packed)
        packed = jnp.where((lane >= share * g + share // 2) & (lane < share * (g + 1)), low[part], packed)
    for d in range(sums_ref.shape[0]):
        sums_ref[d] = packed


def tree_sum(terms):
    while len(terms) > 1:
        terms = [sum(terms[i : i + 2]) for i in range(0, len(terms), 2)]
    return terms[0]


def quadratic(gram, left, right):
    products = []
    for i, a in enumerate(left):
        inside = [gram[max(i, j), min(i, j)] * b for j, b in enumerate(right)]
        products.append(a * tree_sum(inside))
    return tree_sum(products)


def iterate(gram):
    one = jnp.ones_like(gram[0, 0])
    zero = jnp.zeros_like(one)
    residual, direction, answer = [one], [one], []
    norm = gram[0, 0]
    for iteration in range(ITERS):
        applied = [SHIFTS[k] * c if SHIFTS[k] else zero for k, c in enumerate(direction)] + [zero]
        for k, c in enumerate(direction):
            applied[k + 1] = applied[k + 1] + c
        curve = quadratic(gram, direction, applied)
        step = norm / curve
        answer = [a + step * c for a, c in zip(answer + [zero], direction)]
        residual = [r - step * c for r, c in zip(residual + [zero], applied)]
        if iteration + 1 < ITERS:
            following = quadratic(gram, residual, residual)
            ratio = following / norm
            direction = [r + ratio * c for r, c in zip(residual, direction + [zero])]
            norm = following
    return answer, residual


def solve_kernel(sums_ref, coefs_ref, gram_ref):
    share = LANES // 4
    parts = [(sums_ref[d], turned(sums_ref[d], -share // 2)) for d in range(sums_ref.shape[0])]
    while len(parts) > 1:
        parts = [add_pairs(*parts[i], *parts[i + 1]) if i + 1 < len(parts) else parts[i] for i in range(0, len(parts), 2)]
    gram_ref[...] = parts[0][0] + parts[0][1]
    gram = {
        pair: gram_ref[pl.ds(p % SUBLANES, 1), pl.ds(share * (p // SUBLANES), 1)] for p, pair in enumerate(PAIRS)
    }
    answer, residual = iterate(gram)
    for n, coef in enumerate(answer + residual):
        coefs_ref[n] = jnp.broadcast_to(coef, (SUBLANES, LANES))


def combine_kernel(start, depth, where_ref, coefs_ref, *refs):
    basis = refs[: ITERS + 1]
    scale_ref, *out_refs = refs[ITERS + 1 :]
    half = LANES // 2
    lane = lanes_of(SUBLANES)
    rows = partner_rows(where_ref[1], len(out_refs))

    def mix(first):
        answer = [coefs_ref[n] for n in range(ITERS)]
        residual = [coefs_ref[ITERS + n] for n in range(ITERS + 1)]
        for layer in range(8):
            layer = first + layer
            for ref, part in zip(out_refs, rows):
                vectors = [basis_ref[start + layer, part] for basis_ref in basis]
                answered = tree_sum([c * v for c, v in zip(answer, vectors)]) * scale_ref[0, start + layer, part]
                left = tree_sum([c * v for c, v in zip(residual, vectors)]) * scale_ref[1, start + layer, part]
                ref[layer] = jnp.where(lane < half, answered, turned(left, half))

    blocks(depth, 8, mix)


def finish_kernel(start, depth, count, where_ref, *refs):
    parts = refs[:count]
    solution_ref, residual_ref, solved, left, sems = refs[-5:]
    half = LANES // 2
    lane = lanes_of(SUBLANES)
    copies = []
    for first in range(0, depth, 8):
        for layer in range(first, first + 8):
            got = by_partner(where_ref[1], [ref[layer] for ref in parts])
            for p in range(count // 2):
                place = pl.ds(LANES * p, LANES)
                low, high = got[2 * p : 2 * p + 2]
                solved[layer, :, place] = jnp.where(lane < half, low, turned(high, half))
                left[layer, :, place] = jnp.where(lane < half, turned(low, half), high)
    for n, (held, target) in enumerate(((solved, solution_ref), (left, residual_ref))):
        copy = pltpu.make_async_copy(held, target.at[0, pl.ds(start, depth)], sems.at[n])
        copy.start()
        copies.append(copy)
    for copy in copies:
        copy.wait()


def call(kernel, outs, args, smem=0, hbm=0, tail=0, scratch=(), limit=24, flops=10**6, aliases=None, hbm_outs=False):
    out_space = pltpu.HBM if hbm_outs else pltpu.VMEM
    return pl.pallas_call(
        kernel,
        out_shape=[jax.ShapeDtypeStruct(shape, jnp.float32) for shape in outs],
        in_specs=[pl.BlockSpec(memory_space=pltpu.SMEM)] * smem
        + [pl.BlockSpec(memory_space=pltpu.HBM)] * hbm
        + [pl.BlockSpec(memory_space=pltpu.VMEM)] * (len(args) - smem - hbm - tail)
        + [pl.BlockSpec(memory_space=pltpu.HBM)] * tail,
        out_specs=[pl.BlockSpec(memory_space=out_space)] * len(outs),
        scratch_shapes=[pltpu.VMEM(shape, jnp.float32) if isinstance(shape, tuple) else shape for shape in scratch],
        compiler_params=pltpu.CompilerParams(vmem_limit_bytes=limit * 2**20),
        cost_estimate=pl.CostEstimate(flops=flops, bytes_accessed=0, transcendentals=0),
        input_output_aliases=aliases or {},
    )(*args)


def exchanged(parts):
    count = len(parts)
    return [parts[0]] + [
        lax.ppermute(parts[k], "gx", [(i, i ^ k) for i in range(count)]) for k in range(1, count)
    ]


def in_windows(forcing, conduct, diag_add, ice_mask, grounded):
    _, layers, block_x, block_y = forcing.shape
    count_x, count_y = lax.axis_size("gx"), lax.axis_size("gy")
    rows = count_x * block_x
    group = lax.axis_index("group").astype(jnp.int32)
    place_x = lax.axis_index("gx").astype(jnp.int32)
    place_y = lax.axis_index("gy")
    edge = jnp.where(group == 0, 0, layers - 1).astype(jnp.int32)
    inside = jnp.stack([place_y > 0, place_y < count_y - 1]).astype(jnp.float32)
    own = (layers // 2, block_x, LANES)
    rim = (layers // 4, block_x, LANES)
    side = (3, layers // 8, block_x, LANES)
    block = (layers, block_x, block_y)
    chunks = 5 if layers % 40 == 0 else 1
    where = jnp.stack([edge, place_x])
    forcing, conduct, diag_add, ice_mask, grounded = [
        pltpu.with_memory_space_constraint(x, pltpu.HBM)
        for x in (forcing, conduct, diag_add, ice_mask, grounded)
    ]
    *made, low, high, active, shared = call(
        prepare_kernel,
        [(2, *own)] * count_x + [(2, *rim)] * count_x + [own] * count_x + [rim] * count_x
        + [side] * 2 + [ice_mask.shape] * 2,
        (jnp.stack([group, place_x, edge]), forcing, conduct, diag_add, ice_mask, grounded),
        smem=1, hbm=5,
        scratch=[
            block,
            pltpu.VMEM(block, conduct.dtype),
            pltpu.VMEM(block, diag_add.dtype),
            pltpu.VMEM(ice_mask.shape, ice_mask.dtype),
            pltpu.VMEM(grounded.shape, grounded.dtype),
            pltpu.SemaphoreType.DMA((chunks, 3)),
            pltpu.SemaphoreType.DMA((2,)),
        ],
    )
    owns, *left = [made[count_x * n : count_x * (n + 1)] for n in range(4)]
    owns = exchanged(owns)
    received = from_partner(shared, "group", 0)
    up, down = ring(count_y, 1), ring(count_y, -1)
    before, after = lax.ppermute(high, "gy", up), lax.ppermute(low, "gy", down)
    term = active * received
    term_before = lax.ppermute(term[:, -LANES:], "gy", up)
    term_after = lax.ppermute(term[:, :LANES], "gy", down)
    force = (own[0] + rim[0] + 1, block_x, LANES)
    merged = call(
        merge_kernel, [(2, *rim)] * count_x + [force] * count_x,
        (place_x[None], inside, before, after, term, term_before, term_after, *left[0], *left[1], *left[2]), smem=2,
    )
    rims = exchanged(merged[:count_x])
    forces = exchanged(merged[count_x:])
    padded = (layers + 2, rows + 2 * SUBLANES, LANES)
    window = (layers, rows, LANES)
    scale, factor = call(
        scale_kernel, [(2,) + window, window], (place_x[None], *owns, *rims), smem=1,
        scratch=[padded, window],
    )
    *basis, sums = call(
        krylov_kernel, [window] * (ITERS + 1) + [(count_x * count_y, SUBLANES, LANES)],
        (where, scale, factor, *forces), smem=1,
        scratch=[padded] * 2 + [(2, 32, SUBLANES, LANES)], limit=32,
    )
    sums = lax.all_to_all(sums, ("gx", "gy"), 0, 0, tiled=True)
    (coefs,) = call(solve_kernel, [(2 * ITERS + 1, SUBLANES, LANES)], (sums,), scratch=[(SUBLANES, LANES)])
    depth = layers // PARTS
    arrived = []
    for n in range(PARTS):
        mixed = call(
            functools.partial(combine_kernel, n * depth, depth),
            [(depth, block_x, LANES)] * count_x, (where, coefs, *basis, scale), smem=1,
        )
        arrived.append(exchanged(mixed))
    outs = ()
    for n in range(PARTS):
        outs = tuple(
            call(
                functools.partial(finish_kernel, n * depth, depth, count_x),
                [forcing.shape] * 2, (where, *arrived[n], *outs), smem=1, tail=len(outs), hbm_outs=True,
                scratch=[(depth, block_x, block_y)] * 2 + [pltpu.SemaphoreType.DMA((2,))],
                aliases={1 + count_x + i: i for i in range(len(outs))},
            )
        )
    return outs


def fits_windows(layers, block_x, block_y, count_x):
    width = block_y // count_x
    return (
        layers % (LANES // HALO) == 0
        and block_x == SUBLANES
        and block_y % LANES == 0
        and 2 * width == LANES
        and HALO >= 2 * (ITERS + 1)
    )


def per_device(forcing, conduct, diag_add, ice_mask, grounded):
    _, layers, block_x, block_y = forcing.shape
    if not fits_windows(layers, block_x, block_y, lax.axis_size("gx")):
        return on_device(forcing, conduct, diag_add, ice_mask, grounded)
    return in_windows(forcing, conduct, diag_add, ice_mask, grounded)


def solution(mesh):
    in_specs = (
        P("group", None, "gx", "gy"),
        P("group", None, "gx", "gy"),
        P("group", None, "gx", "gy"),
        P("gx", "gy"),
        P("gx", "gy"),
    )
    out_specs = (P("group", None, "gx", "gy"), P("group", None, "gx", "gy"))
    return jax.shard_map(
        per_device, mesh=mesh, in_specs=in_specs, out_specs=out_specs, check_vma=False
    )
```

```python
import functools
import math

import jax
import jax.numpy as jnp
from jax import lax
from jax.experimental import pallas as pl
from jax.experimental.pallas import tpu as pltpu
from jax.sharding import PartitionSpec as P


ITERS = 6
LANES = 128
SUBLANES = 8
HALO = 16
SHIFTS = (0.0, 0.75, 1.5, 0.25, 1.75, 1.0)
UNROLL = 16
PAIRS = tuple((i, j) for i in range(ITERS + 1) for j in range(i + 1) if j < ITERS)


far_weight = 0.25
cross_weight = 0.5
vertical_weight = 4.0
friction_gain = 8.0
NEIGHBOURS = (
    (1, 0, 1.0),
    (-1, 0, 1.0),
    (0, 1, 1.0),
    (0, -1, 1.0),
    (2, 0, far_weight),
    (-2, 0, far_weight),
    (0, 2, far_weight),
    (0, -2, far_weight),
    (1, 1, cross_weight),
    (1, -1, cross_weight),
    (-1, 1, cross_weight),
    (-1, -1, cross_weight),
)


def with_halo(block, sides, width):
    for axis, dim in sides:
        count = lax.axis_size(axis)
        place = lax.axis_index(axis)
        ahead = [(i, (i + 1) % count) for i in range(count)]
        back = [(target, source) for source, target in ahead]
        low = lax.ppermute(
            lax.slice_in_dim(block, block.shape[dim] - width, None, axis=dim), axis, ahead
        )
        high = lax.ppermute(lax.slice_in_dim(block, 0, width, axis=dim), axis, back)
        low = jnp.where(place > 0, low, 0.0)
        high = jnp.where(place < count - 1, high, 0.0)
        block = jnp.concatenate([low, block, high], axis=dim)
    return block


def from_partner(shard, axis, distance):
    return lax.ppermute(shard, axis, [(i, i ^ 1 << distance) for i in range(lax.axis_size(axis))])


def beside_sum(padded, extent_x, extent_y):
    summed = jnp.zeros((padded.shape[0], extent_x, extent_y), jnp.float32)
    for shift_x, shift_y, weight in NEIGHBOURS:
        summed = (
            summed
            + weight
            * padded[:, 2 + shift_x : 2 + shift_x + extent_x, 2 + shift_y : 2 + shift_y + extent_y]
        )
    return summed


def vertical_sum(values):
    zeroes = jnp.zeros_like(values[:1])
    return jnp.concatenate([values[1:], zeroes], 0) + jnp.concatenate([zeroes, values[:-1]], 0)


def spread_padded(padded, values):
    return beside_sum(padded, values.shape[1], values.shape[2]) + vertical_weight * vertical_sum(
        values
    )


def operate(vector, coupling, diagonal):
    scaled = coupling * vector
    padded = with_halo(scaled, (("gx", 1), ("gy", 2)), 2)
    return diagonal * vector - coupling * spread_padded(padded, scaled)


def sum_over(partial, axes):
    count = math.prod(lax.axis_size(axis) for axis in axes)
    sent = jnp.broadcast_to(partial[None, None], (count, 1) + partial.shape)
    return jnp.sum(lax.all_to_all(sent, axes, 0, 0, tiled=True), axis=(0, 1))


def paired_sums(residual, precond, applied):
    partial = jnp.stack([jnp.sum(residual * precond), jnp.sum(applied * precond)])
    summed = sum_over(partial, ("gx", "gy"))
    return summed[0], summed[1]


def on_device(forcing, conduct, diag_add, ice_mask, grounded):
    own_force = forcing[0]
    layers = own_force.shape[0]
    group_id = lax.axis_index("group")
    is_ice = (group_id == 0).astype(jnp.float32)
    ice_cells = ice_mask.astype(jnp.float32)
    ground_cells = grounded.astype(jnp.float32)
    active = ice_cells * (1.0 - (1.0 - is_ice) * ground_cells)
    coupling = jnp.sqrt(conduct[0].astype(jnp.float32)) * active
    layer_index = lax.broadcasted_iota(jnp.int32, (layers, 1, 1), 0)
    edge_layer = jnp.where(group_id == 0, 0, layers - 1).astype(jnp.int32)
    edge_pick = (layer_index == edge_layer).astype(jnp.float32)
    bottom = (layer_index == 0).astype(jnp.float32)
    base_diag = diag_add[0].astype(jnp.float32) + bottom * (
        is_ice * friction_gain * ground_cells * ice_cells
    )
    padded_coupling = with_halo(coupling, (("gx", 1), ("gy", 2)), 2)
    diagonal = base_diag + coupling * spread_padded(padded_coupling, coupling)
    shared_value = active * jnp.mean(own_force, axis=0)
    shared_weight = lax.dynamic_index_in_dim(coupling, edge_layer, 0, keepdims=False)
    received = from_partner(jnp.stack([shared_value, shared_weight]), "group", 0)
    source = active * own_force + edge_pick * (active * received[1] * received[0])
    inverse = 1.0 / diagonal
    solution = jnp.zeros_like(source)
    residual = source
    precond = inverse * residual
    applied = operate(precond, coupling, diagonal)
    norm_now, curve = paired_sums(residual, precond, applied)
    step_size = norm_now / curve
    direction = precond
    along = applied
    for iteration in range(ITERS):
        solution = solution + step_size * direction
        residual = residual - step_size * along
        if iteration + 1 < ITERS:
            precond = inverse * residual
            applied = operate(precond, coupling, diagonal)
            norm_next, curve = paired_sums(residual, precond, applied)
            step_ratio = norm_next / norm_now
            step_size = norm_next / (curve - step_ratio * norm_next / step_size)
            direction = precond + step_ratio * direction
            along = applied + step_ratio * along
            norm_now = norm_next
    return (solution[None], residual[None])


def ring(count, step):
    return [(i, (i + step) % count) for i in range(count)]


def lanes_of(rows):
    return lax.broadcasted_iota(jnp.int32, (rows, LANES), 1)


def blocks(total, size, body):
    def step(g, carry):
        body(g * size)
        return carry

    lax.fori_loop(0, total // size, step, 0)


def spans(start, stop, size, body):
    def step(g, carry):
        body(start + g * size, size)
        return carry

    whole = (stop - start) // size
    if whole:
        lax.fori_loop(0, whole, step, 0)
    if (stop - start) % size:
        body(start + whole * size, (stop - start) % size)


def slots_of(rows):
    return lanes_of(rows) // HALO


RIGHT = tuple((4 + 2 * j) % 8 for j in range(4))
LEFT = tuple((7 + 2 * j) % 8 for j in range(4))


def turned(value, amount):
    return pltpu.roll(value, amount % LANES, 1) if amount % LANES else value


def by_partner(place, values):
    bit = 1
    while bit < len(values):
        swap = (place & bit) != 0
        values = [jnp.where(swap, values[d ^ bit], values[d]) for d in range(len(values))]
        bit *= 2
    return values


def partner_rows(place, count, skip=0):
    return [pl.ds(pl.multiple_of(SUBLANES * (place ^ n) + skip, SUBLANES), SUBLANES) for n in range(count)]


def prepare_kernel(where_ref, force_ref, conduct_ref, diag_ref, ice_ref, ground_ref, *refs):
    count = (len(refs) - 11) // 4
    own_refs, rim_refs, force_own_refs, force_rim_refs = [refs[count * n : count * (n + 1)] for n in range(4)]
    low_ref, high_ref, active_ref, shared_ref, force, conduct, diag, ice, ground, sems, small_sems = refs[4 * count :]
    layers = force.shape[0]
    chunks = sems.shape[0]
    depth = layers // chunks
    small = [
        pltpu.make_async_copy(ice_ref, ice, small_sems.at[0]),
        pltpu.make_async_copy(ground_ref, ground, small_sems.at[1]),
    ]
    copies = []
    for copy in small:
        copy.start()
    for c in range(chunks):
        part = pl.ds(c * depth, depth)
        row = []
        for n, (source, target) in enumerate(((force_ref, force), (conduct_ref, conduct), (diag_ref, diag))):
            copy = pltpu.make_async_copy(source.at[0, part], target.at[part], sems.at[c, n])
            copy.start()
            row.append(copy)
        copies.append(row)
    place = where_ref[1]
    is_ice = jnp.where(where_ref[0] == 0, 1.0, 0.0)
    for copy in small:
        copy.wait()
    ice_cells = ice[...].astype(jnp.float32)
    ground_cells = ground[...].astype(jnp.float32)
    active = ice_cells * (1.0 - (1.0 - is_ice) * ground_cells)
    friction = is_ice * friction_gain * ground_cells * ice_cells
    active_ref[...] = active
    lane = lanes_of(SUBLANES)
    slot = slots_of(SUBLANES)
    half = LANES // 2

    def step(q, total):
        for k in range(3):
            owns, rims_out = (force_own_refs, force_rim_refs) if k == 2 else (own_refs, rim_refs)
            lead = () if k == 2 else (k,)
            low = high = None
            for group in range(2):
                rims = [None] * count
                pair = []
                for j in range(4):
                    layer = q * 8 + group * 4 + j
                    if k == 0:
                        value = jnp.sqrt(conduct[layer].astype(jnp.float32)) * active
                    elif k == 1:
                        value = diag[layer].astype(jnp.float32)
                        if group == 0 and j == 0:
                            value = value + friction * jnp.where(q == 0, 1.0, 0.0)
                    else:
                        value = active * force[layer]
                        total = total + value
                    pieces = [value[:, LANES * p : LANES * (p + 1)] for p in range(count // 2)]
                    halves = [turned(piece, half) for piece in pieces]
                    pair.append((pieces, halves))
                    even = halves if j == 2 else [turned(piece, 32 * j) for piece in pieces]
                    odd = halves if j == 0 else pieces if j == 2 else [turned(piece, half + 32 * j) for piece in pieces]
                    for d in range(count):
                        p = d // 2
                        sources = []
                        if d % 2 == 0:
                            sources.append((RIGHT[j], even[p]))
                            if d:
                                sources.append((LEFT[j], even[p - 1]))
                        else:
                            sources.append((LEFT[j], odd[p]))
                            if d + 1 < count:
                                sources.append((RIGHT[j], odd[p + 1]))
                        for target, source in sources:
                            rims[d] = source if rims[d] is None else jnp.where(slot == target, source, rims[d])
                    if group == 0:
                        first, last, first_slot, last_slot = odd[0], even[-1], RIGHT[j], LEFT[j]
                    else:
                        first, last = turned(pieces[0], 112 + 32 * j), turned(pieces[-1], 80 + 32 * j)
                        first_slot, last_slot = LEFT[j], RIGHT[j]
                    low = first if low is None else jnp.where(slot == first_slot, first, low)
                    high = last if high is None else jnp.where(slot == last_slot, last, high)
                    if j % 2:
                        (even_pieces, even_halves), (odd_pieces, odd_halves) = pair[-2:]
                        packed = []
                        for d in range(count):
                            p = d // 2
                            if d % 2 == 0:
                                packed.append(jnp.where(lane < half, even_pieces[p], odd_halves[p]))
                            else:
                                packed.append(jnp.where(lane < half, even_halves[p], odd_pieces[p]))
                        for ref, packed_value in zip(owns, by_partner(place, packed)):
                            ref[(*lead, q * 4 + group * 2 + j // 2)] = packed_value
                for ref, rim in zip(rims_out, by_partner(place, rims)):
                    ref[(*lead, q * 2 + group)] = rim
            low_ref[k, q] = low
            high_ref[k, q] = high
        return total

    total = jnp.zeros_like(active)
    for c in range(chunks):
        for copy in copies[c]:
            copy.wait()
        total = lax.fori_loop(c * depth // 8, (c + 1) * depth // 8, step, total)
    weight = jnp.sqrt(conduct[where_ref[2]].astype(jnp.float32)) * active
    shared_ref[...] = weight * (total / layers)


def merge_kernel(place_ref, edge_ref, low_ref, high_ref, term_ref, before_ref, after_ref, *refs):
    count = len(refs) // 6
    rims, owns, force_rims, rims_out, *force_out = [refs[count * n : count * (n + 1)] for n in range(6)]
    groups = low_ref.shape[1]
    half_groups = groups // 2
    odd = slots_of(SUBLANES) % 2 == 1
    first = [jnp.where(odd, place_ref[0], -1) == k for k in range(count)]
    last = [jnp.where(odd, -1, place_ref[0] ^ (count - 1)) == k for k in range(count)]

    def step(side, i):
        q = side * half_groups + i
        out = force_out[side]
        for k in range(3):
            before, after = low_ref[k, q], high_ref[k, q]
            if k == 0:
                before, after = before * edge_ref[0], after * edge_ref[1]
            befores, afters = (before, turned(before, 48)), (after, turned(after, 80))
            for n in range(count):
                for group in range(2):
                    g = 2 * q + group
                    rim = force_rims[n][g] if k == 2 else rims[n][k, g]
                    rim = jnp.where(last[n], afters[group], jnp.where(first[n], befores[group], rim))
                    if k == 2:
                        out[n][4 * half_groups + 2 * i + group] = rim
                    else:
                        rims_out[n][k, g] = rim
        for n in range(count):
            for m in range(4):
                out[n][4 * i + m] = owns[n][4 * q + m]

    for i in range(half_groups):
        step(0, i)
        step(1, i)
    lane = lanes_of(SUBLANES)
    half = LANES // 2
    pieces = [term_ref[:, LANES * p : LANES * (p + 1)] for p in range(count // 2)]
    halves = [turned(piece, half) for piece in pieces] + [turned(after_ref[...], half)]
    windows = []
    for d in range(count):
        p = d // 2
        if d % 2 == 0:
            own, right, left = pieces[p], pieces[p], pieces[p - 1] if p else before_ref[...]
        else:
            own, right, left = halves[p], halves[p + 1], halves[p]
        outer = jnp.where(lane >= LANES - HALO, left, 0.0)
        windows.append(jnp.where(lane < half, own, jnp.where(lane < half + HALO, right, outer)))
    for n, value in enumerate(by_partner(place_ref[0], windows)):
        force_out[0][n][6 * half_groups] = value
        force_out[1][n][6 * half_groups] = value


def window_of(own, rim, j, fill):
    lane = lanes_of(SUBLANES)
    half = LANES // 2
    inside = (lane < half + HALO) | (lane >= LANES - HALO)
    return jnp.where(lane < half, turned(own, half * (j % 2)), jnp.where(inside, turned(rim, -32 * j), fill))


def two_sum(a, b):
    total = a + b
    part = total - a
    return total, (a - (total - part)) + (b - part)


def add_pairs(high, low, other_high, other_low):
    total, error = two_sum(high, other_high)
    return total, low + other_low + error


def stencil(held_ref, layer, rows):
    def at(shift):
        return held_ref[layer + 1, pl.ds(SUBLANES + shift, rows)]

    here = at(0)
    near = at(1) + at(-1)
    mixed = here + cross_weight * near
    far = at(2) + at(-2) + turned(here, 2) + turned(here, -2)
    beside = near + turned(mixed, 1) + turned(mixed, -1) + far_weight * far
    above = held_ref[layer + 2, pl.ds(SUBLANES, rows)] + held_ref[layer, pl.ds(SUBLANES, rows)]
    return beside + vertical_weight * above


def scale_kernel(place_ref, *refs):
    count = (len(refs) - 4) // 2
    own_refs, rim_refs = refs[:count], refs[count : 2 * count]
    scale_ref, factor_ref, held_ref, base_ref = refs[2 * count :]
    layers, rows = base_ref.shape[:2]
    clear_edges(held_ref, rows)
    places = partner_rows(place_ref[0], count)
    padded = partner_rows(place_ref[0], count, SUBLANES)

    def gather(first):
        for u in range(2):
            g = first + u
            for n in range(count):
                for j in range(4):
                    layer = 4 * g + j
                    coupling, base = [
                        window_of(own_refs[n][k, 2 * g + j // 2], rim_refs[n][k, g], j, 1.0 if k else 0.0)
                        for k in range(2)
                    ]
                    held_ref[layer + 1, padded[n]] = coupling
                    base_ref[layer, places[n]] = base

    blocks(layers // 4, 2, gather)

    def begin(first):
        for layer in range(UNROLL):
            layer = first + layer
            coupling = held_ref[layer + 1, pl.ds(SUBLANES, rows)]
            diagonal = base_ref[layer] + coupling * stencil(held_ref, layer, rows)
            root = jnp.sqrt(diagonal)
            inverse = 1.0 / root
            scale_ref[0, layer] = inverse
            scale_ref[1, layer] = root
            factor_ref[layer] = coupling * inverse

    blocks(layers, UNROLL, begin)


def clear_edges(ref, rows):
    layers = ref.shape[0]
    empty = jnp.zeros((layers, SUBLANES, LANES), jnp.float32)
    ref[:, :SUBLANES] = empty
    ref[:, SUBLANES + rows :] = empty
    ref[0] = jnp.zeros((rows + 2 * SUBLANES, LANES), jnp.float32)
    ref[layers - 1] = jnp.zeros((rows + 2 * SUBLANES, LANES), jnp.float32)


def begin_part(where_ref, scale_ref, factor_ref, force_refs, vector_ref, held_ref, start, origin):
    count = len(force_refs)
    groups = (force_refs[0].shape[0] - 1) // 3
    places = partner_rows(where_ref[1], count)
    padded = partner_rows(where_ref[1], count, SUBLANES)

    def begin(first, number):
        for u in range(number):
            g = first + u
            for n in range(count):
                term = force_refs[n][3 * groups]
                for j in range(4):
                    layer = start + 4 * g + j
                    source = window_of(force_refs[n][2 * g + j // 2], force_refs[n][2 * groups + g], j, 0.0)
                    source = source + term * jnp.where(layer == where_ref[0], 1.0, 0.0)
                    vector = source * scale_ref[0, layer, places[n]]
                    vector_ref[layer - origin, places[n]] = vector
                    held_ref[layer - origin + 1, padded[n]] = factor_ref[layer, places[n]] * vector

    spans(0, groups, 4, begin)


def apply_part(k, factor_ref, basis, held, start, stop, origin):
    rows = factor_ref.shape[1]
    source_ref, target_ref = held[k % 2], held[(k + 1) % 2]

    def apply(first, number):
        for layer in range(number):
            layer = first + layer
            factor = factor_ref[layer]
            spread = stencil(source_ref, layer - origin, rows)
            before = basis[k][layer - origin]
            before = (1.0 - SHIFTS[k]) * before if SHIFTS[k] else before
            vector = before - factor * spread
            basis[k + 1][layer - origin] = vector
            if k + 1 < ITERS:
                target_ref[layer - origin + 1, pl.ds(SUBLANES, rows)] = factor * vector

    spans(start, stop, UNROLL, apply)


def products_part(basis, gram_ref, layers):
    rows = basis[0].shape[1]
    lane = lanes_of(SUBLANES)
    half = LANES // 2

    def products(first):
        sums = [None] * len(PAIRS)
        for n in range(0, 8, 2):
            for d in range(rows // SUBLANES):
                part = pl.ds(SUBLANES * d, SUBLANES)
                vectors = [
                    jnp.where(lane < half, ref[first + n, part], turned(ref[first + n + 1, part], half))
                    for ref in basis
                ]
                for p, (i, j) in enumerate(PAIRS):
                    product = vectors[j] * vectors[i]
                    sums[p] = product if sums[p] is None else sums[p] + product
        for p in range(len(PAIRS)):
            high, low = add_pairs(gram_ref[0, p], gram_ref[1, p], sums[p], 0.0)
            gram_ref[0, p] = high
            gram_ref[1, p] = low

    blocks(layers, 8, products)


def lower_kernel(where_ref, scale_ref, factor_ref, *refs):
    count = len(refs) - ITERS - 1 - 3
    basis = refs[count : count + ITERS + 1]
    gram_ref, *held = refs[count + ITERS + 1 :]
    half, rows = basis[0].shape[:2]
    for ref in held:
        clear_edges(ref, rows)
    begin_part(where_ref, scale_ref, factor_ref, refs[:count], basis[0], held[0], 0, 0)
    for k in range(ITERS):
        apply_part(k, factor_ref, basis, held, 0, half - 1 - k, 0)
    gram_ref[...] = jnp.zeros(gram_ref.shape, jnp.float32)
    products_part(basis, gram_ref, half - 8)


def upper_kernel(where_ref, scale_ref, factor_ref, *refs):
    count = len(refs) - 2 * (ITERS + 1) - 5
    below = refs[count : count + ITERS + 1]
    part_ref = refs[count + ITERS + 1]
    basis = refs[count + ITERS + 2 : count + 2 * ITERS + 3]
    sums_ref, gram_ref, *held = refs[count + 2 * ITERS + 3 :]
    half, rows = below[0].shape[:2]
    layers = factor_ref.shape[0]
    origin = half - 8
    lane = lanes_of(SUBLANES)
    for ref in held:
        clear_edges(ref, rows)
    for k in range(ITERS + 1):
        for layer in range(origin, half - k):
            basis[k][layer - origin] = below[k][layer]
    begin_part(where_ref, scale_ref, factor_ref, refs[:count], basis[0], held[0], half, origin)
    for k in range(ITERS):
        for layer in (half - k - 2, half - k - 1):
            held[k % 2][layer - origin + 1, pl.ds(SUBLANES, rows)] = factor_ref[layer] * below[k][layer]
        apply_part(k, factor_ref, basis, held, half - 1 - k, layers, origin)
    gram_ref[...] = part_ref[...]
    products_part(basis, gram_ref, layers - origin)
    high, low = gram_ref[0, :, 0], gram_ref[1, :, 0]
    for row in range(1, SUBLANES):
        high, low = add_pairs(high, low, gram_ref[0, :, row], gram_ref[1, :, row])
    turn = LANES // 2
    while turn:
        high, low = add_pairs(high, low, pltpu.roll(high, turn, 1), pltpu.roll(low, turn, 1))
        turn //= 2
    packed = high[:SUBLANES]
    share = LANES // 4
    for g in range(4):
        part = slice(SUBLANES * g, SUBLANES * (g + 1))
        if g:
            packed = jnp.where(lane >= share * g, high[part], packed)
        packed = jnp.where((lane >= share * g + share // 2) & (lane < share * (g + 1)), low[part], packed)
    for d in range(sums_ref.shape[0]):
        sums_ref[d] = packed


def tree_sum(terms):
    while len(terms) > 1:
        terms = [sum(terms[i : i + 2]) for i in range(0, len(terms), 2)]
    return terms[0]


def quadratic(gram, left, right):
    products = []
    for i, a in enumerate(left):
        inside = [gram[max(i, j), min(i, j)] * b for j, b in enumerate(right)]
        products.append(a * tree_sum(inside))
    return tree_sum(products)


def iterate(gram):
    one = jnp.ones_like(gram[0, 0])
    zero = jnp.zeros_like(one)
    residual, direction, answer = [one], [one], []
    norm = gram[0, 0]
    for iteration in range(ITERS):
        applied = [SHIFTS[k] * c if SHIFTS[k] else zero for k, c in enumerate(direction)] + [zero]
        for k, c in enumerate(direction):
            applied[k + 1] = applied[k + 1] + c
        curve = quadratic(gram, direction, applied)
        step = norm / curve
        answer = [a + step * c for a, c in zip(answer + [zero], direction)]
        residual = [r - step * c for r, c in zip(residual + [zero], applied)]
        if iteration + 1 < ITERS:
            following = quadratic(gram, residual, residual)
            ratio = following / norm
            direction = [r + ratio * c for r, c in zip(residual, direction + [zero])]
            norm = following
    return answer, residual


def solve_kernel(sums_ref, coefs_ref, gram_ref):
    share = LANES // 4
    parts = [(sums_ref[d], turned(sums_ref[d], -share // 2)) for d in range(sums_ref.shape[0])]
    while len(parts) > 1:
        parts = [add_pairs(*parts[i], *parts[i + 1]) if i + 1 < len(parts) else parts[i] for i in range(0, len(parts), 2)]
    gram_ref[...] = parts[0][0] + parts[0][1]
    gram = {
        pair: gram_ref[pl.ds(p % SUBLANES, 1), pl.ds(share * (p // SUBLANES), 1)] for p, pair in enumerate(PAIRS)
    }
    answer, residual = iterate(gram)
    for n, coef in enumerate(answer + residual):
        coefs_ref[n] = jnp.broadcast_to(coef, (SUBLANES, LANES))


def combine_kernel(start, depth, where_ref, coefs_ref, *refs):
    basis = refs[: ITERS + 1]
    scale_ref, *out_refs = refs[ITERS + 1 :]
    half = LANES // 2
    lane = lanes_of(SUBLANES)
    rows = partner_rows(where_ref[1], len(out_refs))

    def mix(first):
        answer = [coefs_ref[n] for n in range(ITERS)]
        residual = [coefs_ref[ITERS + n] for n in range(ITERS + 1)]
        for layer in range(8):
            layer = first + layer
            for ref, part in zip(out_refs, rows):
                vectors = [basis_ref[layer, part] for basis_ref in basis]
                answered = tree_sum([c * v for c, v in zip(answer, vectors)]) * scale_ref[0, start + layer, part]
                left = tree_sum([c * v for c, v in zip(residual, vectors)]) * scale_ref[1, start + layer, part]
                ref[layer] = jnp.where(lane < half, answered, turned(left, half))

    blocks(depth, 8, mix)


def finish_kernel(start, depth, count, where_ref, *refs):
    parts = refs[:count]
    solution_ref, residual_ref, solved, left, sems = refs[-5:]
    half = LANES // 2
    lane = lanes_of(SUBLANES)
    copies = []
    for first in range(0, depth, 8):
        for layer in range(first, first + 8):
            got = by_partner(where_ref[1], [ref[layer] for ref in parts])
            for p in range(count // 2):
                place = pl.ds(LANES * p, LANES)
                low, high = got[2 * p : 2 * p + 2]
                solved[layer, :, place] = jnp.where(lane < half, low, turned(high, half))
                left[layer, :, place] = jnp.where(lane < half, turned(low, half), high)
        for n, (held, target) in enumerate(((solved, solution_ref), (left, residual_ref))):
            copy = pltpu.make_async_copy(
                held.at[pl.ds(first, 8)], target.at[0, pl.ds(start + first, 8)], sems.at[n, first // 8]
            )
            copy.start()
            copies.append(copy)
    for copy in copies:
        copy.wait()


def call(kernel, outs, args, smem=0, hbm=0, tail=0, scratch=(), limit=24, flops=10**6, aliases=None, hbm_outs=False):
    out_space = pltpu.HBM if hbm_outs else pltpu.VMEM
    return pl.pallas_call(
        kernel,
        out_shape=[jax.ShapeDtypeStruct(shape, jnp.float32) for shape in outs],
        in_specs=[pl.BlockSpec(memory_space=pltpu.SMEM)] * smem
        + [pl.BlockSpec(memory_space=pltpu.HBM)] * hbm
        + [pl.BlockSpec(memory_space=pltpu.VMEM)] * (len(args) - smem - hbm - tail)
        + [pl.BlockSpec(memory_space=pltpu.HBM)] * tail,
        out_specs=[pl.BlockSpec(memory_space=out_space)] * len(outs),
        scratch_shapes=[pltpu.VMEM(shape, jnp.float32) if isinstance(shape, tuple) else shape for shape in scratch],
        compiler_params=pltpu.CompilerParams(vmem_limit_bytes=limit * 2**20),
        cost_estimate=pl.CostEstimate(flops=flops, bytes_accessed=0, transcendentals=0),
        input_output_aliases=aliases or {},
    )(*args)


def exchanged(parts):
    count = len(parts)
    return [parts[0]] + [
        lax.ppermute(parts[k], "gx", [(i, i ^ k) for i in range(count)]) for k in range(1, count)
    ]


def in_windows(forcing, conduct, diag_add, ice_mask, grounded):
    _, layers, block_x, block_y = forcing.shape
    count_x, count_y = lax.axis_size("gx"), lax.axis_size("gy")
    rows = count_x * block_x
    group = lax.axis_index("group").astype(jnp.int32)
    place_x = lax.axis_index("gx").astype(jnp.int32)
    place_y = lax.axis_index("gy")
    edge = jnp.where(group == 0, 0, layers - 1).astype(jnp.int32)
    inside = jnp.stack([place_y > 0, place_y < count_y - 1]).astype(jnp.float32)
    own = (layers // 2, block_x, LANES)
    rim = (layers // 4, block_x, LANES)
    side = (3, layers // 8, block_x, LANES)
    block = (layers, block_x, block_y)
    chunks = 5 if layers % 40 == 0 else 1
    where = jnp.stack([edge, place_x])
    forcing, conduct, diag_add, ice_mask, grounded = [
        pltpu.with_memory_space_constraint(x, pltpu.HBM)
        for x in (forcing, conduct, diag_add, ice_mask, grounded)
    ]
    *made, low, high, active, shared = call(
        prepare_kernel,
        [(2, *own)] * count_x + [(2, *rim)] * count_x + [own] * count_x + [rim] * count_x
        + [side] * 2 + [ice_mask.shape] * 2,
        (jnp.stack([group, place_x, edge]), forcing, conduct, diag_add, ice_mask, grounded),
        smem=1, hbm=5,
        scratch=[
            block,
            pltpu.VMEM(block, conduct.dtype),
            pltpu.VMEM(block, diag_add.dtype),
            pltpu.VMEM(ice_mask.shape, ice_mask.dtype),
            pltpu.VMEM(grounded.shape, grounded.dtype),
            pltpu.SemaphoreType.DMA((chunks, 3)),
            pltpu.SemaphoreType.DMA((2,)),
        ],
    )
    owns, *left = [made[count_x * n : count_x * (n + 1)] for n in range(4)]
    owns = exchanged(owns)
    received = from_partner(shared, "group", 0)
    up, down = ring(count_y, 1), ring(count_y, -1)
    before, after = lax.ppermute(high, "gy", up), lax.ppermute(low, "gy", down)
    term = active * received
    term_before = lax.ppermute(term[:, -LANES:], "gy", up)
    term_after = lax.ppermute(term[:, :LANES], "gy", down)
    force = ((own[0] + rim[0]) // 2 + 1, block_x, LANES)
    merged = call(
        merge_kernel, [(2, *rim)] * count_x + [force] * 2 * count_x,
        (place_x[None], inside, before, after, term, term_before, term_after, *left[0], *left[1], *left[2]), smem=2,
    )
    rims = exchanged(merged[:count_x])
    forces = []
    for n in range(2):
        forces.append(exchanged(merged[count_x * (n + 1) : count_x * (n + 2)]))
    padded = (layers + 2, rows + 2 * SUBLANES, LANES)
    window = (layers, rows, LANES)
    scale, factor = call(
        scale_kernel, [(2,) + window, window], (place_x[None], *owns, *rims), smem=1,
        scratch=[padded, window],
    )
    half = layers // 2
    depths = (half - 8, layers - half + 8)
    gram = (2, 32, SUBLANES, LANES)
    *below, part = call(
        lower_kernel, [(half, rows, LANES)] * (ITERS + 1) + [gram],
        (where, scale, factor, *forces[0]), smem=1, scratch=[(half + 2,) + padded[1:]] * 2, limit=32,
    )
    *beyond, sums = call(
        upper_kernel,
        [(depths[1], rows, LANES)] * (ITERS + 1) + [(count_x * count_y, SUBLANES, LANES)],
        (where, scale, factor, *forces[1], *below, part), smem=1,
        scratch=[gram] + [(depths[1] + 2,) + padded[1:]] * 2, limit=32,
    )
    sums = lax.all_to_all(sums, ("gx", "gy"), 0, 0, tiled=True)
    (coefs,) = call(solve_kernel, [(2 * ITERS + 1, SUBLANES, LANES)], (sums,), scratch=[(SUBLANES, LANES)])
    starts = (0, depths[0])
    arrived = []
    for start, depth, basis in zip(starts, depths, (below, beyond)):
        mixed = call(
            functools.partial(combine_kernel, start, depth),
            [(depth, block_x, LANES)] * count_x, (where, coefs, *basis, scale), smem=1,
        )
        arrived.append(exchanged(mixed))
    outs = ()
    for n, (start, depth) in enumerate(zip(starts, depths)):
        outs = tuple(
            call(
                functools.partial(finish_kernel, start, depth, count_x),
                [forcing.shape] * 2, (where, *arrived[n], *outs), smem=1, tail=len(outs), hbm_outs=True,
                scratch=[(depth, block_x, block_y)] * 2 + [pltpu.SemaphoreType.DMA((2, depth // 8))],
                aliases={1 + count_x + i: i for i in range(len(outs))},
            )
        )
    return outs


def fits_windows(layers, block_x, block_y, count_x):
    width = block_y // count_x
    return (
        layers % 16 == 0
        and layers >= 32
        and block_x == SUBLANES
        and block_y % LANES == 0
        and 2 * width == LANES
        and HALO >= 2 * (ITERS + 1)
    )


def per_device(forcing, conduct, diag_add, ice_mask, grounded):
    _, layers, block_x, block_y = forcing.shape
    if not fits_windows(layers, block_x, block_y, lax.axis_size("gx")):
        return on_device(forcing, conduct, diag_add, ice_mask, grounded)
    return in_windows(forcing, conduct, diag_add, ice_mask, grounded)


def solution(mesh):
    in_specs = (
        P("group", None, "gx", "gy"),
        P("group", None, "gx", "gy"),
        P("group", None, "gx", "gy"),
        P("gx", "gy"),
        P("gx", "gy"),
    )
    out_specs = (P("group", None, "gx", "gy"), P("group", None, "gx", "gy"))
    return jax.shard_map(
        per_device, mesh=mesh, in_specs=in_specs, out_specs=out_specs, check_vma=False
    )
```

```python
import functools
import math

import jax
import jax.numpy as jnp
from jax import lax
from jax.experimental import pallas as pl
from jax.experimental.pallas import tpu as pltpu
from jax.sharding import PartitionSpec as P


ITERS = 6
LANES = 128
SUBLANES = 8
HALO = 16
SHIFTS = (0.0, 0.75, 1.5, 0.25, 1.75, 1.0)
UNROLL = 16
PAIRS = tuple((i, j) for i in range(ITERS + 1) for j in range(i + 1) if j < ITERS)


far_weight = 0.25
cross_weight = 0.5
vertical_weight = 4.0
friction_gain = 8.0
NEIGHBOURS = (
    (1, 0, 1.0),
    (-1, 0, 1.0),
    (0, 1, 1.0),
    (0, -1, 1.0),
    (2, 0, far_weight),
    (-2, 0, far_weight),
    (0, 2, far_weight),
    (0, -2, far_weight),
    (1, 1, cross_weight),
    (1, -1, cross_weight),
    (-1, 1, cross_weight),
    (-1, -1, cross_weight),
)


def with_halo(block, sides, width):
    for axis, dim in sides:
        count = lax.axis_size(axis)
        place = lax.axis_index(axis)
        ahead = [(i, (i + 1) % count) for i in range(count)]
        back = [(target, source) for source, target in ahead]
        low = lax.ppermute(
            lax.slice_in_dim(block, block.shape[dim] - width, None, axis=dim), axis, ahead
        )
        high = lax.ppermute(lax.slice_in_dim(block, 0, width, axis=dim), axis, back)
        low = jnp.where(place > 0, low, 0.0)
        high = jnp.where(place < count - 1, high, 0.0)
        block = jnp.concatenate([low, block, high], axis=dim)
    return block


def from_partner(shard, axis, distance):
    return lax.ppermute(shard, axis, [(i, i ^ 1 << distance) for i in range(lax.axis_size(axis))])


def beside_sum(padded, extent_x, extent_y):
    summed = jnp.zeros((padded.shape[0], extent_x, extent_y), jnp.float32)
    for shift_x, shift_y, weight in NEIGHBOURS:
        summed = (
            summed
            + weight
            * padded[:, 2 + shift_x : 2 + shift_x + extent_x, 2 + shift_y : 2 + shift_y + extent_y]
        )
    return summed


def vertical_sum(values):
    zeroes = jnp.zeros_like(values[:1])
    return jnp.concatenate([values[1:], zeroes], 0) + jnp.concatenate([zeroes, values[:-1]], 0)


def spread_padded(padded, values):
    return beside_sum(padded, values.shape[1], values.shape[2]) + vertical_weight * vertical_sum(
        values
    )


def operate(vector, coupling, diagonal):
    scaled = coupling * vector
    padded = with_halo(scaled, (("gx", 1), ("gy", 2)), 2)
    return diagonal * vector - coupling * spread_padded(padded, scaled)


def sum_over(partial, axes):
    count = math.prod(lax.axis_size(axis) for axis in axes)
    sent = jnp.broadcast_to(partial[None, None], (count, 1) + partial.shape)
    return jnp.sum(lax.all_to_all(sent, axes, 0, 0, tiled=True), axis=(0, 1))


def paired_sums(residual, precond, applied):
    partial = jnp.stack([jnp.sum(residual * precond), jnp.sum(applied * precond)])
    summed = sum_over(partial, ("gx", "gy"))
    return summed[0], summed[1]


def on_device(forcing, conduct, diag_add, ice_mask, grounded):
    own_force = forcing[0]
    layers = own_force.shape[0]
    group_id = lax.axis_index("group")
    is_ice = (group_id == 0).astype(jnp.float32)
    ice_cells = ice_mask.astype(jnp.float32)
    ground_cells = grounded.astype(jnp.float32)
    active = ice_cells * (1.0 - (1.0 - is_ice) * ground_cells)
    coupling = jnp.sqrt(conduct[0].astype(jnp.float32)) * active
    layer_index = lax.broadcasted_iota(jnp.int32, (layers, 1, 1), 0)
    edge_layer = jnp.where(group_id == 0, 0, layers - 1).astype(jnp.int32)
    edge_pick = (layer_index == edge_layer).astype(jnp.float32)
    bottom = (layer_index == 0).astype(jnp.float32)
    base_diag = diag_add[0].astype(jnp.float32) + bottom * (
        is_ice * friction_gain * ground_cells * ice_cells
    )
    padded_coupling = with_halo(coupling, (("gx", 1), ("gy", 2)), 2)
    diagonal = base_diag + coupling * spread_padded(padded_coupling, coupling)
    shared_value = active * jnp.mean(own_force, axis=0)
    shared_weight = lax.dynamic_index_in_dim(coupling, edge_layer, 0, keepdims=False)
    received = from_partner(jnp.stack([shared_value, shared_weight]), "group", 0)
    source = active * own_force + edge_pick * (active * received[1] * received[0])
    inverse = 1.0 / diagonal
    solution = jnp.zeros_like(source)
    residual = source
    precond = inverse * residual
    applied = operate(precond, coupling, diagonal)
    norm_now, curve = paired_sums(residual, precond, applied)
    step_size = norm_now / curve
    direction = precond
    along = applied
    for iteration in range(ITERS):
        solution = solution + step_size * direction
        residual = residual - step_size * along
        if iteration + 1 < ITERS:
            precond = inverse * residual
            applied = operate(precond, coupling, diagonal)
            norm_next, curve = paired_sums(residual, precond, applied)
            step_ratio = norm_next / norm_now
            step_size = norm_next / (curve - step_ratio * norm_next / step_size)
            direction = precond + step_ratio * direction
            along = applied + step_ratio * along
            norm_now = norm_next
    return (solution[None], residual[None])


def ring(count, step):
    return [(i, (i + step) % count) for i in range(count)]


def lanes_of(rows):
    return lax.broadcasted_iota(jnp.int32, (rows, LANES), 1)


def blocks(total, size, body):
    def step(g, carry):
        body(g * size)
        return carry

    lax.fori_loop(0, total // size, step, 0)


def spans(start, stop, size, body):
    def step(g, carry):
        body(start + g * size, size)
        return carry

    whole = (stop - start) // size
    if whole:
        lax.fori_loop(0, whole, step, 0)
    if (stop - start) % size:
        body(start + whole * size, (stop - start) % size)


def slots_of(rows):
    return lanes_of(rows) // HALO


RIGHT = tuple((4 + 2 * j) % 8 for j in range(4))
LEFT = tuple((7 + 2 * j) % 8 for j in range(4))


def turned(value, amount):
    return pltpu.roll(value, amount % LANES, 1) if amount % LANES else value


def by_partner(place, values):
    bit = 1
    while bit < len(values):
        swap = (place & bit) != 0
        values = [jnp.where(swap, values[d ^ bit], values[d]) for d in range(len(values))]
        bit *= 2
    return values


def partner_rows(place, count, skip=0):
    return [pl.ds(pl.multiple_of(SUBLANES * (place ^ n) + skip, SUBLANES), SUBLANES) for n in range(count)]


def prepare_kernel(where_ref, force_ref, conduct_ref, diag_ref, ice_ref, ground_ref, *refs):
    count = (len(refs) - 11) // 4
    own_refs, rim_refs, force_own_refs, force_rim_refs = [refs[count * n : count * (n + 1)] for n in range(4)]
    low_ref, high_ref, active_ref, shared_ref, force, conduct, diag, ice, ground, sems, small_sems = refs[4 * count :]
    layers = force.shape[0]
    chunks = sems.shape[0]
    depth = layers // chunks
    small = [
        pltpu.make_async_copy(ice_ref, ice, small_sems.at[0]),
        pltpu.make_async_copy(ground_ref, ground, small_sems.at[1]),
    ]
    copies = []
    for copy in small:
        copy.start()
    for c in range(chunks):
        part = pl.ds(c * depth, depth)
        row = []
        for n, (source, target) in enumerate(((force_ref, force), (conduct_ref, conduct), (diag_ref, diag))):
            copy = pltpu.make_async_copy(source.at[0, part], target.at[part], sems.at[c, n])
            copy.start()
            row.append(copy)
        copies.append(row)
    place = where_ref[1]
    is_ice = jnp.where(where_ref[0] == 0, 1.0, 0.0)
    for copy in small:
        copy.wait()
    ice_cells = ice[...].astype(jnp.float32)
    ground_cells = ground[...].astype(jnp.float32)
    active = ice_cells * (1.0 - (1.0 - is_ice) * ground_cells)
    friction = is_ice * friction_gain * ground_cells * ice_cells
    active_ref[...] = active
    lane = lanes_of(SUBLANES)
    slot = slots_of(SUBLANES)
    half = LANES // 2

    def step(q, total):
        for k in range(3):
            owns, rims_out = (force_own_refs, force_rim_refs) if k == 2 else (own_refs, rim_refs)
            lead = () if k == 2 else (k,)
            low = high = None
            for group in range(2):
                rims = [None] * count
                pair = []
                for j in range(4):
                    layer = q * 8 + group * 4 + j
                    if k == 0:
                        value = jnp.sqrt(conduct[layer].astype(jnp.float32)) * active
                    elif k == 1:
                        value = diag[layer].astype(jnp.float32)
                        if group == 0 and j == 0:
                            value = value + friction * jnp.where(q == 0, 1.0, 0.0)
                    else:
                        value = active * force[layer]
                        total = total + value
                    pieces = [value[:, LANES * p : LANES * (p + 1)] for p in range(count // 2)]
                    halves = [turned(piece, half) for piece in pieces]
                    pair.append((pieces, halves))
                    even = halves if j == 2 else [turned(piece, 32 * j) for piece in pieces]
                    odd = halves if j == 0 else pieces if j == 2 else [turned(piece, half + 32 * j) for piece in pieces]
                    for d in range(count):
                        p = d // 2
                        sources = []
                        if d % 2 == 0:
                            sources.append((RIGHT[j], even[p]))
                            if d:
                                sources.append((LEFT[j], even[p - 1]))
                        else:
                            sources.append((LEFT[j], odd[p]))
                            if d + 1 < count:
                                sources.append((RIGHT[j], odd[p + 1]))
                        for target, source in sources:
                            rims[d] = source if rims[d] is None else jnp.where(slot == target, source, rims[d])
                    if group == 0:
                        first, last, first_slot, last_slot = odd[0], even[-1], RIGHT[j], LEFT[j]
                    else:
                        first, last = turned(pieces[0], 112 + 32 * j), turned(pieces[-1], 80 + 32 * j)
                        first_slot, last_slot = LEFT[j], RIGHT[j]
                    low = first if low is None else jnp.where(slot == first_slot, first, low)
                    high = last if high is None else jnp.where(slot == last_slot, last, high)
                    if j % 2:
                        (even_pieces, even_halves), (odd_pieces, odd_halves) = pair[-2:]
                        packed = []
                        for d in range(count):
                            p = d // 2
                            if d % 2 == 0:
                                packed.append(jnp.where(lane < half, even_pieces[p], odd_halves[p]))
                            else:
                                packed.append(jnp.where(lane < half, even_halves[p], odd_pieces[p]))
                        for ref, packed_value in zip(owns, by_partner(place, packed)):
                            ref[(*lead, q * 4 + group * 2 + j // 2)] = packed_value
                for ref, rim in zip(rims_out, by_partner(place, rims)):
                    ref[(*lead, q * 2 + group)] = rim
            low_ref[k, q] = low
            high_ref[k, q] = high
        return total

    total = jnp.zeros_like(active)
    for c in range(chunks):
        for copy in copies[c]:
            copy.wait()
        total = lax.fori_loop(c * depth // 8, (c + 1) * depth // 8, step, total)
    weight = jnp.sqrt(conduct[where_ref[2]].astype(jnp.float32)) * active
    shared_ref[...] = weight * (total / layers)


def merge_kernel(place_ref, edge_ref, low_ref, high_ref, term_ref, before_ref, after_ref, *refs):
    count = len(refs) // 6
    rims, owns, force_rims, rims_out, *force_out = [refs[count * n : count * (n + 1)] for n in range(6)]
    groups = low_ref.shape[1]
    half_groups = groups // 2
    odd = slots_of(SUBLANES) % 2 == 1
    first = [jnp.where(odd, place_ref[0], -1) == k for k in range(count)]
    last = [jnp.where(odd, -1, place_ref[0] ^ (count - 1)) == k for k in range(count)]

    def step(side, i):
        q = side * half_groups + i
        out = force_out[side]
        for k in range(3):
            before, after = low_ref[k, q], high_ref[k, q]
            if k == 0:
                before, after = before * edge_ref[0], after * edge_ref[1]
            befores, afters = (before, turned(before, 48)), (after, turned(after, 80))
            for n in range(count):
                for group in range(2):
                    g = 2 * q + group
                    rim = force_rims[n][g] if k == 2 else rims[n][k, g]
                    rim = jnp.where(last[n], afters[group], jnp.where(first[n], befores[group], rim))
                    if k == 2:
                        out[n][4 * half_groups + 2 * i + group] = rim
                    else:
                        rims_out[n][k, g] = rim
        for n in range(count):
            for m in range(4):
                out[n][4 * i + m] = owns[n][4 * q + m]

    for i in range(half_groups):
        step(0, i)
        step(1, i)
    lane = lanes_of(SUBLANES)
    half = LANES // 2
    pieces = [term_ref[:, LANES * p : LANES * (p + 1)] for p in range(count // 2)]
    halves = [turned(piece, half) for piece in pieces] + [turned(after_ref[...], half)]
    windows = []
    for d in range(count):
        p = d // 2
        if d % 2 == 0:
            own, right, left = pieces[p], pieces[p], pieces[p - 1] if p else before_ref[...]
        else:
            own, right, left = halves[p], halves[p + 1], halves[p]
        outer = jnp.where(lane >= LANES - HALO, left, 0.0)
        windows.append(jnp.where(lane < half, own, jnp.where(lane < half + HALO, right, outer)))
    for n, value in enumerate(by_partner(place_ref[0], windows)):
        force_out[0][n][6 * half_groups] = value
        force_out[1][n][6 * half_groups] = value


def window_of(own, rim, j, fill):
    lane = lanes_of(SUBLANES)
    half = LANES // 2
    inside = (lane < half + HALO) | (lane >= LANES - HALO)
    return jnp.where(lane < half, turned(own, half * (j % 2)), jnp.where(inside, turned(rim, -32 * j), fill))


def two_sum(a, b):
    total = a + b
    part = total - a
    return total, (a - (total - part)) + (b - part)


def add_pairs(high, low, other_high, other_low):
    total, error = two_sum(high, other_high)
    return total, low + other_low + error


def stencil_first(held_ref, layer, rows):
    def at(shift):
        return held_ref[layer + 1, pl.ds(SUBLANES + shift, rows)]

    here = at(0)
    near = at(1) + at(-1)
    wide = turned(here + cross_weight * near, 1) + far_weight * (here + turned(here, 2))
    far = (at(2) - here) + (at(-2) - here)
    above = held_ref[layer + 2, pl.ds(SUBLANES, rows)] + held_ref[layer, pl.ds(SUBLANES, rows)]
    return near + far_weight * far + vertical_weight * above + wide, wide


def spread_over(held_ref, flat_ref, wide_ref, start, stop, origin, use):
    rows = flat_ref.shape[1]

    def first_half(first, number):
        for u in range(number):
            flat, wide = stencil_first(held_ref, first + u - origin, rows)
            flat_ref[first + u - origin] = flat
            wide_ref[first + u - origin] = wide

    def second_half(first, number):
        for u in range(number):
            spread = flat_ref[first + u - origin] + turned(wide_ref[first + u - origin], -2)
            use(first + u, spread)

    size = min(UNROLL, stop - start)

    def step(b, carry):
        second_half(start + (b - 1) * size, size)
        first_half(start + b * size, size)
        return carry

    whole, rest = divmod(stop - start, size)
    end = start + whole * size
    first_half(start, size)
    lax.fori_loop(1, whole, step, 0)
    second_half(end - size, size)
    if rest:
        first_half(end, rest)
        second_half(end, rest)


def scale_kernel(place_ref, *refs):
    count = (len(refs) - 6) // 2
    own_refs, rim_refs = refs[:count], refs[count : 2 * count]
    scale_ref, factor_ref, held_ref, base_ref, *scratch = refs[2 * count :]
    layers, rows = base_ref.shape[:2]
    clear_edges(held_ref, rows)
    places = partner_rows(place_ref[0], count)
    padded = partner_rows(place_ref[0], count, SUBLANES)

    def gather(first):
        for u in range(2):
            g = first + u
            for n in range(count):
                for j in range(4):
                    layer = 4 * g + j
                    coupling, base = [
                        window_of(own_refs[n][k, 2 * g + j // 2], rim_refs[n][k, g], j, 1.0 if k else 0.0)
                        for k in range(2)
                    ]
                    held_ref[layer + 1, padded[n]] = coupling
                    base_ref[layer, places[n]] = base

    blocks(layers // 4, 2, gather)

    def use(layer, spread):
        coupling = held_ref[layer + 1, pl.ds(SUBLANES, rows)]
        root = jnp.sqrt(base_ref[layer] + coupling * spread)
        inverse = 1.0 / root
        scale_ref[0, layer] = inverse
        scale_ref[1, layer] = root
        factor_ref[layer] = coupling * inverse

    spread_over(held_ref, *scratch, 0, layers, 0, use)


def clear_edges(ref, rows):
    layers = ref.shape[0]
    empty = jnp.zeros((layers, SUBLANES, LANES), jnp.float32)
    ref[:, :SUBLANES] = empty
    ref[:, SUBLANES + rows :] = empty
    ref[0] = jnp.zeros((rows + 2 * SUBLANES, LANES), jnp.float32)
    ref[layers - 1] = jnp.zeros((rows + 2 * SUBLANES, LANES), jnp.float32)


def begin_part(where_ref, scale_ref, factor_ref, force_refs, vector_ref, held_ref, start, origin):
    count = len(force_refs)
    groups = (force_refs[0].shape[0] - 1) // 3
    places = partner_rows(where_ref[1], count)
    padded = partner_rows(where_ref[1], count, SUBLANES)

    def begin(first, number):
        for u in range(number):
            g = first + u
            for n in range(count):
                term = force_refs[n][3 * groups]
                for j in range(4):
                    layer = start + 4 * g + j
                    source = window_of(force_refs[n][2 * g + j // 2], force_refs[n][2 * groups + g], j, 0.0)
                    source = source + term * jnp.where(layer == where_ref[0], 1.0, 0.0)
                    vector = source * scale_ref[0, layer, places[n]]
                    vector_ref[layer - origin, places[n]] = vector
                    held_ref[layer - origin + 1, padded[n]] = factor_ref[layer, places[n]] * vector

    spans(0, groups, 4, begin)


def apply_part(k, factor_ref, basis, held, scratch, start, stop, origin):
    rows = factor_ref.shape[1]
    source_ref, target_ref = held[k % 2], held[(k + 1) % 2]

    def use(layer, spread):
        factor = factor_ref[layer]
        before = basis[k][layer - origin]
        before = (1.0 - SHIFTS[k]) * before if SHIFTS[k] else before
        vector = before - factor * spread
        basis[k + 1][layer - origin] = vector
        if k + 1 < ITERS:
            target_ref[layer - origin + 1, pl.ds(SUBLANES, rows)] = factor * vector

    spread_over(source_ref, *scratch, start, stop, origin, use)


def products_part(basis, gram_ref, layers):
    rows = basis[0].shape[1]
    lane = lanes_of(SUBLANES)
    half = LANES // 2

    def products(first):
        sums = [None] * len(PAIRS)
        for n in range(0, 8, 2):
            for d in range(rows // SUBLANES):
                part = pl.ds(SUBLANES * d, SUBLANES)
                vectors = [
                    jnp.where(lane < half, ref[first + n, part], turned(ref[first + n + 1, part], half))
                    for ref in basis
                ]
                for p, (i, j) in enumerate(PAIRS):
                    product = vectors[j] * vectors[i]
                    sums[p] = product if sums[p] is None else sums[p] + product
        for p in range(len(PAIRS)):
            high, low = add_pairs(gram_ref[0, p], gram_ref[1, p], sums[p], 0.0)
            gram_ref[0, p] = high
            gram_ref[1, p] = low

    blocks(layers, 8, products)


def lower_kernel(where_ref, scale_ref, factor_ref, *refs):
    count = len(refs) - ITERS - 1 - 5
    basis = refs[count : count + ITERS + 1]
    gram_ref, *held, flat_ref, wide_ref = refs[count + ITERS + 1 :]
    scratch = flat_ref, wide_ref
    half, rows = basis[0].shape[:2]
    for ref in held:
        clear_edges(ref, rows)
    begin_part(where_ref, scale_ref, factor_ref, refs[:count], basis[0], held[0], 0, 0)
    for k in range(ITERS):
        apply_part(k, factor_ref, basis, held, scratch, 0, half - 1 - k, 0)
    gram_ref[...] = jnp.zeros(gram_ref.shape, jnp.float32)
    products_part(basis, gram_ref, half - 8)


def upper_kernel(where_ref, scale_ref, factor_ref, *refs):
    count = len(refs) - 2 * (ITERS + 1) - 7
    below = refs[count : count + ITERS + 1]
    part_ref = refs[count + ITERS + 1]
    basis = refs[count + ITERS + 2 : count + 2 * ITERS + 3]
    sums_ref, gram_ref, *held, flat_ref, wide_ref = refs[count + 2 * ITERS + 3 :]
    scratch = flat_ref, wide_ref
    half, rows = below[0].shape[:2]
    layers = factor_ref.shape[0]
    origin = half - 8
    lane = lanes_of(SUBLANES)
    for ref in held:
        clear_edges(ref, rows)
    for k in range(ITERS + 1):
        for layer in range(origin, half - k):
            basis[k][layer - origin] = below[k][layer]
    begin_part(where_ref, scale_ref, factor_ref, refs[:count], basis[0], held[0], half, origin)
    for k in range(ITERS):
        for layer in (half - k - 2, half - k - 1):
            held[k % 2][layer - origin + 1, pl.ds(SUBLANES, rows)] = factor_ref[layer] * below[k][layer]
        apply_part(k, factor_ref, basis, held, scratch, half - 1 - k, layers, origin)
    gram_ref[...] = part_ref[...]
    products_part(basis, gram_ref, layers - origin)
    high, low = gram_ref[0, :, 0], gram_ref[1, :, 0]
    for row in range(1, SUBLANES):
        high, low = add_pairs(high, low, gram_ref[0, :, row], gram_ref[1, :, row])
    turn = LANES // 2
    while turn:
        high, low = add_pairs(high, low, pltpu.roll(high, turn, 1), pltpu.roll(low, turn, 1))
        turn //= 2
    packed = high[:SUBLANES]
    share = LANES // 4
    for g in range(4):
        part = slice(SUBLANES * g, SUBLANES * (g + 1))
        if g:
            packed = jnp.where(lane >= share * g, high[part], packed)
        packed = jnp.where((lane >= share * g + share // 2) & (lane < share * (g + 1)), low[part], packed)
    for d in range(sums_ref.shape[0]):
        sums_ref[d] = packed


def tree_sum(terms):
    while len(terms) > 1:
        terms = [sum(terms[i : i + 2]) for i in range(0, len(terms), 2)]
    return terms[0]


def quadratic(gram, left, right):
    products = []
    for i, a in enumerate(left):
        inside = [gram[max(i, j), min(i, j)] * b for j, b in enumerate(right)]
        products.append(a * tree_sum(inside))
    return tree_sum(products)


def iterate(gram):
    one = jnp.ones_like(gram[0, 0])
    zero = jnp.zeros_like(one)
    residual, direction, answer = [one], [one], []
    norm = gram[0, 0]
    for iteration in range(ITERS):
        applied = [SHIFTS[k] * c if SHIFTS[k] else zero for k, c in enumerate(direction)] + [zero]
        for k, c in enumerate(direction):
            applied[k + 1] = applied[k + 1] + c
        curve = quadratic(gram, direction, applied)
        step = norm / curve
        answer = [a + step * c for a, c in zip(answer + [zero], direction)]
        residual = [r - step * c for r, c in zip(residual + [zero], applied)]
        if iteration + 1 < ITERS:
            following = quadratic(gram, residual, residual)
            ratio = following / norm
            direction = [r + ratio * c for r, c in zip(residual, direction + [zero])]
            norm = following
    return answer, residual


def solve_kernel(sums_ref, coefs_ref, gram_ref):
    share = LANES // 4
    parts = [(sums_ref[d], turned(sums_ref[d], -share // 2)) for d in range(sums_ref.shape[0])]
    while len(parts) > 1:
        parts = [add_pairs(*parts[i], *parts[i + 1]) if i + 1 < len(parts) else parts[i] for i in range(0, len(parts), 2)]
    gram_ref[...] = parts[0][0] + parts[0][1]
    gram = {
        pair: gram_ref[pl.ds(p % SUBLANES, 1), pl.ds(share * (p // SUBLANES), 1)] for p, pair in enumerate(PAIRS)
    }
    answer, residual = iterate(gram)
    for n, coef in enumerate(answer + residual):
        coefs_ref[n] = jnp.broadcast_to(coef, (SUBLANES, LANES))


def combine_kernel(start, depth, where_ref, coefs_ref, *refs):
    basis = refs[: ITERS + 1]
    scale_ref, *out_refs = refs[ITERS + 1 :]
    half = LANES // 2
    lane = lanes_of(SUBLANES)
    rows = partner_rows(where_ref[1], len(out_refs))

    def mix(first):
        answer = [coefs_ref[n] for n in range(ITERS)]
        residual = [coefs_ref[ITERS + n] for n in range(ITERS + 1)]
        for layer in range(8):
            layer = first + layer
            for ref, part in zip(out_refs, rows):
                vectors = [basis_ref[layer, part] for basis_ref in basis]
                answered = tree_sum([c * v for c, v in zip(answer, vectors)]) * scale_ref[0, start + layer, part]
                left = tree_sum([c * v for c, v in zip(residual, vectors)]) * scale_ref[1, start + layer, part]
                ref[layer] = jnp.where(lane < half, answered, turned(left, half))

    blocks(depth, 8, mix)


def finish_kernel(start, depth, count, where_ref, *refs):
    parts = refs[:count]
    solution_ref, residual_ref, solved, left, sems = refs[-5:]
    half = LANES // 2
    lane = lanes_of(SUBLANES)
    copies = []
    for first in range(0, depth, 8):
        for layer in range(first, first + 8):
            got = by_partner(where_ref[1], [ref[layer] for ref in parts])
            for p in range(count // 2):
                place = pl.ds(LANES * p, LANES)
                low, high = got[2 * p : 2 * p + 2]
                solved[layer, :, place] = jnp.where(lane < half, low, turned(high, half))
                left[layer, :, place] = jnp.where(lane < half, turned(low, half), high)
        for n, (held, target) in enumerate(((solved, solution_ref), (left, residual_ref))):
            copy = pltpu.make_async_copy(
                held.at[pl.ds(first, 8)], target.at[0, pl.ds(start + first, 8)], sems.at[n, first // 8]
            )
            copy.start()
            copies.append(copy)
    for copy in copies:
        copy.wait()


def call(kernel, outs, args, smem=0, hbm=0, tail=0, scratch=(), limit=24, flops=10**6, aliases=None, hbm_outs=False):
    out_space = pltpu.HBM if hbm_outs else pltpu.VMEM
    return pl.pallas_call(
        kernel,
        out_shape=[jax.ShapeDtypeStruct(shape, jnp.float32) for shape in outs],
        in_specs=[pl.BlockSpec(memory_space=pltpu.SMEM)] * smem
        + [pl.BlockSpec(memory_space=pltpu.HBM)] * hbm
        + [pl.BlockSpec(memory_space=pltpu.VMEM)] * (len(args) - smem - hbm - tail)
        + [pl.BlockSpec(memory_space=pltpu.HBM)] * tail,
        out_specs=[pl.BlockSpec(memory_space=out_space)] * len(outs),
        scratch_shapes=[pltpu.VMEM(shape, jnp.float32) if isinstance(shape, tuple) else shape for shape in scratch],
        compiler_params=pltpu.CompilerParams(vmem_limit_bytes=limit * 2**20),
        cost_estimate=pl.CostEstimate(flops=flops, bytes_accessed=0, transcendentals=0),
        input_output_aliases=aliases or {},
    )(*args)


def exchanged(parts):
    count = len(parts)
    return [parts[0]] + [
        lax.ppermute(parts[k], "gx", [(i, i ^ k) for i in range(count)]) for k in range(1, count)
    ]


def in_windows(forcing, conduct, diag_add, ice_mask, grounded):
    _, layers, block_x, block_y = forcing.shape
    count_x, count_y = lax.axis_size("gx"), lax.axis_size("gy")
    rows = count_x * block_x
    group = lax.axis_index("group").astype(jnp.int32)
    place_x = lax.axis_index("gx").astype(jnp.int32)
    place_y = lax.axis_index("gy")
    edge = jnp.where(group == 0, 0, layers - 1).astype(jnp.int32)
    inside = jnp.stack([place_y > 0, place_y < count_y - 1]).astype(jnp.float32)
    own = (layers // 2, block_x, LANES)
    rim = (layers // 4, block_x, LANES)
    side = (3, layers // 8, block_x, LANES)
    block = (layers, block_x, block_y)
    chunks = 5 if layers % 40 == 0 else 1
    where = jnp.stack([edge, place_x])
    forcing, conduct, diag_add, ice_mask, grounded = [
        pltpu.with_memory_space_constraint(x, pltpu.HBM)
        for x in (forcing, conduct, diag_add, ice_mask, grounded)
    ]
    *made, low, high, active, shared = call(
        prepare_kernel,
        [(2, *own)] * count_x + [(2, *rim)] * count_x + [own] * count_x + [rim] * count_x
        + [side] * 2 + [ice_mask.shape] * 2,
        (jnp.stack([group, place_x, edge]), forcing, conduct, diag_add, ice_mask, grounded),
        smem=1, hbm=5,
        scratch=[
            block,
            pltpu.VMEM(block, conduct.dtype),
            pltpu.VMEM(block, diag_add.dtype),
            pltpu.VMEM(ice_mask.shape, ice_mask.dtype),
            pltpu.VMEM(grounded.shape, grounded.dtype),
            pltpu.SemaphoreType.DMA((chunks, 3)),
            pltpu.SemaphoreType.DMA((2,)),
        ],
    )
    owns, *left = [made[count_x * n : count_x * (n + 1)] for n in range(4)]
    owns = exchanged(owns)
    received = from_partner(shared, "group", 0)
    up, down = ring(count_y, 1), ring(count_y, -1)
    before, after = lax.ppermute(high, "gy", up), lax.ppermute(low, "gy", down)
    term = active * received
    term_before = lax.ppermute(term[:, -LANES:], "gy", up)
    term_after = lax.ppermute(term[:, :LANES], "gy", down)
    force = ((own[0] + rim[0]) // 2 + 1, block_x, LANES)
    merged = call(
        merge_kernel, [(2, *rim)] * count_x + [force] * 2 * count_x,
        (place_x[None], inside, before, after, term, term_before, term_after, *left[0], *left[1], *left[2]), smem=2,
    )
    rims = exchanged(merged[:count_x])
    forces = []
    for n in range(2):
        forces.append(exchanged(merged[count_x * (n + 1) : count_x * (n + 2)]))
    padded = (layers + 2, rows + 2 * SUBLANES, LANES)
    window = (layers, rows, LANES)
    scale, factor = call(
        scale_kernel, [(2,) + window, window], (place_x[None], *owns, *rims), smem=1,
        scratch=[padded] + [window] * 3,
    )
    half = layers // 2
    depths = (half - 8, layers - half + 8)
    gram = (2, 32, SUBLANES, LANES)
    *below, part = call(
        lower_kernel, [(half, rows, LANES)] * (ITERS + 1) + [gram],
        (where, scale, factor, *forces[0]), smem=1, scratch=[(half + 2,) + padded[1:]] * 2 + [(half, rows, LANES)] * 2, limit=32,
    )
    *beyond, sums = call(
        upper_kernel,
        [(depths[1], rows, LANES)] * (ITERS + 1) + [(count_x * count_y, SUBLANES, LANES)],
        (where, scale, factor, *forces[1], *below, part), smem=1,
        scratch=[gram] + [(depths[1] + 2,) + padded[1:]] * 2 + [(depths[1], rows, LANES)] * 2, limit=32,
    )
    sums = lax.all_to_all(sums, ("gx", "gy"), 0, 0, tiled=True)
    (coefs,) = call(solve_kernel, [(2 * ITERS + 1, SUBLANES, LANES)], (sums,), scratch=[(SUBLANES, LANES)])
    starts = (0, depths[0])
    arrived = []
    for start, depth, basis in zip(starts, depths, (below, beyond)):
        mixed = call(
            functools.partial(combine_kernel, start, depth),
            [(depth, block_x, LANES)] * count_x, (where, coefs, *basis, scale), smem=1,
        )
        arrived.append(exchanged(mixed))
    outs = ()
    for n, (start, depth) in enumerate(zip(starts, depths)):
        outs = tuple(
            call(
                functools.partial(finish_kernel, start, depth, count_x),
                [forcing.shape] * 2, (where, *arrived[n], *outs), smem=1, tail=len(outs), hbm_outs=True,
                scratch=[(depth, block_x, block_y)] * 2 + [pltpu.SemaphoreType.DMA((2, depth // 8))],
                aliases={1 + count_x + i: i for i in range(len(outs))},
            )
        )
    return outs


def fits_windows(layers, block_x, block_y, count_x):
    width = block_y // count_x
    return (
        layers % 16 == 0
        and layers >= 32
        and block_x == SUBLANES
        and block_y % LANES == 0
        and 2 * width == LANES
        and HALO >= 2 * (ITERS + 1)
    )


def per_device(forcing, conduct, diag_add, ice_mask, grounded):
    _, layers, block_x, block_y = forcing.shape
    if not fits_windows(layers, block_x, block_y, lax.axis_size("gx")):
        return on_device(forcing, conduct, diag_add, ice_mask, grounded)
    return in_windows(forcing, conduct, diag_add, ice_mask, grounded)


def solution(mesh):
    in_specs = (
        P("group", None, "gx", "gy"),
        P("group", None, "gx", "gy"),
        P("group", None, "gx", "gy"),
        P("gx", "gy"),
        P("gx", "gy"),
    )
    out_specs = (P("group", None, "gx", "gy"), P("group", None, "gx", "gy"))
    return jax.shard_map(
        per_device, mesh=mesh, in_specs=in_specs, out_specs=out_specs, check_vma=False
    )
```

```python
import functools
import math

import jax
import jax.numpy as jnp
from jax import lax
from jax.experimental import pallas as pl
from jax.experimental.pallas import tpu as pltpu
from jax.sharding import PartitionSpec as P


ITERS = 6
LANES = 128
SUBLANES = 8
HALO = 16
SHIFTS = (0.0, 0.75, 1.5, 0.25, 1.75, 1.0)
UNROLL = 16
PAIRS = tuple((i, j) for i in range(ITERS + 1) for j in range(i + 1) if j < ITERS)


far_weight = 0.25
cross_weight = 0.5
vertical_weight = 4.0
friction_gain = 8.0
NEIGHBOURS = (
    (1, 0, 1.0),
    (-1, 0, 1.0),
    (0, 1, 1.0),
    (0, -1, 1.0),
    (2, 0, far_weight),
    (-2, 0, far_weight),
    (0, 2, far_weight),
    (0, -2, far_weight),
    (1, 1, cross_weight),
    (1, -1, cross_weight),
    (-1, 1, cross_weight),
    (-1, -1, cross_weight),
)


def with_halo(block, sides, width):
    for axis, dim in sides:
        count = lax.axis_size(axis)
        place = lax.axis_index(axis)
        ahead = [(i, (i + 1) % count) for i in range(count)]
        back = [(target, source) for source, target in ahead]
        low = lax.ppermute(
            lax.slice_in_dim(block, block.shape[dim] - width, None, axis=dim), axis, ahead
        )
        high = lax.ppermute(lax.slice_in_dim(block, 0, width, axis=dim), axis, back)
        low = jnp.where(place > 0, low, 0.0)
        high = jnp.where(place < count - 1, high, 0.0)
        block = jnp.concatenate([low, block, high], axis=dim)
    return block


def from_partner(shard, axis, distance):
    return lax.ppermute(shard, axis, [(i, i ^ 1 << distance) for i in range(lax.axis_size(axis))])


def beside_sum(padded, extent_x, extent_y):
    summed = jnp.zeros((padded.shape[0], extent_x, extent_y), jnp.float32)
    for shift_x, shift_y, weight in NEIGHBOURS:
        summed = (
            summed
            + weight
            * padded[:, 2 + shift_x : 2 + shift_x + extent_x, 2 + shift_y : 2 + shift_y + extent_y]
        )
    return summed


def vertical_sum(values):
    zeroes = jnp.zeros_like(values[:1])
    return jnp.concatenate([values[1:], zeroes], 0) + jnp.concatenate([zeroes, values[:-1]], 0)


def spread_padded(padded, values):
    return beside_sum(padded, values.shape[1], values.shape[2]) + vertical_weight * vertical_sum(
        values
    )


def operate(vector, coupling, diagonal):
    scaled = coupling * vector
    padded = with_halo(scaled, (("gx", 1), ("gy", 2)), 2)
    return diagonal * vector - coupling * spread_padded(padded, scaled)


def sum_over(partial, axes):
    count = math.prod(lax.axis_size(axis) for axis in axes)
    sent = jnp.broadcast_to(partial[None, None], (count, 1) + partial.shape)
    return jnp.sum(lax.all_to_all(sent, axes, 0, 0, tiled=True), axis=(0, 1))


def paired_sums(residual, precond, applied):
    partial = jnp.stack([jnp.sum(residual * precond), jnp.sum(applied * precond)])
    summed = sum_over(partial, ("gx", "gy"))
    return summed[0], summed[1]


def on_device(forcing, conduct, diag_add, ice_mask, grounded):
    own_force = forcing[0]
    layers = own_force.shape[0]
    group_id = lax.axis_index("group")
    is_ice = (group_id == 0).astype(jnp.float32)
    ice_cells = ice_mask.astype(jnp.float32)
    ground_cells = grounded.astype(jnp.float32)
    active = ice_cells * (1.0 - (1.0 - is_ice) * ground_cells)
    coupling = jnp.sqrt(conduct[0].astype(jnp.float32)) * active
    layer_index = lax.broadcasted_iota(jnp.int32, (layers, 1, 1), 0)
    edge_layer = jnp.where(group_id == 0, 0, layers - 1).astype(jnp.int32)
    edge_pick = (layer_index == edge_layer).astype(jnp.float32)
    bottom = (layer_index == 0).astype(jnp.float32)
    base_diag = diag_add[0].astype(jnp.float32) + bottom * (
        is_ice * friction_gain * ground_cells * ice_cells
    )
    padded_coupling = with_halo(coupling, (("gx", 1), ("gy", 2)), 2)
    diagonal = base_diag + coupling * spread_padded(padded_coupling, coupling)
    shared_value = active * jnp.mean(own_force, axis=0)
    shared_weight = lax.dynamic_index_in_dim(coupling, edge_layer, 0, keepdims=False)
    received = from_partner(jnp.stack([shared_value, shared_weight]), "group", 0)
    source = active * own_force + edge_pick * (active * received[1] * received[0])
    inverse = 1.0 / diagonal
    solution = jnp.zeros_like(source)
    residual = source
    precond = inverse * residual
    applied = operate(precond, coupling, diagonal)
    norm_now, curve = paired_sums(residual, precond, applied)
    step_size = norm_now / curve
    direction = precond
    along = applied
    for iteration in range(ITERS):
        solution = solution + step_size * direction
        residual = residual - step_size * along
        if iteration + 1 < ITERS:
            precond = inverse * residual
            applied = operate(precond, coupling, diagonal)
            norm_next, curve = paired_sums(residual, precond, applied)
            step_ratio = norm_next / norm_now
            step_size = norm_next / (curve - step_ratio * norm_next / step_size)
            direction = precond + step_ratio * direction
            along = applied + step_ratio * along
            norm_now = norm_next
    return (solution[None], residual[None])


def ring(count, step):
    return [(i, (i + step) % count) for i in range(count)]


def lanes_of(rows):
    return lax.broadcasted_iota(jnp.int32, (rows, LANES), 1)


def blocks(total, size, body):
    def step(g, carry):
        body(g * size)
        return carry

    lax.fori_loop(0, total // size, step, 0)


def spans(start, stop, size, body):
    def step(g, carry):
        body(start + g * size, size)
        return carry

    whole = (stop - start) // size
    if whole:
        lax.fori_loop(0, whole, step, 0)
    if (stop - start) % size:
        body(start + whole * size, (stop - start) % size)


def slots_of(rows):
    return lanes_of(rows) // HALO


RIGHT = tuple((4 + 2 * j) % 8 for j in range(4))
LEFT = tuple((7 + 2 * j) % 8 for j in range(4))


def turned(value, amount):
    return pltpu.roll(value, amount % LANES, 1) if amount % LANES else value


def by_partner(place, values):
    bit = 1
    while bit < len(values):
        swap = (place & bit) != 0
        values = [jnp.where(swap, values[d ^ bit], values[d]) for d in range(len(values))]
        bit *= 2
    return values


def partner_rows(place, count, skip=0):
    return [pl.ds(pl.multiple_of(SUBLANES * (place ^ n) + skip, SUBLANES), SUBLANES) for n in range(count)]


def prepare_kernel(where_ref, force_ref, conduct_ref, diag_ref, ice_ref, ground_ref, *refs):
    count = (len(refs) - 11) // 4
    own_refs, rim_refs, force_own_refs, force_rim_refs = [refs[count * n : count * (n + 1)] for n in range(4)]
    low_ref, high_ref, active_ref, shared_ref, force, conduct, diag, ice, ground, sems, small_sems = refs[4 * count :]
    layers = force.shape[0]
    chunks = sems.shape[0]
    depth = layers // chunks
    small = [
        pltpu.make_async_copy(ice_ref, ice, small_sems.at[0]),
        pltpu.make_async_copy(ground_ref, ground, small_sems.at[1]),
    ]
    copies = []
    for copy in small:
        copy.start()
    for c in range(chunks):
        part = pl.ds(c * depth, depth)
        row = []
        for n, (source, target) in enumerate(((force_ref, force), (conduct_ref, conduct), (diag_ref, diag))):
            copy = pltpu.make_async_copy(source.at[0, part], target.at[part], sems.at[c, n])
            copy.start()
            row.append(copy)
        copies.append(row)
    place = where_ref[1]
    is_ice = jnp.where(where_ref[0] == 0, 1.0, 0.0)
    for copy in small:
        copy.wait()
    ice_cells = ice[...].astype(jnp.float32)
    ground_cells = ground[...].astype(jnp.float32)
    active = ice_cells * (1.0 - (1.0 - is_ice) * ground_cells)
    friction = is_ice * friction_gain * ground_cells * ice_cells
    active_ref[...] = active
    lane = lanes_of(SUBLANES)
    slot = slots_of(SUBLANES)
    half = LANES // 2

    def step(q, total):
        for k in range(3):
            owns, rims_out = (force_own_refs, force_rim_refs) if k == 2 else (own_refs, rim_refs)
            lead = () if k == 2 else (k,)
            low = high = None
            for group in range(2):
                rims = [None] * count
                pair = []
                for j in range(4):
                    layer = q * 8 + group * 4 + j
                    if k == 0:
                        value = jnp.sqrt(conduct[layer].astype(jnp.float32)) * active
                    elif k == 1:
                        value = diag[layer].astype(jnp.float32)
                        if group == 0 and j == 0:
                            value = value + friction * jnp.where(q == 0, 1.0, 0.0)
                    else:
                        value = active * force[layer]
                        total = total + value
                    pieces = [value[:, LANES * p : LANES * (p + 1)] for p in range(count // 2)]
                    halves = [turned(piece, half) for piece in pieces]
                    pair.append((pieces, halves))
                    even = halves if j == 2 else [turned(piece, 32 * j) for piece in pieces]
                    odd = halves if j == 0 else pieces if j == 2 else [turned(piece, half + 32 * j) for piece in pieces]
                    for d in range(count):
                        p = d // 2
                        sources = []
                        if d % 2 == 0:
                            sources.append((RIGHT[j], even[p]))
                            if d:
                                sources.append((LEFT[j], even[p - 1]))
                        else:
                            sources.append((LEFT[j], odd[p]))
                            if d + 1 < count:
                                sources.append((RIGHT[j], odd[p + 1]))
                        for target, source in sources:
                            rims[d] = source if rims[d] is None else jnp.where(slot == target, source, rims[d])
                    if group == 0:
                        first, last, first_slot, last_slot = odd[0], even[-1], RIGHT[j], LEFT[j]
                    else:
                        first, last = turned(pieces[0], 112 + 32 * j), turned(pieces[-1], 80 + 32 * j)
                        first_slot, last_slot = LEFT[j], RIGHT[j]
                    low = first if low is None else jnp.where(slot == first_slot, first, low)
                    high = last if high is None else jnp.where(slot == last_slot, last, high)
                    if j % 2:
                        (even_pieces, even_halves), (odd_pieces, odd_halves) = pair[-2:]
                        packed = []
                        for d in range(count):
                            p = d // 2
                            if d % 2 == 0:
                                packed.append(jnp.where(lane < half, even_pieces[p], odd_halves[p]))
                            else:
                                packed.append(jnp.where(lane < half, even_halves[p], odd_pieces[p]))
                        for ref, packed_value in zip(owns, by_partner(place, packed)):
                            ref[(*lead, q * 4 + group * 2 + j // 2)] = packed_value
                for ref, rim in zip(rims_out, by_partner(place, rims)):
                    ref[(*lead, q * 2 + group)] = rim
            low_ref[k, q] = low
            high_ref[k, q] = high
        return total

    total = jnp.zeros_like(active)
    for c in range(chunks):
        for copy in copies[c]:
            copy.wait()
        total = lax.fori_loop(c * depth // 8, (c + 1) * depth // 8, step, total)
    weight = jnp.sqrt(conduct[where_ref[2]].astype(jnp.float32)) * active
    shared_ref[...] = weight * (total / layers)


def merge_kernel(place_ref, edge_ref, low_ref, high_ref, term_ref, before_ref, after_ref, *refs):
    count = len(refs) // 6
    rims, owns, force_rims, rims_out, *force_out = [refs[count * n : count * (n + 1)] for n in range(6)]
    groups = low_ref.shape[1]
    half_groups = groups // 2
    odd = slots_of(SUBLANES) % 2 == 1
    first = [jnp.where(odd, place_ref[0], -1) == k for k in range(count)]
    last = [jnp.where(odd, -1, place_ref[0] ^ (count - 1)) == k for k in range(count)]

    def step(side, i):
        q = side * half_groups + i
        out = force_out[side]
        for k in range(3):
            before, after = low_ref[k, q], high_ref[k, q]
            if k == 0:
                before, after = before * edge_ref[0], after * edge_ref[1]
            befores, afters = (before, turned(before, 48)), (after, turned(after, 80))
            for n in range(count):
                for group in range(2):
                    g = 2 * q + group
                    rim = force_rims[n][g] if k == 2 else rims[n][k, g]
                    rim = jnp.where(last[n], afters[group], jnp.where(first[n], befores[group], rim))
                    if k == 2:
                        out[n][4 * half_groups + 2 * i + group] = rim
                    else:
                        rims_out[n][k, g] = rim
        for n in range(count):
            for m in range(4):
                out[n][4 * i + m] = owns[n][4 * q + m]

    for i in range(half_groups):
        step(0, i)
        step(1, i)
    lane = lanes_of(SUBLANES)
    half = LANES // 2
    pieces = [term_ref[:, LANES * p : LANES * (p + 1)] for p in range(count // 2)]
    halves = [turned(piece, half) for piece in pieces] + [turned(after_ref[...], half)]
    windows = []
    for d in range(count):
        p = d // 2
        if d % 2 == 0:
            own, right, left = pieces[p], pieces[p], pieces[p - 1] if p else before_ref[...]
        else:
            own, right, left = halves[p], halves[p + 1], halves[p]
        outer = jnp.where(lane >= LANES - HALO, left, 0.0)
        windows.append(jnp.where(lane < half, own, jnp.where(lane < half + HALO, right, outer)))
    for n, value in enumerate(by_partner(place_ref[0], windows)):
        force_out[0][n][6 * half_groups] = value
        force_out[1][n][6 * half_groups] = value


def window_of(own, rim, j, fill):
    lane = lanes_of(SUBLANES)
    half = LANES // 2
    inside = (lane < half + HALO) | (lane >= LANES - HALO)
    return jnp.where(lane < half, turned(own, half * (j % 2)), jnp.where(inside, turned(rim, -32 * j), fill))


def two_sum(a, b):
    total = a + b
    part = total - a
    return total, (a - (total - part)) + (b - part)


def add_pairs(high, low, other_high, other_low):
    total, error = two_sum(high, other_high)
    return total, low + other_low + error


def stencil_first(held_ref, layer, rows):
    def at(shift):
        return held_ref[layer + 1, pl.ds(SUBLANES + shift, rows)]

    here = at(0)
    near = at(1) + at(-1)
    wide = turned(here + cross_weight * near, 1) + far_weight * (here + turned(here, 2))
    far = (at(2) - here) + (at(-2) - here)
    above = held_ref[layer + 2, pl.ds(SUBLANES, rows)] + held_ref[layer, pl.ds(SUBLANES, rows)]
    return near + far_weight * far + vertical_weight * above + wide, wide


def spread_over(held_ref, flat_ref, wide_ref, start, stop, origin, use):
    rows = flat_ref.shape[1]

    def first_half(first, number):
        for u in range(number):
            flat, wide = stencil_first(held_ref, first + u - origin, rows)
            flat_ref[first + u - origin] = flat
            wide_ref[first + u - origin] = wide

    def second_half(first, number):
        for u in range(number):
            spread = flat_ref[first + u - origin] + turned(wide_ref[first + u - origin], -2)
            use(first + u, spread)

    size = min(UNROLL, stop - start)

    def step(b, carry):
        second_half(start + (b - 1) * size, size)
        first_half(start + b * size, size)
        return carry

    whole, rest = divmod(stop - start, size)
    end = start + whole * size
    first_half(start, size)
    lax.fori_loop(1, whole, step, 0)
    second_half(end - size, size)
    if rest:
        first_half(end, rest)
        second_half(end, rest)


def scale_kernel(place_ref, *refs):
    count = (len(refs) - 6) // 2
    own_refs, rim_refs = refs[:count], refs[count : 2 * count]
    scale_ref, factor_ref, held_ref, base_ref, *scratch = refs[2 * count :]
    layers, rows = base_ref.shape[:2]
    clear_edges(held_ref, rows)
    places = partner_rows(place_ref[0], count)
    padded = partner_rows(place_ref[0], count, SUBLANES)

    def gather(first):
        for u in range(2):
            g = first + u
            for n in range(count):
                for j in range(4):
                    layer = 4 * g + j
                    coupling, base = [
                        window_of(own_refs[n][k, 2 * g + j // 2], rim_refs[n][k, g], j, 1.0 if k else 0.0)
                        for k in range(2)
                    ]
                    held_ref[layer + 1, padded[n]] = coupling
                    base_ref[layer, places[n]] = base

    blocks(layers // 4, 2, gather)

    def use(layer, spread):
        coupling = held_ref[layer + 1, pl.ds(SUBLANES, rows)]
        root = jnp.sqrt(base_ref[layer] + coupling * spread)
        inverse = 1.0 / root
        scale_ref[0, layer] = inverse
        scale_ref[1, layer] = root
        factor_ref[layer] = coupling * inverse

    spread_over(held_ref, *scratch, 0, layers, 0, use)


def clear_edges(ref, rows):
    layers = ref.shape[0]
    empty = jnp.zeros((layers, SUBLANES, LANES), jnp.float32)
    ref[:, :SUBLANES] = empty
    ref[:, SUBLANES + rows :] = empty
    ref[0] = jnp.zeros((rows + 2 * SUBLANES, LANES), jnp.float32)
    ref[layers - 1] = jnp.zeros((rows + 2 * SUBLANES, LANES), jnp.float32)


def begin_part(where_ref, scale_ref, factor_ref, force_refs, vector_ref, held_ref, start, origin):
    count = len(force_refs)
    groups = (force_refs[0].shape[0] - 1) // 3
    places = partner_rows(where_ref[1], count)
    padded = partner_rows(where_ref[1], count, SUBLANES)

    def begin(first, number):
        for u in range(number):
            g = first + u
            for n in range(count):
                term = force_refs[n][3 * groups]
                for j in range(4):
                    layer = start + 4 * g + j
                    source = window_of(force_refs[n][2 * g + j // 2], force_refs[n][2 * groups + g], j, 0.0)
                    source = source + term * jnp.where(layer == where_ref[0], 1.0, 0.0)
                    vector = source * scale_ref[0, layer, places[n]]
                    vector_ref[layer - origin, places[n]] = vector
                    held_ref[layer - origin + 1, padded[n]] = factor_ref[layer, places[n]] * vector

    spans(0, groups, 4, begin)


def apply_part(k, factor_ref, basis, held, scratch, start, stop, origin):
    rows = factor_ref.shape[1]
    source_ref, target_ref = held[k % 2], held[(k + 1) % 2]

    def use(layer, spread):
        factor = factor_ref[layer]
        before = basis[k][layer - origin]
        before = (1.0 - SHIFTS[k]) * before if SHIFTS[k] else before
        vector = before - factor * spread
        basis[k + 1][layer - origin] = vector
        if k + 1 < ITERS:
            target_ref[layer - origin + 1, pl.ds(SUBLANES, rows)] = factor * vector

    spread_over(source_ref, *scratch, start, stop, origin, use)


def products_part(basis, gram_ref, layers):
    rows = basis[0].shape[1]
    lane = lanes_of(SUBLANES)
    half = LANES // 2

    def products(first):
        sums = [None] * len(PAIRS)
        for n in range(0, 8, 2):
            for d in range(rows // SUBLANES):
                part = pl.ds(SUBLANES * d, SUBLANES)
                vectors = [
                    jnp.where(lane < half, ref[first + n, part], turned(ref[first + n + 1, part], half))
                    for ref in basis
                ]
                for p, (i, j) in enumerate(PAIRS):
                    product = vectors[j] * vectors[i]
                    sums[p] = product if sums[p] is None else sums[p] + product
        for p in range(len(PAIRS)):
            high, low = add_pairs(gram_ref[0, p], gram_ref[1, p], sums[p], 0.0)
            gram_ref[0, p] = high
            gram_ref[1, p] = low

    blocks(layers, 8, products)


def lower_kernel(where_ref, scale_ref, factor_ref, *refs):
    count = len(refs) - ITERS - 1 - 5
    basis = refs[count : count + ITERS + 1]
    gram_ref, *held, flat_ref, wide_ref = refs[count + ITERS + 1 :]
    scratch = flat_ref, wide_ref
    half, rows = basis[0].shape[:2]
    for ref in held:
        clear_edges(ref, rows)
    begin_part(where_ref, scale_ref, factor_ref, refs[:count], basis[0], held[0], 0, 0)
    for k in range(ITERS):
        apply_part(k, factor_ref, basis, held, scratch, 0, half - 1 - k, 0)
    gram_ref[...] = jnp.zeros(gram_ref.shape, jnp.float32)
    products_part(basis, gram_ref, half - 8)


def upper_kernel(where_ref, scale_ref, factor_ref, *refs):
    count = len(refs) - 2 * (ITERS + 1) - 7
    below = refs[count : count + ITERS + 1]
    part_ref = refs[count + ITERS + 1]
    basis = refs[count + ITERS + 2 : count + 2 * ITERS + 3]
    sums_ref, gram_ref, *held, flat_ref, wide_ref = refs[count + 2 * ITERS + 3 :]
    scratch = flat_ref, wide_ref
    half, rows = below[0].shape[:2]
    layers = factor_ref.shape[0]
    origin = half - 8
    lane = lanes_of(SUBLANES)
    for ref in held:
        clear_edges(ref, rows)
    for k in range(ITERS + 1):
        for layer in range(origin, half - k):
            basis[k][layer - origin] = below[k][layer]
    begin_part(where_ref, scale_ref, factor_ref, refs[:count], basis[0], held[0], half, origin)
    for k in range(ITERS):
        for layer in (half - k - 2, half - k - 1):
            held[k % 2][layer - origin + 1, pl.ds(SUBLANES, rows)] = factor_ref[layer] * below[k][layer]
        apply_part(k, factor_ref, basis, held, scratch, half - 1 - k, layers, origin)
    gram_ref[...] = part_ref[...]
    products_part(basis, gram_ref, layers - origin)
    high, low = gram_ref[0, :, 0], gram_ref[1, :, 0]
    for row in range(1, SUBLANES):
        high, low = add_pairs(high, low, gram_ref[0, :, row], gram_ref[1, :, row])
    for turn, ways in ((32, 4), (8, 4), (2, 4), (1, 2)):
        pairs = [(high, low)] + [(turned(high, turn * n), turned(low, turn * n)) for n in range(1, ways)]
        while len(pairs) > 1:
            pairs = [add_pairs(*pairs[i], *pairs[i + 1]) for i in range(0, len(pairs), 2)]
        high, low = pairs[0]
    packed = high[:SUBLANES]
    share = LANES // 4
    for g in range(4):
        part = slice(SUBLANES * g, SUBLANES * (g + 1))
        if g:
            packed = jnp.where(lane >= share * g, high[part], packed)
        packed = jnp.where((lane >= share * g + share // 2) & (lane < share * (g + 1)), low[part], packed)
    for d in range(sums_ref.shape[0]):
        sums_ref[d] = packed


def tree_sum(terms):
    while len(terms) > 1:
        terms = [sum(terms[i : i + 2]) for i in range(0, len(terms), 2)]
    return terms[0]


def quadratic(gram, left, right):
    products = []
    for i, a in enumerate(left):
        inside = [gram[max(i, j), min(i, j)] * b for j, b in enumerate(right)]
        products.append(a * tree_sum(inside))
    return tree_sum(products)


def iterate(gram):
    one = jnp.ones_like(gram[0, 0])
    zero = jnp.zeros_like(one)
    residual, direction, answer = [one], [one], []
    norm = gram[0, 0]
    for iteration in range(ITERS):
        applied = [SHIFTS[k] * c if SHIFTS[k] else zero for k, c in enumerate(direction)] + [zero]
        for k, c in enumerate(direction):
            applied[k + 1] = applied[k + 1] + c
        curve = quadratic(gram, direction, applied)
        step = norm / curve
        answer = [a + step * c for a, c in zip(answer + [zero], direction)]
        residual = [r - step * c for r, c in zip(residual + [zero], applied)]
        if iteration + 1 < ITERS:
            following = quadratic(gram, residual, residual)
            ratio = following / norm
            direction = [r + ratio * c for r, c in zip(residual, direction + [zero])]
            norm = following
    return answer, residual


def solve_kernel(sums_ref, coefs_ref, gram_ref):
    share = LANES // 4
    parts = [(sums_ref[d], turned(sums_ref[d], -share // 2)) for d in range(sums_ref.shape[0])]
    while len(parts) > 1:
        parts = [add_pairs(*parts[i], *parts[i + 1]) if i + 1 < len(parts) else parts[i] for i in range(0, len(parts), 2)]
    gram_ref[...] = parts[0][0] + parts[0][1]
    gram = {
        pair: gram_ref[pl.ds(p % SUBLANES, 1), pl.ds(share * (p // SUBLANES), 1)] for p, pair in enumerate(PAIRS)
    }
    answer, residual = iterate(gram)
    for n, coef in enumerate(answer + residual):
        coefs_ref[n] = jnp.broadcast_to(coef, (SUBLANES, LANES))


def first_kernel(start, depth, where_ref, sums_ref, *refs):
    *rest, coefs_ref, gram_ref = refs
    solve_kernel(sums_ref, coefs_ref, gram_ref)
    combine_kernel(start, depth, where_ref, coefs_ref, *rest)


def combine_kernel(start, depth, where_ref, coefs_ref, *refs):
    basis = refs[: ITERS + 1]
    scale_ref, *out_refs = refs[ITERS + 1 :]
    half = LANES // 2
    lane = lanes_of(SUBLANES)
    rows = partner_rows(where_ref[1], len(out_refs))

    def mix(first):
        answer = [coefs_ref[n] for n in range(ITERS)]
        residual = [coefs_ref[ITERS + n] for n in range(ITERS + 1)]
        for layer in range(8):
            layer = first + layer
            for ref, part in zip(out_refs, rows):
                vectors = [basis_ref[layer, part] for basis_ref in basis]
                answered = tree_sum([c * v for c, v in zip(answer, vectors)]) * scale_ref[0, start + layer, part]
                left = tree_sum([c * v for c, v in zip(residual, vectors)]) * scale_ref[1, start + layer, part]
                ref[layer] = jnp.where(lane < half, answered, turned(left, half))

    blocks(depth, 8, mix)


def finish_kernel(start, depth, count, where_ref, *refs):
    parts = refs[:count]
    solution_ref, residual_ref, solved, left, sems = refs[-5:]
    half = LANES // 2
    lane = lanes_of(SUBLANES)
    copies = []
    for first in range(0, depth, 8):
        for layer in range(first, first + 8):
            got = by_partner(where_ref[1], [ref[layer] for ref in parts])
            for p in range(count // 2):
                place = pl.ds(LANES * p, LANES)
                low, high = got[2 * p : 2 * p + 2]
                solved[layer, :, place] = jnp.where(lane < half, low, turned(high, half))
                left[layer, :, place] = jnp.where(lane < half, turned(low, half), high)
        for n, (held, target) in enumerate(((solved, solution_ref), (left, residual_ref))):
            copy = pltpu.make_async_copy(
                held.at[pl.ds(first, 8)], target.at[0, pl.ds(start + first, 8)], sems.at[n, first // 8]
            )
            copy.start()
            copies.append(copy)
    for copy in copies:
        copy.wait()


def call(kernel, outs, args, smem=0, hbm=0, tail=0, scratch=(), limit=24, flops=10**6, aliases=None, hbm_outs=False):
    out_space = pltpu.HBM if hbm_outs else pltpu.VMEM
    return pl.pallas_call(
        kernel,
        out_shape=[jax.ShapeDtypeStruct(shape, jnp.float32) for shape in outs],
        in_specs=[pl.BlockSpec(memory_space=pltpu.SMEM)] * smem
        + [pl.BlockSpec(memory_space=pltpu.HBM)] * hbm
        + [pl.BlockSpec(memory_space=pltpu.VMEM)] * (len(args) - smem - hbm - tail)
        + [pl.BlockSpec(memory_space=pltpu.HBM)] * tail,
        out_specs=[pl.BlockSpec(memory_space=out_space)] * len(outs),
        scratch_shapes=[pltpu.VMEM(shape, jnp.float32) if isinstance(shape, tuple) else shape for shape in scratch],
        compiler_params=pltpu.CompilerParams(vmem_limit_bytes=limit * 2**20),
        cost_estimate=pl.CostEstimate(flops=flops, bytes_accessed=0, transcendentals=0),
        input_output_aliases=aliases or {},
    )(*args)


def exchanged(parts):
    count = len(parts)
    return [parts[0]] + [
        lax.ppermute(parts[k], "gx", [(i, i ^ k) for i in range(count)]) for k in range(1, count)
    ]


def in_windows(forcing, conduct, diag_add, ice_mask, grounded):
    _, layers, block_x, block_y = forcing.shape
    count_x, count_y = lax.axis_size("gx"), lax.axis_size("gy")
    rows = count_x * block_x
    group = lax.axis_index("group").astype(jnp.int32)
    place_x = lax.axis_index("gx").astype(jnp.int32)
    place_y = lax.axis_index("gy")
    edge = jnp.where(group == 0, 0, layers - 1).astype(jnp.int32)
    inside = jnp.stack([place_y > 0, place_y < count_y - 1]).astype(jnp.float32)
    own = (layers // 2, block_x, LANES)
    rim = (layers // 4, block_x, LANES)
    side = (3, layers // 8, block_x, LANES)
    block = (layers, block_x, block_y)
    chunks = 5 if layers % 40 == 0 else 1
    where = jnp.stack([edge, place_x])
    forcing, conduct, diag_add, ice_mask, grounded = [
        pltpu.with_memory_space_constraint(x, pltpu.HBM)
        for x in (forcing, conduct, diag_add, ice_mask, grounded)
    ]
    *made, low, high, active, shared = call(
        prepare_kernel,
        [(2, *own)] * count_x + [(2, *rim)] * count_x + [own] * count_x + [rim] * count_x
        + [side] * 2 + [ice_mask.shape] * 2,
        (jnp.stack([group, place_x, edge]), forcing, conduct, diag_add, ice_mask, grounded),
        smem=1, hbm=5,
        scratch=[
            block,
            pltpu.VMEM(block, conduct.dtype),
            pltpu.VMEM(block, diag_add.dtype),
            pltpu.VMEM(ice_mask.shape, ice_mask.dtype),
            pltpu.VMEM(grounded.shape, grounded.dtype),
            pltpu.SemaphoreType.DMA((chunks, 3)),
            pltpu.SemaphoreType.DMA((2,)),
        ],
    )
    owns, *left = [made[count_x * n : count_x * (n + 1)] for n in range(4)]
    owns = exchanged(owns)
    received = from_partner(shared, "group", 0)
    up, down = ring(count_y, 1), ring(count_y, -1)
    before, after = lax.ppermute(high, "gy", up), lax.ppermute(low, "gy", down)
    term = active * received
    term_before = lax.ppermute(term[:, -LANES:], "gy", up)
    term_after = lax.ppermute(term[:, :LANES], "gy", down)
    force = ((own[0] + rim[0]) // 2 + 1, block_x, LANES)
    merged = call(
        merge_kernel, [(2, *rim)] * count_x + [force] * 2 * count_x,
        (place_x[None], inside, before, after, term, term_before, term_after, *left[0], *left[1], *left[2]), smem=2,
    )
    rims = exchanged(merged[:count_x])
    forces = []
    for n in range(2):
        forces.append(exchanged(merged[count_x * (n + 1) : count_x * (n + 2)]))
    padded = (layers + 2, rows + 2 * SUBLANES, LANES)
    window = (layers, rows, LANES)
    scale, factor = call(
        scale_kernel, [(2,) + window, window], (place_x[None], *owns, *rims), smem=1,
        scratch=[padded] + [window] * 3,
    )
    half = layers // 2
    depths = (half - 8, layers - half + 8)
    gram = (2, 32, SUBLANES, LANES)
    *below, part = call(
        lower_kernel, [(half, rows, LANES)] * (ITERS + 1) + [gram],
        (where, scale, factor, *forces[0]), smem=1, scratch=[(half + 2,) + padded[1:]] * 2 + [(half, rows, LANES)] * 2, limit=32,
    )
    *beyond, sums = call(
        upper_kernel,
        [(depths[1], rows, LANES)] * (ITERS + 1) + [(count_x * count_y, SUBLANES, LANES)],
        (where, scale, factor, *forces[1], *below, part), smem=1,
        scratch=[gram] + [(depths[1] + 2,) + padded[1:]] * 2 + [(depths[1], rows, LANES)] * 2, limit=32,
    )
    sums = lax.all_to_all(sums, ("gx", "gy"), 0, 0, tiled=True)
    starts = (0, depths[0])
    arrived = []
    for n, (start, depth, basis) in enumerate(zip(starts, depths, (below, beyond))):
        outs = [(depth, block_x, LANES)] * count_x
        if n == 0:
            *mixed, coefs = call(
                functools.partial(first_kernel, start, depth),
                outs + [(2 * ITERS + 1, SUBLANES, LANES)], (where, sums, *basis, scale), smem=1,
                scratch=[(SUBLANES, LANES)],
            )
        else:
            mixed = call(
                functools.partial(combine_kernel, start, depth),
                outs, (where, coefs, *basis, scale), smem=1,
            )
        arrived.append(exchanged(mixed))
    outs = ()
    for n, (start, depth) in enumerate(zip(starts, depths)):
        outs = tuple(
            call(
                functools.partial(finish_kernel, start, depth, count_x),
                [forcing.shape] * 2, (where, *arrived[n], *outs), smem=1, tail=len(outs), hbm_outs=True,
                scratch=[(depth, block_x, block_y)] * 2 + [pltpu.SemaphoreType.DMA((2, depth // 8))],
                aliases={1 + count_x + i: i for i in range(len(outs))},
            )
        )
    return outs


def fits_windows(layers, block_x, block_y, count_x):
    width = block_y // count_x
    return (
        layers % 16 == 0
        and layers >= 32
        and block_x == SUBLANES
        and block_y % LANES == 0
        and 2 * width == LANES
        and HALO >= 2 * (ITERS + 1)
    )


def per_device(forcing, conduct, diag_add, ice_mask, grounded):
    _, layers, block_x, block_y = forcing.shape
    if not fits_windows(layers, block_x, block_y, lax.axis_size("gx")):
        return on_device(forcing, conduct, diag_add, ice_mask, grounded)
    return in_windows(forcing, conduct, diag_add, ice_mask, grounded)


def solution(mesh):
    in_specs = (
        P("group", None, "gx", "gy"),
        P("group", None, "gx", "gy"),
        P("group", None, "gx", "gy"),
        P("gx", "gy"),
        P("gx", "gy"),
    )
    out_specs = (P("group", None, "gx", "gy"), P("group", None, "gx", "gy"))
    return jax.shard_map(
        per_device, mesh=mesh, in_specs=in_specs, out_specs=out_specs, check_vma=False
    )
```
